8 devices in a mesh: dp: 2 (over z, y), sp: 4 (over x, core).
Axes of the slice: x: 2, y: 2, z: 1, core: 2. Of those that a mesh axis runs over, the one named last changes fastest.
Arguments:
- image_tokens: bfloat16 [32, 1024, 1536], P('dp', 'sp'), parts along dimension 0
- ln1_gain: float32 [2, 1536], replicated
- ln1_shift: float32 [2, 1536], replicated
- w_qkv: bfloat16 [2, 1536, 3, 16, 96], replicated
- b_qkv: float32 [2, 3, 16, 96], replicated
- w_out: bfloat16 [2, 16, 96, 1536], replicated
- b_out: float32 [2, 1536], replicated
- ln2_gain: float32 [2, 1536], replicated
- ln2_shift: float32 [2, 1536], replicated
- w_up: bfloat16 [2, 1536, 6144], replicated
- b_up: float32 [2, 6144], replicated
- w_down: bfloat16 [2, 6144, 1536], replicated
- b_down: float32 [2, 1536], replicated
Outputs:
- output: bfloat16 [32, 1024, 1536], P('dp', 'sp'), parts along dimension 0
There are 2 independent parts. The reference program is written for one: setup_inputs(seed, part) draws one part's arguments, and reference() takes and returns one part's arrays. A program takes and returns all parts, laid end to end along the dimension named above; an argument that names none is the same for every part.
All inputs are finite; a program needn't handle non-finite values.
Results may differ from the reference program's by a relative error of at most 0.014479.
Values are sent between devices in bfloat16 or wider.
A program may use at most 1 GiB of HBM per device.

```python
import jax
import jax.numpy as jnp
from jax import lax

IMAGES = 16
SEQ_LEN = 1024
WIDTH = 1536
HEADS = 16
HEAD_DIM = 96
MLP_DIM = 6144
LAYERS = 2
LN_EPS = 1e-6


def layer_norm(tokens, ln_gain, ln_shift):
    values = tokens.astype(jnp.float32)
    mean_val = jnp.mean(values, axis=-1, keepdims=True)
    centred = values - mean_val
    var_val = jnp.mean(centred * centred, axis=-1, keepdims=True)
    return (centred * lax.rsqrt(var_val + LN_EPS) * ln_gain + ln_shift).astype(jnp.bfloat16)


def one_head(head_inputs):
    q_head, k_head, v_head = head_inputs
    score_scale = q_head.shape[-1] ** -0.5
    scores = jnp.einsum('bqe,bke->bqk', q_head.astype(jnp.float32), k_head.astype(jnp.float32)) * score_scale
    row_peak = jnp.max(scores, axis=-1, keepdims=True)
    prob_vals = jnp.exp(scores - row_peak)
    row_total = jnp.sum(prob_vals, axis=-1, keepdims=True)
    mixed_vals = jnp.einsum('bqk,bke->bqe', prob_vals.astype(jnp.bfloat16).astype(jnp.float32), v_head.astype(jnp.float32))
    return (mixed_vals / row_total).astype(jnp.bfloat16)


def encoder_layer(hidden, layer_params):
    (ln1_gain, ln1_shift, w_qkv, b_qkv, w_out, b_out, ln2_gain, ln2_shift, w_up, b_up, w_down, b_down) = layer_params
    normed = layer_norm(hidden, ln1_gain, ln1_shift)
    qkv_all = jnp.einsum('bsd,dthe->bsthe', normed.astype(jnp.float32), w_qkv.astype(jnp.float32)) + b_qkv
    per_head = jnp.moveaxis(qkv_all.astype(jnp.bfloat16), 3, 0)
    heads_out = lax.map(one_head, (per_head[:, :, :, 0], per_head[:, :, :, 1], per_head[:, :, :, 2]))
    attn_proj = jnp.einsum('hbse,hed->bsd', heads_out.astype(jnp.float32), w_out.astype(jnp.float32)) + b_out
    mid_state = (hidden.astype(jnp.float32) + attn_proj).astype(jnp.bfloat16)
    normed_two = layer_norm(mid_state, ln2_gain, ln2_shift)
    up_proj = jnp.einsum('bsd,df->bsf', normed_two.astype(jnp.float32), w_up.astype(jnp.float32)) + b_up
    active = jax.nn.gelu(up_proj, approximate=True).astype(jnp.bfloat16)
    down_proj = jnp.einsum('bsf,fd->bsd', active.astype(jnp.float32), w_down.astype(jnp.float32)) + b_down
    return (mid_state.astype(jnp.float32) + down_proj).astype(jnp.bfloat16)


def setup_inputs(seed: int = 0, part: int = 0) -> dict:
    part_key = jax.random.fold_in(jax.random.key(seed), part)
    key_pattern, key_noise = jax.random.split(part_key, 2)
    period = SEQ_LEN // 8
    half_width = WIDTH // 2
    pattern = jax.random.normal(key_pattern, (IMAGES, period, half_width), jnp.float32)
    repeated = jnp.tile(pattern, (1, SEQ_LEN // period, 1))
    noise_part = jax.random.normal(key_noise, (IMAGES, SEQ_LEN, WIDTH - half_width), jnp.float32)
    image_tokens = jnp.concatenate([repeated, noise_part], axis=-1).astype(jnp.bfloat16)
    key_set = jax.random.split(jax.random.key(seed + 1), 14)
    row_scale = jnp.where(jnp.arange(WIDTH) < half_width, 1.0, 0.2)[:, None, None]
    head_shape = (LAYERS, WIDTH, HEADS, HEAD_DIM)
    w_query = 2.0 * WIDTH ** -0.5 * row_scale * jax.random.normal(key_set[0], head_shape, jnp.float32)
    w_key = w_query + 0.1 * WIDTH ** -0.5 * jax.random.normal(key_set[1], head_shape, jnp.float32)
    w_value = WIDTH ** -0.5 * jax.random.normal(key_set[2], head_shape, jnp.float32)
    w_qkv = jnp.stack([w_query, w_key, w_value], axis=2).astype(jnp.bfloat16)
    b_qkv = 0.3 * jax.random.normal(key_set[3], (LAYERS, 3, HEADS, HEAD_DIM), jnp.float32)
    w_out = (1.5 * WIDTH ** -0.5 * jax.random.normal(key_set[4], (LAYERS, HEADS, HEAD_DIM, WIDTH), jnp.float32)).astype(jnp.bfloat16)
    b_out = 0.3 * jax.random.normal(key_set[5], (LAYERS, WIDTH), jnp.float32)
    ln1_gain = 1.0 + 0.2 * jax.random.normal(key_set[6], (LAYERS, WIDTH), jnp.float32)
    ln1_shift = 0.3 * jax.random.normal(key_set[7], (LAYERS, WIDTH), jnp.float32)
    ln2_gain = 1.0 + 0.2 * jax.random.normal(key_set[8], (LAYERS, WIDTH), jnp.float32)
    ln2_shift = 0.3 * jax.random.normal(key_set[9], (LAYERS, WIDTH), jnp.float32)
    w_up = (WIDTH ** -0.5 * jax.random.normal(key_set[10], (LAYERS, WIDTH, MLP_DIM), jnp.float32)).astype(jnp.bfloat16)
    b_up = 0.3 * jax.random.normal(key_set[11], (LAYERS, MLP_DIM), jnp.float32)
    w_down = (0.5 * MLP_DIM ** -0.5 * jax.random.normal(key_set[12], (LAYERS, MLP_DIM, WIDTH), jnp.float32)).astype(jnp.bfloat16)
    b_down = 0.3 * jax.random.normal(key_set[13], (LAYERS, WIDTH), jnp.float32)
    return {'image_tokens': image_tokens, 'ln1_gain': ln1_gain, 'ln1_shift': ln1_shift, 'w_qkv': w_qkv, 'b_qkv': b_qkv, 'w_out': w_out, 'b_out': b_out, 'ln2_gain': ln2_gain, 'ln2_shift': ln2_shift, 'w_up': w_up, 'b_up': b_up, 'w_down': w_down, 'b_down': b_down}


def reference(image_tokens, ln1_gain, ln1_shift, w_qkv, b_qkv, w_out, b_out, ln2_gain, ln2_shift, w_up, b_up, w_down, b_down):
    stacked = (ln1_gain, ln1_shift, w_qkv, b_qkv, w_out, b_out, ln2_gain, ln2_shift, w_up, b_up, w_down, b_down)

    def layer_body(hidden, layer_params):
        return encoder_layer(hidden, layer_params), None

    return lax.scan(layer_body, image_tokens, stacked)[0]
```

```python
import jax
import jax.numpy as jnp
from jax import lax
from jax.sharding import PartitionSpec as P

LN_EPS = 1e-6


def layer_norm(tokens, ln_gain, ln_shift):
    values = tokens.astype(jnp.float32)
    mean_val = jnp.mean(values, axis=-1, keepdims=True)
    centred = values - mean_val
    var_val = jnp.mean(centred * centred, axis=-1, keepdims=True)
    return (centred * lax.rsqrt(var_val + LN_EPS) * ln_gain + ln_shift).astype(jnp.bfloat16)


def attend(q_part, k_part, v_part):
    score_scale = q_part.shape[-1] ** -0.5
    scores = jnp.einsum('bqhe,bkhe->bhqk', q_part, k_part, preferred_element_type=jnp.float32) * score_scale
    row_peak = jnp.max(scores, axis=-1, keepdims=True)
    prob_vals = jnp.exp(scores - row_peak)
    row_total = jnp.sum(prob_vals, axis=-1, keepdims=True)
    mixed_vals = jnp.einsum('bhqk,bkhe->bhqe', prob_vals.astype(jnp.bfloat16), v_part, preferred_element_type=jnp.float32)
    return (mixed_vals / row_total).astype(jnp.bfloat16)


def mlp_block(mid_state, ln2_gain, ln2_shift, w_up, b_up, w_down, b_down):
    normed = layer_norm(mid_state, ln2_gain, ln2_shift)
    up_proj = jnp.einsum('bsd,df->bsf', normed, w_up, preferred_element_type=jnp.float32) + b_up
    active = jax.nn.gelu(up_proj, approximate=True).astype(jnp.bfloat16)
    down_proj = jnp.einsum('bsf,fd->bsd', active, w_down, preferred_element_type=jnp.float32) + b_down
    return (mid_state.astype(jnp.float32) + down_proj).astype(jnp.bfloat16)


def solution(mesh):
    token_spec = P('dp', 'sp', None)

    def device_step(image_tokens, ln1_gain, ln1_shift, w_qkv, b_qkv, w_out, b_out, ln2_gain, ln2_shift, w_up, b_up, w_down, b_down):
        hidden = lax.all_to_all(image_tokens, 'sp', 0, 1, tiled=True)
        for layer_idx in range(w_qkv.shape[0]):
            normed = layer_norm(hidden, ln1_gain[layer_idx], ln1_shift[layer_idx])
            qkv = (jnp.einsum('bsd,dthe->bsthe', normed, w_qkv[layer_idx], preferred_element_type=jnp.float32) + b_qkv[layer_idx]).astype(jnp.bfloat16)
            attn = attend(qkv[:, :, 0], qkv[:, :, 1], qkv[:, :, 2])
            attn_proj = jnp.einsum('bhse,hed->bsd', attn, w_out[layer_idx], preferred_element_type=jnp.float32) + b_out[layer_idx]
            mid_state = (hidden.astype(jnp.float32) + attn_proj).astype(jnp.bfloat16)
            hidden = mlp_block(mid_state, ln2_gain[layer_idx], ln2_shift[layer_idx], w_up[layer_idx], b_up[layer_idx], w_down[layer_idx], b_down[layer_idx])
        return lax.all_to_all(hidden, 'sp', 1, 0, tiled=True)

    return jax.shard_map(device_step, mesh=mesh, in_specs=(token_spec,) + (P(),) * 12, out_specs=token_spec, check_vma=False)
```

```python
import functools
import jax
import jax.numpy as jnp
from jax import lax
from jax.experimental import pallas as pl
from jax.experimental.pallas import tpu as pltpu
from jax.sharding import PartitionSpec as P

LN_EPS = 1e-6
HD = 96
HEADS = 16
D = 1536
F = 6144
SEQ = 1024
C = HD ** -0.5 * 1.4426950408889634
LOW = 2.0 ** -80
VMEM_MAX = 67043328
f32, bf16 = jnp.float32, jnp.bfloat16

def dot_nt(a, b):
    return lax.dot_general(a, b, (((1,), (1,)), ((), ())), preferred_element_type=f32)

def dot_tn(a, b):
    return lax.dot_general(a, b, (((0,), (0,)), ((), ())), preferred_element_type=f32)

def dot(a, b):
    return jnp.dot(a, b, preferred_element_type=f32)

def ln_rows(load, store, gain, shift, rows, step=16):
    for r in range(0, rows, step):
        v = load(r, step)
        mu = jnp.sum(v, axis=-1, keepdims=True) * (1.0 / D)
        c = v - mu
        var = jnp.sum(c * c, axis=-1, keepdims=True) * (1.0 / D)
        store(r, step, (c * lax.rsqrt(var + LN_EPS) * gain + shift).astype(bf16))

def qkv_kernel(x_ref, xn_ref, g_ref, s_ref, w_hbm, b_ref, q_ref, k_ref, v_ref, nq_ref, nk_ref, w, na, nb, sem, *, layer, tm):
    i = pl.program_id(0)
    ch = 4 * HD
    per = D // ch
    cuts = (0, ch, 4 * ch, 12 * ch)
    order = [1, 0, 2]
    use = [t * D + c * ch for t in order for c in range(per)]
    def copy(n):
        return pltpu.make_async_copy(w_hbm.at[layer, pl.ds(use[n], ch)], w.at[pl.ds(use[n], ch)], sem.at[n])
    gain, shift = g_ref[...], s_ref[...]
    def norm(src, r0, dst):
        def st(r, n, v):
            dst[r:r + n, :] = v
        return lambda lo, n: ln_rows(lambda r, m: src[r0 + lo + r:r0 + lo + r + m, :].astype(f32), lambda r, m, v: st(lo + r, m, v), gain, shift, n)
    @pl.when(i == 0)
    def _():
        for n in range(len(use)):
            copy(n).start()
        norm(x_ref, 0, na)(0, tm)
        copy(0).wait()
    waits = {1: (1, 4), 4: (4, 12)}
    for sub, n_s in ((0, na), (1, nb)):
        nxt = norm(x_ref, tm, nb) if sub == 0 else norm(xn_ref, 0, na)
        cols = slice(sub * tm, (sub + 1) * tm)
        for n in range(len(use)):
            if sub == 0 and n in waits:
                @pl.when(i == 0)
                def _():
                    for c in range(*waits[n]):
                        copy(c).wait()
            t, c = order[n // per], n % per
            r0 = use[n]
            y = dot_nt(w[r0:r0 + ch, :], n_s[...])
            bias = jnp.concatenate([b_ref[r0:r0 + ch, :]] * (tm // 128), axis=1)
            yb = (y + bias).astype(bf16)
            if t == 2:
                v_ref[c * ch:(c + 1) * ch, cols] = yb
            else:
                if t == 0:
                    q_ref[c * ch:(c + 1) * ch, cols] = yb
                for h in range(4):
                    hh = c * 4 + h
                    yh = yb[h * HD:(h + 1) * HD, :]
                    yf = yh.astype(f32)
                    nn = jnp.sum(yf * yf, axis=0, keepdims=True)
                    if t == 0:
                        nq_ref[hh:hh + 1, cols] = nn
                    else:
                        nk_ref[hh:hh + 1, cols] = nn
                        one = (lax.broadcasted_iota(jnp.int32, (32, tm), 0) == 0).astype(f32).astype(bf16)
                        k_ref[hh, cols, :] = jnp.concatenate([yh, one], axis=0).T
            if sub == 0 and n >= 4:
                lo = (n - 4) * (tm // 8)
                nxt(lo, tm // 8)
        if sub == 1:
            nxt(0, tm)

def qkv(x, g, s, wt, b, layer, flags=None):
    T = x.shape[0]
    tm = 512
    n = T // (2 * tm)
    row = pl.BlockSpec((1, D), lambda i: (0, 0))
    col = lambda r: pl.BlockSpec((r, 2 * tm), lambda i: (0, i))
    sd = jax.ShapeDtypeStruct
    return pl.pallas_call(
        functools.partial(qkv_kernel, layer=layer, tm=tm),
        out_shape=(sd((D, T), bf16), sd((HEADS, T, 128), bf16), sd((D, T), bf16), sd((HEADS, T), f32), sd((HEADS, T), f32)),
        grid=(n,),
        in_specs=[pl.BlockSpec((2 * tm, D), lambda i: (i, 0)),
                  pl.BlockSpec((tm, D), lambda i: (jnp.minimum(2 * (i + 1), 2 * n - 1), 0)),
                  row, row, pl.BlockSpec(memory_space=pltpu.HBM), pl.BlockSpec((3 * D, 128), lambda i: (0, 0))],
        out_specs=(col(D), pl.BlockSpec((HEADS, 2 * tm, 128), lambda i: (0, i, 0)), col(D), col(HEADS), col(HEADS)),
        scratch_shapes=[pltpu.VMEM((3 * D, D), bf16), pltpu.VMEM((tm, D), bf16), pltpu.VMEM((tm, D), bf16),
                        pltpu.SemaphoreType.DMA((12,))],
        compiler_params=pltpu.CompilerParams(vmem_limit_bytes=VMEM_MAX, dimension_semantics=("arbitrary",), **({"flags": flags} if flags else {})),
        cost_estimate=pl.CostEstimate(flops=2 * T * D * 3 * D, bytes_accessed=3 * D * D * 2 + T * D * 10, transcendentals=0),
        name="qkv",
    )(x, x, g, s, wt, b)

def attn_kernel(q_ref, k_ref, v_ref, nq_ref, nk_ref, o_ref, *, hp, nq, kb, lag):
    S = q_ref.shape[-1]
    nk = S // kb
    units = [(h, q, k) for h in range(hp) for q in range(S // nq) for k in range(nk)]
    st, lows, acc, rhs = {}, [], {}, {}
    def rows(h):
        return slice(h * HD, (h + 1) * HD)
    def shift_rows(h, q):
        kmax = jnp.max(nk_ref[h:h + 1, :], axis=1, keepdims=True)
        m = jnp.sqrt(nq_ref[h:h + 1, q * nq:(q + 1) * nq] * kmax) * (-1.0 - 2.0 ** -7)
        tile = jnp.where(lax.broadcasted_iota(jnp.int32, (32, nq), 0) == 0, jnp.broadcast_to(m, (32, nq)), 0.0)
        return tile.astype(bf16)
    def score(u):
        h, q, k = u
        if k == 0:
            rhs[h, q] = jnp.concatenate([q_ref[rows(h), q * nq:(q + 1) * nq], shift_rows(h, q)], axis=0)
        st[u] = dot(k_ref[h, k * kb:(k + 1) * kb, :], rhs[h, q])
    def mix(u):
        h, q, k = u
        p = jnp.exp2(st.pop(u) * C)
        ls = jnp.sum(p.reshape(kb // 8, 8, nq), axis=0)
        pv = dot(v_ref[rows(h), k * kb:(k + 1) * kb], p.astype(bf16))
        if k:
            a, b = acc[h, q]
            ls, pv = a + ls, b + pv
        acc[h, q] = (ls, pv)
        if k == nk - 1:
            a, b = acc.pop((h, q))
            l = jnp.sum(a, axis=0, keepdims=True)
            lows.append(l)
            o_ref[rows(h), q * nq:(q + 1) * nq] = (b * (1.0 / l)).astype(bf16)
    n = len(units)
    for i in range(n + lag):
        if i < n:
            score(units[i])
        if i >= lag:
            mix(units[i - lag])
    low = lows[0]
    for l in lows[1:]:
        low = jnp.minimum(low, l)
    low = jnp.min(low)

    @pl.when(jnp.logical_not(low >= LOW))
    def _():
        qb = 256
        def body(j, c):
            h = lax.div(j, S // qb)
            qs = pl.ds(pl.multiple_of(lax.rem(j, S // qb) * qb, qb), qb)
            r = pl.ds(pl.multiple_of(h * HD, 32), HD)
            s = dot(k_ref[h, :, :HD], q_ref[r, qs])
            m = jnp.max(s, axis=0, keepdims=True)
            p = jnp.exp2((s - m) * C)
            l = jnp.sum(p, axis=0, keepdims=True)
            o_ref[r, qs] = (dot(v_ref[r, :], p.astype(bf16)) / l).astype(bf16)
            return c
        lax.fori_loop(0, hp * (S // qb), body, 0)

def attn(q, k, v, nq2, nk2, hp=8, nq=512, kb=256, lag=3, flags=None):
    T = q.shape[1]
    S = SEQ
    nh = HEADS // hp
    blk = pl.BlockSpec((hp * HD, S), lambda i, j: (j, i))
    nrm = pl.BlockSpec((hp, S), lambda i, j: (j, i))
    return pl.pallas_call(
        functools.partial(attn_kernel, hp=hp, nq=nq, kb=kb, lag=lag),
        out_shape=jax.ShapeDtypeStruct((D, T), bf16),
        grid=(T // S, nh),
        in_specs=[blk, pl.BlockSpec((hp, S, 128), lambda i, j: (j, i, 0)), blk, nrm, nrm],
        out_specs=blk,
        compiler_params=pltpu.CompilerParams(vmem_limit_bytes=VMEM_MAX, dimension_semantics=("arbitrary", "arbitrary"), **({"flags": flags} if flags else {})),
        cost_estimate=pl.CostEstimate(flops=4 * T * S * D, bytes_accessed=T * D * 9, transcendentals=T * S * HEADS),
        name="attn",
    )(q, k, v, nq2, nk2)

def gelu(u):
    c = 0.7978845608028654
    return (0.5 * u) * (1.0 + jnp.tanh(u * (c + (c * 0.044715) * (u * u))))

def mlp_kernel(x_hbm, o_hbm, wo_hbm, bo_ref, g_ref, s_ref, wu_hbm, bu_ref, wd_hbm, bd_ref, out_ref,
               xb, ob, wo, wu, wd, m_s, n_s, act, acc, xsem, osem, wsem, *, layer, tm, fc, nc):
    i = pl.program_id(0)
    nblk = pl.num_programs(0)
    nj = F // fc
    def x_copy(b, slot):
        return pltpu.make_async_copy(x_hbm.at[pl.ds(b * tm, tm)], xb.at[slot], xsem.at[slot])
    def o_copy(b, slot):
        return pltpu.make_async_copy(o_hbm.at[:, pl.ds(b * tm, tm)], ob.at[slot], osem.at[slot])
    wo_copy = pltpu.make_async_copy(wo_hbm.at[layer], wo, wsem.at[0])
    def wu_copy(j):
        return pltpu.make_async_copy(wu_hbm.at[layer, :, pl.ds(j * fc, fc)], wu.at[:, pl.ds(j * fc, fc)], wsem.at[1 + j])
    def wd_copy(j):
        return pltpu.make_async_copy(wd_hbm.at[layer, pl.ds(j * fc, fc)], wd.at[pl.ds(j * fc, fc)], wsem.at[1 + nj + j])
    gain, shift = g_ref[...], s_ref[...]
    bo = bo_ref[...]

    def project(slot, c):
        cs = slice(c * nc, (c + 1) * nc)
        y = dot_tn(ob[slot], wo[:, cs])
        m_s[:, cs] = (xb[slot, :, cs].astype(f32) + (y + bo[:, cs])).astype(bf16)

    def norm():
        def st(r, n, v):
            n_s[r:r + n, :] = v
        ln_rows(lambda r, n: m_s[r:r + n, :].astype(f32), st, gain, shift, tm)

    @pl.when(i == 0)
    def _():
        x_copy(0, 0).start()
        o_copy(0, 0).start()
        wo_copy.start()
        wu_copy(0).start()
        for j in range(nj):
            if j + 1 < nj:
                wu_copy(j + 1).start()
            wd_copy(j).start()
        x_copy(1, 1).start()
        o_copy(1, 1).start()
        x_copy(0, 0).wait()
        o_copy(0, 0).wait()
        wo_copy.wait()
        for c in range(D // nc):
            project(0, c)
        norm()
        wu_copy(0).wait()

    def up(j, c):
        f0 = j * fc + c * nc
        u = dot(n_s[...], wu[:, f0:f0 + nc]) + bu_ref[:, f0:f0 + nc]
        act[j % 2, :, c * nc:(c + 1) * nc] = gelu(u).astype(bf16)

    def down(j, c):
        cs = slice(c * nc, (c + 1) * nc)
        y = dot(act[j % 2], wd[j * fc:(j + 1) * fc, cs])
        if j == 0:
            acc[:, cs] = (m_s[:, cs].astype(f32) + bd_ref[:, cs]) + y
        elif j < nj - 1:
            acc[:, cs] = acc[:, cs] + y
        else:
            out_ref[:, cs] = (acc[:, cs] + y).astype(bf16)

    for c in range(fc // nc):
        up(0, c)
    for j in range(1, nj):
        if j <= 2:
            @pl.when(i == 0)
            def _():
                if j == 1:
                    wu_copy(1).wait()
                    wd_copy(0).wait()
                else:
                    for jj in range(2, nj):
                        wu_copy(jj).wait()
                    for jj in range(1, nj):
                        wd_copy(jj).wait()
        for c in range(max(fc, D) // nc):
            if c < fc // nc:
                up(j, c)
            if c < D // nc:
                down(j - 1, c)
    slot = lax.rem(i + 1, 2)

    @pl.when(i + 1 < nblk)
    def _():
        x_copy(i + 1, slot).wait()
        o_copy(i + 1, slot).wait()

    @pl.when(i + 2 < nblk)
    def _():
        x_copy(i + 2, 1 - slot).start()
        o_copy(i + 2, 1 - slot).start()

    for c in range(D // nc):
        project(slot, c)
    for c in range(D // nc):
        down(nj - 1, c)
    norm()

def mlp(x, o, wo, bo, g, s, wu, bu, wd, bd, layer, tm=512, fc=1024, nc=256, flags=None):
    T = x.shape[0]
    row = lambda n: pl.BlockSpec((1, n), lambda i: (0, 0))
    hbm = pl.BlockSpec(memory_space=pltpu.HBM)
    nj = F // fc
    dma = pltpu.SemaphoreType.DMA
    return pl.pallas_call(
        functools.partial(mlp_kernel, layer=layer, tm=tm, fc=fc, nc=nc),
        out_shape=jax.ShapeDtypeStruct((T, D), bf16),
        grid=(T // tm,),
        in_specs=[hbm, hbm, hbm, row(D), row(D), row(D), hbm, row(F), hbm, row(D)],
        out_specs=pl.BlockSpec((tm, D), lambda i: (i, 0)),
        scratch_shapes=[pltpu.VMEM((2, tm, D), bf16), pltpu.VMEM((2, D, tm), bf16), pltpu.VMEM((D, D), bf16),
                        pltpu.VMEM((D, F), bf16), pltpu.VMEM((F, D), bf16), pltpu.VMEM((tm, D), bf16), pltpu.VMEM((tm, D), bf16),
                        pltpu.VMEM((2, tm, fc), bf16), pltpu.VMEM((tm, D), f32), dma((2,)), dma((2,)), dma((1 + 2 * nj,))],
        compiler_params=pltpu.CompilerParams(vmem_limit_bytes=VMEM_MAX, dimension_semantics=("arbitrary",), **({"flags": flags} if flags else {})),
        cost_estimate=pl.CostEstimate(flops=2 * T * D * (2 * F + D), bytes_accessed=(2 * F + D) * D * 2 + T * D * 6, transcendentals=T * F),
        name="mlp",
    )(x, o, wo, bo, g, s, wu, bu, wd, bd)


def solution(mesh):
    token_spec = P('dp', 'sp', None)

    def device_step(image_tokens, ln1_gain, ln1_shift, w_qkv, b_qkv, w_out, b_out, ln2_gain, ln2_shift, w_up, b_up, w_down, b_down):
        layers = w_qkv.shape[0]
        w_t = w_qkv.transpose(0, 2, 3, 4, 1).reshape(layers, 3 * D, D)
        b_t = jnp.broadcast_to(b_qkv.reshape(layers, 3 * D, 1), (layers, 3 * D, 128))
        w_o = w_out.reshape(layers, D, D)
        hidden = lax.all_to_all(image_tokens, 'sp', 0, 1, tiled=True)
        shape = hidden.shape
        h = hidden.reshape(-1, D)
        for l in range(layers):
            row = lambda a: a[l].reshape(1, -1)
            q, k, v, nq2, nk2 = qkv(h, row(ln1_gain), row(ln1_shift), w_t, b_t[l], l)
            o = attn(q, k, v, nq2, nk2)
            h = mlp(h, o, w_o, row(b_out), row(ln2_gain), row(ln2_shift), w_up, row(b_up), w_down, row(b_down), l)
        return lax.all_to_all(h.reshape(shape), 'sp', 1, 0, tiled=True)

    return jax.shard_map(device_step, mesh=mesh, in_specs=(token_spec,) + (P(),) * 12, out_specs=token_spec, check_vma=False)
```

```python
import functools

import jax
import jax.numpy as jnp
from jax import lax
from jax.experimental import pallas as pl
from jax.experimental.pallas import tpu as pltpu
from jax.sharding import PartitionSpec as P

LN_EPS = 1e-6
HD = 96
HEADS = 16
D = HD * HEADS
F = 4 * D
IMAGES = 4
BLK = 256
SEQ = 4 * BLK
T = IMAGES * SEQ
CH = 4 * HD
C = HD ** -0.5 * 1.4426950408889634
LOW = 2.0 ** -80
VMEM_MAX = 67043328
f32, bf16 = jnp.float32, jnp.bfloat16
MESH = pl.DeviceIdType.MESH
HBM = pl.BlockSpec(memory_space=pltpu.HBM)


def dot(a, b):
    return jnp.dot(a, b, preferred_element_type=f32)


def dot_nt(a, b):
    return lax.dot_general(a, b, (((1,), (1,)), ((), ())), preferred_element_type=f32)


def dot_tn(a, b):
    return lax.dot_general(a, b, (((0,), (0,)), ((), ())), preferred_element_type=f32)


def row(n):
    return pl.BlockSpec((1, n), lambda *_: (0, 0))


def ln_rows(load, store, gain, shift, start, rows, step=16):
    for r in range(start, start + rows, step):
        v = load(r, step).astype(f32)
        mu = jnp.sum(v, axis=-1, keepdims=True) * (1.0 / D)
        c = v - mu
        var = jnp.sum(c * c, axis=-1, keepdims=True) * (1.0 / D)
        store(r, step, (c * lax.rsqrt(var + LN_EPS) * gain + shift).astype(bf16))


def qkv_kernel(*refs, layer, n, copy_h, alias):
    (_, xa, xb, xan, xbn, g_ref, s_ref, w_hbm, b_ref), refs = refs[:9], refs[9:]
    refs = refs[alias:]
    (q_ref, k_ref, v_ref, nq_ref, nk_ref), refs = refs[:5], refs[5:]
    if copy_h:
        h_ref, refs = refs[0], refs[1:]
    w, n_s, n_next, sem = refs
    i = pl.program_id(0)
    tm = 2 * BLK
    per = D // CH
    order = (1, 0, 2)
    gain, shift = g_ref[...], s_ref[...]

    def w_rows(o, c):
        return order[o] * D + c * CH

    def w_copy(o, c):
        r = pl.ds(w_rows(o, c), CH)
        return pltpu.make_async_copy(w_hbm.at[layer, r], w.at[r], sem.at[o * per + c])

    def norm(a, b, dst, start, rows):
        def load(r, m):
            return a[0, r:r + m, :] if r < BLK else b[0, r - BLK:r - BLK + m, :]
        def store(r, m, v):
            dst[r:r + m, :] = v
        ln_rows(load, store, gain, shift, start, rows)

    def project(o, c):
        t = order[o]
        if isinstance(c, int):
            r0, rw = c * CH, t * D + c * CH
        else:
            r0, rw = pl.multiple_of(c * CH, CH), pl.multiple_of(t * D + c * CH, CH)
        y = dot_nt(w[pl.ds(rw, CH), :], n_s[...])
        bias = jnp.concatenate([b_ref[pl.ds(rw, CH), :]] * (tm // 128), axis=1)
        yb = (y + bias).astype(bf16)
        if t == 2:
            v_ref[pl.ds(r0, CH), :] = yb
            return
        if t == 0:
            q_ref[pl.ds(r0, CH), :] = yb
        for h in range(CH // HD):
            hh = c * (CH // HD) + h
            yh = yb[h * HD:(h + 1) * HD, :]
            yf = yh.astype(f32)
            nn = jnp.sum(yf * yf, axis=0, keepdims=True)
            if t == 0:
                nq_ref[pl.ds(hh, 1), :] = nn
            else:
                nk_ref[pl.ds(hh, 1), :] = nn
                one = (lax.broadcasted_iota(jnp.int32, (128 - HD, tm), 0) == 0).astype(f32).astype(bf16)
                k_ref[hh] = jnp.concatenate([yh, one], axis=0).T

    def keep():
        if copy_h:
            h_ref[:BLK, :] = xa[0]
            h_ref[BLK:, :] = xb[0]

    @pl.when(i == 0)
    def _():
        for o in range(3):
            for c in range(per):
                w_copy(o, c).start()
        norm(xa, xb, n_s, 0, tm)
        for o in range(3):
            def step(c, carry):
                w_copy(o, c).wait()
                project(o, c)
                return carry
            lax.fori_loop(0, per, step, 0)
        keep()
        if n > 1:
            norm(xan, xbn, n_next, 0, tm)

    if n > 1:
        @pl.when(i > 0)
        def _():
            n_s[...] = n_next[...]
            for o in range(3):
                for c in range(per):
                    project(o, c)
                    m = o * per + c - 2
                    if 0 <= m < 8:
                        norm(xan, xbn, n_next, m * (tm // 8), tm // 8)
            keep()


def qkv(me, xa, xa_map, xb, xb_map, g, s, wt, b, layer, n, out_block, copy_h, into=None, after=None):
    tm = 2 * BLK
    last = n - 1
    piece = lambda f, d: pl.BlockSpec((1, BLK, D), lambda i, m: (f(jnp.minimum(i + d, last), m), 0, 0))
    col = lambda r: pl.BlockSpec((r, tm), lambda i, m: (0, out_block(i)))
    sd = jax.ShapeDtypeStruct
    shapes = [sd((D, T), bf16), sd((HEADS, T, 128), bf16), sd((D, T), bf16), sd((HEADS, T), f32), sd((HEADS, T), f32)]
    specs = [col(D), pl.BlockSpec((HEADS, tm, 128), lambda i, m: (0, out_block(i), 0)), col(D), col(HEADS), col(HEADS)]
    if copy_h:
        shapes.append(sd((T, D), bf16))
        specs.append(pl.BlockSpec((tm, D), lambda i, m: (out_block(i), 0)))
    extra = list(into or ()) + ([after] if after is not None else [])
    return pl.pallas_call(
        functools.partial(qkv_kernel, layer=layer, n=n, copy_h=copy_h, alias=len(extra)),
        out_shape=tuple(shapes),
        grid_spec=pltpu.PrefetchScalarGridSpec(
            num_scalar_prefetch=1, grid=(n,),
            in_specs=[piece(xa_map, 0), piece(xb_map, 0), piece(xa_map, 1), piece(xb_map, 1), row(D), row(D), HBM,
                      pl.BlockSpec((3 * D, 128), lambda *_: (0, 0))] + [HBM] * len(extra),
            out_specs=tuple(specs),
            scratch_shapes=[pltpu.VMEM((3 * D, D), bf16), pltpu.VMEM((tm, D), bf16), pltpu.VMEM((tm, D), bf16),
                            pltpu.SemaphoreType.DMA((12,))]),
        input_output_aliases={9 + a: a for a in range(len(into or ()))},
        compiler_params=pltpu.CompilerParams(vmem_limit_bytes=VMEM_MAX, dimension_semantics=("arbitrary",)),
        cost_estimate=pl.CostEstimate(flops=2 * n * tm * D * 3 * D, bytes_accessed=3 * D * D * 2 + n * tm * D * 10, transcendentals=0),
        name="qkv",
    )(me, xa, xb, xa, xb, g, s, wt, b, *extra)


def attn_kernel(q_ref, k_ref, v_ref, nq_ref, nk_ref, o_ref, *, hp, nq, kb, lag):
    nk = SEQ // kb
    units = [(h, q, k) for h in range(hp) for q in range(SEQ // nq) for k in range(nk)]
    st, lows, acc, rhs = {}, [], {}, {}

    def rows(h):
        return slice(h * HD, (h + 1) * HD)

    def shift_rows(h, q):
        kmax = jnp.max(nk_ref[0, h:h + 1, :], axis=1, keepdims=True)
        m = jnp.sqrt(nq_ref[0, h:h + 1, q * nq:(q + 1) * nq] * kmax) * (-1.0 - 2.0 ** -7)
        first = lax.broadcasted_iota(jnp.int32, (128 - HD, nq), 0) == 0
        return jnp.where(first, jnp.broadcast_to(m, (128 - HD, nq)), 0.0).astype(bf16)

    def score(u):
        h, q, k = u
        if k == 0:
            rhs[h, q] = jnp.concatenate([q_ref[rows(h), q * nq:(q + 1) * nq], shift_rows(h, q)], axis=0)
        st[u] = dot(k_ref[h, k * kb:(k + 1) * kb, :], rhs[h, q])

    def mix(u):
        h, q, k = u
        p = jnp.exp2(st.pop(u) * C)
        ls = jnp.sum(p.reshape(kb // 8, 8, nq), axis=0)
        pv = dot(v_ref[rows(h), k * kb:(k + 1) * kb], p.astype(bf16))
        if k:
            a, b = acc[h, q]
            ls, pv = a + ls, b + pv
        acc[h, q] = (ls, pv)
        if k == nk - 1:
            a, b = acc.pop((h, q))
            l = jnp.sum(a, axis=0, keepdims=True)
            lows.append(l)
            o_ref[rows(h), q * nq:(q + 1) * nq] = (b * (1.0 / l)).astype(bf16)

    for i in range(len(units) + lag):
        if i < len(units):
            score(units[i])
        if i >= lag:
            mix(units[i - lag])
    low = lows[0]
    for l in lows[1:]:
        low = jnp.minimum(low, l)
    low = jnp.min(low)

    @pl.when(jnp.logical_not(low >= LOW))
    def _():
        qb = 256
        def body(j, c):
            h = lax.div(j, SEQ // qb)
            qs = pl.ds(pl.multiple_of(lax.rem(j, SEQ // qb) * qb, qb), qb)
            r = pl.ds(pl.multiple_of(h * HD, 32), HD)
            s = dot(k_ref[h, :, :HD], q_ref[r, qs])
            m = jnp.max(s, axis=0, keepdims=True)
            p = jnp.exp2((s - m) * C)
            l = jnp.sum(p, axis=0, keepdims=True)
            o_ref[r, qs] = (dot(v_ref[r, :], p.astype(bf16)) / l).astype(bf16)
            return c
        lax.fori_loop(0, hp * (SEQ // qb), body, 0)


def attn(q, k, v, nq2, nk2, first, count, hp=8, nq=512, kb=256, lag=3):
    blk = pl.BlockSpec((hp * HD, SEQ), lambda i, j: (j, first + i))
    nrm = pl.BlockSpec((1, hp, SEQ), lambda i, j: (j, 0, first + i))
    split = lambda a: a.reshape(HEADS // hp, hp, T)
    return pl.pallas_call(
        functools.partial(attn_kernel, hp=hp, nq=nq, kb=kb, lag=lag),
        out_shape=jax.ShapeDtypeStruct((D, count * SEQ), bf16),
        grid=(count, HEADS // hp),
        in_specs=[blk, pl.BlockSpec((hp, SEQ, 128), lambda i, j: (j, first + i, 0)), blk, nrm, nrm],
        out_specs=pl.BlockSpec((hp * HD, SEQ), lambda i, j: (j, i)),
        compiler_params=pltpu.CompilerParams(vmem_limit_bytes=VMEM_MAX, dimension_semantics=("arbitrary", "arbitrary")),
        cost_estimate=pl.CostEstimate(flops=4 * count * SEQ * SEQ * D, bytes_accessed=count * SEQ * D * 9, transcendentals=count * SEQ * SEQ * HEADS),
        name="attn",
    )(q, k, v, split(nq2), split(nk2))


def gelu(u):
    c = 0.7978845608028654
    return (0.5 * u) * (1.0 + jnp.tanh(u * (c + (c * 0.044715) * (u * u))))


def mlp_kernel(*refs, layer, base, n, fc, nc, alias, send):
    (x_hbm, o_hbm, wo_hbm, bo_ref, g_ref, s_ref, wu_hbm, bu_ref, wd_hbm, bd_ref), refs = refs[:10], refs[10:]
    refs = refs[alias:]
    out_ref, refs = refs[0], refs[1:]
    (xb, ob, wo, wu, wd, m_s, n_s, act, acc, xsem, osem, wsem), refs = refs[:12], refs[12:]
    i = pl.program_id(0)
    tm = BLK
    nj = F // fc
    gain, shift, bo = g_ref[...], s_ref[...], bo_ref[...]

    def block(g):
        if not send:
            return g
        p, m = g // IMAGES, g % IMAGES
        return m * 4 + jnp.where(p < 2, p + 2, 3 - p)

    def x_copy(g):
        slot = g % 2
        return pltpu.make_async_copy(x_hbm.at[pl.ds((base + block(g)) * tm, tm)], xb.at[slot], xsem.at[slot])

    def o_copy(g):
        slot = g % 2
        return pltpu.make_async_copy(o_hbm.at[:, pl.ds(pl.multiple_of(block(g) * tm, tm), tm)], ob.at[slot], osem.at[slot])

    wo_copy = pltpu.make_async_copy(wo_hbm.at[layer], wo, wsem.at[0])

    def wu_copy(j):
        cols = pl.ds(pl.multiple_of(j * fc, fc), fc)
        return pltpu.make_async_copy(wu_hbm.at[layer, :, cols], wu.at[:, cols], wsem.at[1 + j])

    def wd_copy(j):
        r = pl.ds(pl.multiple_of(j * fc, fc), fc)
        return pltpu.make_async_copy(wd_hbm.at[layer, r], wd.at[r], wsem.at[1 + nj + j])

    if send:
        out_v, ssem, rsem = refs
        dp, me = lax.axis_index("dp"), lax.axis_index("sp")
        slots = out_v.shape[0]

        def peer(k):
            return jnp.where(k == 1, me + 1 - 2 * (me % 2), jnp.where(k == 2, lax.rem(me + 2, 4), 3 - me))

        def remote(g):
            p, m = g // IMAGES, g % IMAGES
            k = jnp.where(p < 2, p + 2, 3 - p)
            return pltpu.make_async_remote_copy(
                src_ref=out_v.at[g % slots], dst_ref=out_ref.at[me * IMAGES + m], send_sem=ssem.at[g], recv_sem=rsem.at[g],
                device_id=(dp, peer(k)), device_id_type=MESH)

        def local(g):
            m = g % IMAGES
            return pltpu.make_async_copy(out_v.at[g % slots], out_ref.at[me * IMAGES + m], ssem.at[g])

    def put(cs, v):
        if send:
            out_v[i % slots, :, cs] = v
        else:
            out_ref[:, cs] = v

    def cols(c):
        return slice(c * nc, (c + 1) * nc)

    def project(slot):
        for c in range(D // nc):
            y = dot_tn(ob[slot], wo[:, cols(c)])
            m_s[:, cols(c)] = (xb[slot, :, cols(c)].astype(f32) + (y + bo[:, cols(c)])).astype(bf16)

    def norm():
        def store(r, m, v):
            n_s[r:r + m, :] = v
        ln_rows(lambda r, m: m_s[r:r + m, :], store, gain, shift, 0, tm)

    @pl.when(i == 0)
    def _():
        if send:
            barrier = pltpu.get_barrier_semaphore()
            for k in range(1, 4):
                pl.semaphore_signal(barrier, inc=1, device_id=(dp, peer(k)), device_id_type=MESH)
            pl.semaphore_wait(barrier, 3)
        x_copy(0).start()
        o_copy(0).start()
        wo_copy.start()
        for j in range(nj):
            wu_copy(j).start()
            wd_copy(j).start()
            if j == 0 and n > 1:
                x_copy(1).start()
                o_copy(1).start()
        x_copy(0).wait()
        o_copy(0).wait()
        wo_copy.wait()
        project(0)
        if n > 2:
            x_copy(2).start()
            o_copy(2).start()
        norm()
        acc[...] = m_s[...].astype(f32) + bd_ref[...]

        def chunk(j, carry):
            wu_copy(j).wait()
            for c in range(fc // nc):
                f0 = pl.ds(pl.multiple_of(j * fc + c * nc, nc), nc)
                act[0, :, cols(c)] = gelu(dot(n_s[...], wu[:, f0]) + bu_ref[:, f0]).astype(bf16)
            wd_copy(j).wait()
            for c in range(D // nc):
                acc[:, cols(c)] = acc[:, cols(c)] + dot(act[0], wd[pl.ds(pl.multiple_of(j * fc, fc), fc), cols(c)])
            return carry
        lax.fori_loop(0, nj, chunk, 0)
        for c in range(D // nc):
            put(cols(c), acc[:, cols(c)].astype(bf16))
        if n > 1:
            x_copy(1).wait()
            o_copy(1).wait()
            project(1)
            norm()

    def up(j, c):
        f0 = j * fc + c * nc
        act[j % 2, :, cols(c)] = gelu(dot(n_s[...], wu[:, f0:f0 + nc]) + bu_ref[:, f0:f0 + nc]).astype(bf16)

    def down(j, c):
        y = dot(act[j % 2], wd[j * fc:(j + 1) * fc, cols(c)])
        if j == 0:
            acc[:, cols(c)] = (m_s[:, cols(c)].astype(f32) + bd_ref[:, cols(c)]) + y
        elif j < nj - 1:
            acc[:, cols(c)] = acc[:, cols(c)] + y
        else:
            put(cols(c), (acc[:, cols(c)] + y).astype(bf16))

    if n > 1:
        @pl.when(i > 0)
        def _():
            @pl.when(i + 1 < n)
            def _():
                x_copy(i + 1).wait()
                o_copy(i + 1).wait()

            @pl.when(i + 2 < n)
            def _():
                x_copy(i + 2).start()
                o_copy(i + 2).start()

            if send:
                @pl.when(i - 1 < 3 * IMAGES)
                def _():
                    remote(i - 1).start()

                @pl.when(i - 1 >= 3 * IMAGES)
                def _():
                    local(i - 1).start()

                @pl.when(i >= slots)
                def _():
                    remote(i - slots).wait_send()

            for c in range(fc // nc):
                up(0, c)
            for j in range(1, nj):
                for c in range(max(fc, D) // nc):
                    if c < fc // nc:
                        up(j, c)
                    if c < D // nc:
                        down(j - 1, c)
            project((i + 1) % 2)
            for c in range(D // nc):
                down(nj - 1, c)
            norm()

            if send:
                @pl.when(i == n - 1)
                def _():
                    local(n - 1).start()
                    for g in range(n - slots, 3 * IMAGES):
                        remote(g).wait_send()
                    for g in range(3 * IMAGES, n):
                        local(g).wait()
                    for g in range(3 * IMAGES):
                        remote(g).wait_recv()


def mlp(x, o, wo, bo, g, s, wu, bu, wd, bd, layer, first, count, into=None, send=False, fc=1536, nc=512):
    n = count * SEQ // BLK
    base = first * SEQ // BLK
    nj = F // fc
    dma = pltpu.SemaphoreType.DMA
    vm = pltpu.VMEM
    scratch = [vm((2, BLK, D), bf16), vm((2, D, BLK), bf16), vm((D, D), bf16), vm((D, F), bf16), vm((F, D), bf16), vm((BLK, D), bf16),
               vm((BLK, D), bf16), vm((2, BLK, fc), bf16), vm((BLK, D), f32), dma((2,)), dma((2,)), dma((1 + 2 * nj,))]
    params = dict(vmem_limit_bytes=VMEM_MAX, dimension_semantics=("arbitrary",))
    if send:
        scratch += [vm((8, BLK, D), bf16), dma((n,)), dma((3 * IMAGES,))]
        out_shape, out_spec = jax.ShapeDtypeStruct((4 * IMAGES, BLK, D), bf16), HBM
        params.update(collective_id=0, has_side_effects=True)
    else:
        out_shape, out_spec = jax.ShapeDtypeStruct((T, D), bf16), pl.BlockSpec((BLK, D), lambda i: (base + i, 0))
    extra = [] if into is None else [into]
    tok = n * BLK
    return pl.pallas_call(
        functools.partial(mlp_kernel, layer=layer, base=base, n=n, fc=fc, nc=nc, alias=len(extra), send=send),
        out_shape=out_shape,
        grid=(n,),
        in_specs=[HBM, HBM, HBM, row(D), row(D), row(D), HBM, row(F), HBM, row(D)] + [HBM] * len(extra),
        out_specs=out_spec,
        scratch_shapes=scratch,
        input_output_aliases={10: 0} if extra else {},
        compiler_params=pltpu.CompilerParams(**params),
        cost_estimate=pl.CostEstimate(flops=2 * tok * D * (2 * F + D), bytes_accessed=(2 * F + D) * D * 2 + tok * D * 6, transcendentals=tok * F),
        name="mlp",
    )(x, o, wo, bo, g, s, wu, bu, wd, bd, *extra)

def solution(mesh):
    token_spec = P('dp', 'sp', None)

    def device_step(image_tokens, ln1_gain, ln1_shift, w_qkv, b_qkv, w_out, b_out, ln2_gain, ln2_shift, w_up, b_up, w_down, b_down):
        layers = w_qkv.shape[0]
        w_t = w_qkv.transpose(0, 2, 3, 4, 1).reshape(layers, 3 * D, D)
        b_t = jnp.broadcast_to(b_qkv.reshape(layers, 3 * D, 1), (layers, 3 * D, 128))
        w_o = w_out.reshape(layers, D, D)
        me = lax.axis_index('sp')
        me1 = me.reshape(1).astype(jnp.int32)

        def exchange(k, first, count):
            part = lax.dynamic_slice_in_dim(image_tokens, (me ^ k) * IMAGES + first, count)
            return lax.ppermute(part, 'sp', [(s, s ^ k) for s in range(4)])

        near = exchange(1, 0, IMAGES)
        far_a, far_b = exchange(2, 0, 1), exchange(3, 0, 1)
        rest_a, rest_b = exchange(2, 1, IMAGES - 1), exchange(3, 1, IMAGES - 1)

        def args(l):
            r = lambda a: a[l].reshape(1, -1)
            pre = (r(ln1_gain), r(ln1_shift), w_t, b_t[l], l)
            post = (w_o, r(b_out), r(ln2_gain), r(ln2_shift), w_up, r(b_up), w_down, r(b_down), l)
            return pre, post

        pre, post = args(0)
        here = lambda i, m: i
        bufs = qkv(me1, image_tokens, lambda i, m: m[0] * IMAGES + i, near, here, *pre, IMAGES, lambda i: 2 * i, True)
        bufs = qkv(me1, far_a, here, far_b, here, *pre, 1, lambda i: 1, True, into=bufs)
        o = attn(*bufs[:5], 0, 1)
        h = mlp(bufs[5], o, *post, 0, 1)
        bufs = qkv(me1, rest_a, here, rest_b, here, *pre, IMAGES - 1, lambda i: 2 * i + 3, True, into=bufs, after=h)
        o = attn(*bufs[:5], 1, IMAGES - 1)
        h = mlp(bufs[5], o, *post, 1, IMAGES - 1, into=h)
        for l in range(1, layers):
            pre, post = args(l)
            x = h.reshape(4 * IMAGES, BLK, D)
            bufs = qkv(me1, x, lambda i, m: 2 * i, x, lambda i, m: 2 * i + 1, *pre, 2 * IMAGES, lambda i: i, False)
            o = attn(*bufs[:5], 0, IMAGES)
            h = mlp(h, o, *post, 0, IMAGES, send=l == layers - 1)
        return h

    return jax.shard_map(device_step, mesh=mesh, in_specs=(token_spec,) + (P(),) * 12, out_specs=token_spec, check_vma=False)
```

```python
import functools

import jax
import jax.numpy as jnp
from jax import lax
from jax.experimental import pallas as pl
from jax.experimental.pallas import tpu as pltpu
from jax.sharding import PartitionSpec as P

LN_EPS = 1e-6
HD = 96
HEADS = 16
D = HD * HEADS
F = 4 * D
IMAGES = 4
BLK = 256
SEQ = 4 * BLK
T = IMAGES * SEQ
CH = 4 * HD
C = HD ** -0.5 * 1.4426950408889634
LOW = 2.0 ** -80
f32, bf16 = jnp.float32, jnp.bfloat16
MESH = pl.DeviceIdType.MESH
HBM = pl.BlockSpec(memory_space=pltpu.HBM)


def dot(a, b):
    return jnp.dot(a, b, preferred_element_type=f32)


def dot_nt(a, b):
    return lax.dot_general(a, b, (((1,), (1,)), ((), ())), preferred_element_type=f32)


def dot_tn(a, b):
    return lax.dot_general(a, b, (((0,), (0,)), ((), ())), preferred_element_type=f32)


VMEM = pl.BlockSpec(memory_space=pltpu.VMEM)
ATTN_LIMIT = 17 << 20
MLP_LIMIT = 15 << 20


def at_hbm(*arrays):
    return tuple(pltpu.with_memory_space_constraint(a, pltpu.HBM) for a in arrays)


def at_vmem(*arrays):
    return tuple(pltpu.with_memory_space_constraint(a, pltpu.VMEM) for a in arrays)


def whole(shape):
    return pl.BlockSpec(shape, lambda *_: (0,) * len(shape))


def ln_rows(load, store, gain, shift, start, rows, step=16):
    for r in range(start, start + rows, step):
        v = load(r, step).astype(f32)
        mu = jnp.sum(v, axis=-1, keepdims=True) * (1.0 / D)
        c = v - mu
        var = jnp.sum(c * c, axis=-1, keepdims=True) * (1.0 / D)
        store(r, step, (c * lax.rsqrt(var + LN_EPS) * gain + shift).astype(bf16))


def start_kernel(par, a_ref, b_ref, bias_ref, w_hbm, sa_ref, sb_ref, w_out, b0_out, b1_out, sem):
    i = pl.program_id(0)
    w_copy = pltpu.make_async_copy(w_hbm.at[0], w_out, sem)

    @pl.when(i == 0)
    def _():
        w_copy.start()
        for l, out in ((0, b0_out), (1, b1_out)):
            for t in range(3):
                cols = bias_ref[l, t].T
                for h in range(HEADS):
                    r = (t * HEADS + h) * HD
                    out[r:r + HD, :] = jnp.broadcast_to(cols[:, h:h + 1], (HD, 128))

    sa_ref[...] = a_ref[...]
    sb_ref[...] = b_ref[...]

    @pl.when(i == pl.num_programs(0) - 1)
    def _():
        w_copy.wait()


def start(par, tokens, w_t, b_qkv):
    sd = jax.ShapeDtypeStruct
    piece = lambda k: pl.BlockSpec((1, BLK, D), lambda i, p: ((p[0] ^ k) * IMAGES + 1 + i, 0, 0))
    out = pl.BlockSpec((1, BLK, D), lambda i, p: (i, 0, 0))
    part = sd((IMAGES - 1, BLK, D), bf16)
    bias = sd((3 * D, 128), f32)
    return pl.pallas_call(
        start_kernel,
        out_shape=(part, part, pltpu.VMEM((3 * D, D), bf16), bias, bias),
        grid_spec=pltpu.PrefetchScalarGridSpec(
            num_scalar_prefetch=1, grid=(IMAGES - 1,),
            in_specs=[piece(2), piece(3), whole(b_qkv.shape), HBM],
            out_specs=(out, out, VMEM, whole((3 * D, 128)), whole((3 * D, 128))),
            scratch_shapes=[pltpu.SemaphoreType.DMA(())]),
        compiler_params=pltpu.CompilerParams(vmem_limit_bytes=40 << 20, dimension_semantics=("arbitrary",)),
        cost_estimate=pl.CostEstimate(flops=1 << 30, bytes_accessed=30 << 20, transcendentals=0),
        name="start",
    )(par, *at_hbm(tokens, tokens), b_qkv, w_t)


def qkv_kernel(*refs, layer, n, copy_h, alias, fetch):
    (_, xa, xb, xan, xbn, g_ref, s_ref, w, b_ref), refs = refs[:9], refs[9:]
    refs = refs[alias:]
    (q_ref, k_ref, v_ref, nq_ref, nk_ref), refs = refs[:5], refs[5:]
    if copy_h:
        h_ref, refs = refs[0], refs[1:]
    n_s, n_next = refs[:2]
    if fetch:
        w_hbm, w, w_sem = w, refs[2], refs[3]
        w_copy = pltpu.make_async_copy(w_hbm.at[layer], w, w_sem)
    i = pl.program_id(0)
    tm = 2 * BLK
    per = D // CH
    order = (1, 0, 2)
    gain, shift = g_ref[layer:layer + 1, :], s_ref[layer:layer + 1, :]

    def norm(a, b, start, rows):
        def load(r, m):
            return a[0, r:r + m, :] if r < BLK else b[0, r - BLK:r - BLK + m, :]
        def store(r, m, v):
            n_next[r:r + m, :] = v
        ln_rows(load, store, gain, shift, start, rows)

    def project(o, c):
        t = order[o]
        r0, rw = c * CH, t * D + c * CH
        y = dot_nt(w[rw:rw + CH, :], n_s[...])
        bias = jnp.concatenate([b_ref[rw:rw + CH, :]] * (tm // 128), axis=1)
        yb = (y + bias).astype(bf16)
        if t == 2:
            v_ref[r0:r0 + CH, :] = yb
            return
        if t == 0:
            q_ref[r0:r0 + CH, :] = yb
        for h in range(CH // HD):
            hh = c * (CH // HD) + h
            yh = yb[h * HD:(h + 1) * HD, :]
            yf = yh.astype(f32)
            nn = jnp.sum(yf * yf, axis=0, keepdims=True)
            if t == 0:
                nq_ref[hh:hh + 1, :] = nn
            else:
                nk_ref[hh:hh + 1, :] = nn
                one = (lax.broadcasted_iota(jnp.int32, (128 - HD, tm), 0) == 0).astype(f32).astype(bf16)
                k_ref[hh] = jnp.concatenate([yh, one], axis=0).T

    @pl.when(i == 0)
    def _():
        if fetch:
            w_copy.start()
        norm(xa, xb, 0, tm)
        if fetch:
            w_copy.wait()

    n_s[...] = n_next[...]
    for o in range(3):
        for c in range(per):
            project(o, c)
            m = o * per + c - 2
            if n > 1 and 0 <= m < 8:
                norm(xan, xbn, m * (tm // 8), tm // 8)
    if copy_h:
        h_ref[:BLK, :] = xa[0]
        h_ref[BLK:, :] = xb[0]


def qkv(par, xa, xa_map, xb, xb_map, g, s, w, b, layer, n, out_block, copy_h, into=None, after=None):
    tm = 2 * BLK
    last = n - 1
    piece = lambda f, d: pl.BlockSpec((1, BLK, D), lambda i, m: (f(jnp.minimum(i + d, last), m), 0, 0))
    col = lambda r: pl.BlockSpec((r, tm), lambda i, m: (0, out_block(i)))
    shapes = [pltpu.HBM((D, T), bf16), pltpu.HBM((HEADS, T, 128), bf16), pltpu.HBM((D, T), bf16), pltpu.HBM((HEADS, T), f32), pltpu.HBM((HEADS, T), f32)]
    specs = [col(D), pl.BlockSpec((HEADS, tm, 128), lambda i, m: (0, out_block(i), 0)), col(D), col(HEADS), col(HEADS)]
    if copy_h:
        shapes.append(pltpu.HBM((T, D), bf16))
        specs.append(pl.BlockSpec((tm, D), lambda i, m: (out_block(i), 0)))
    extra = list(into or ()) + ([after] if after is not None else [])
    fetch = w.ndim == 3
    return pl.pallas_call(
        functools.partial(qkv_kernel, layer=layer, n=n, copy_h=copy_h, alias=len(extra), fetch=fetch),
        out_shape=tuple(shapes),
        grid_spec=pltpu.PrefetchScalarGridSpec(
            num_scalar_prefetch=1, grid=(n,),
            in_specs=[piece(xa_map, 0), piece(xb_map, 0), piece(xa_map, 1), piece(xb_map, 1), whole((2, D)), whole((2, D)), HBM if fetch else VMEM,
                      whole((3 * D, 128))] + [HBM] * len(extra),
            out_specs=tuple(specs),
            scratch_shapes=[pltpu.VMEM((tm, D), bf16), pltpu.VMEM((tm, D), bf16)]
            + ([pltpu.VMEM((3 * D, D), bf16), pltpu.SemaphoreType.DMA(())] if fetch else [])),
        input_output_aliases={9 + a: a for a in range(len(into or ()))},
        compiler_params=pltpu.CompilerParams(vmem_limit_bytes=48 << 20, dimension_semantics=("arbitrary",)),
        cost_estimate=pl.CostEstimate(flops=2 * n * tm * D * 3 * D, bytes_accessed=n * tm * D * 10, transcendentals=0),
        name="qkv",
    )(par, *at_hbm(xa, xb, xa, xb), *at_hbm(g, s), *(at_hbm(w) if fetch else at_vmem(w)), *at_hbm(b), *extra)


def attn_kernel(q_ref, k_ref, v_ref, nq_ref, nk_ref, wo_hbm, wu_hbm, wd_hbm, o_ref, wb, sem, *, layer, hp, nq, kb, lag):
    step = pl.program_id(0) * pl.num_programs(1) + pl.program_id(1)
    parts = [wo_hbm.at[layer]] + [wu_hbm.at[layer, :, c * D:(c + 1) * D] for c in range(F // D)] + [wd_hbm.at[layer]]
    copies = [pltpu.make_async_copy(p, wb.at[c * D:(c + 1) * D] if c <= F // D else wb.at[(1 + F // D) * D:], sem.at[c]) for c, p in enumerate(parts)]

    @pl.when(step == 0)
    def _():
        for c in copies:
            c.start()

    @pl.when(step == pl.num_programs(0) * pl.num_programs(1) - 1)
    def _():
        for c in copies:
            c.wait()

    nk = SEQ // kb
    units = [(h, q, k) for h in range(hp) for q in range(SEQ // nq) for k in range(nk)]
    st, lows, acc, rhs = {}, [], {}, {}

    def rows(h):
        return slice(h * HD, (h + 1) * HD)

    def shift_rows(h, q):
        kmax = jnp.max(nk_ref[0, h:h + 1, :], axis=1, keepdims=True)
        m = jnp.sqrt(nq_ref[0, h:h + 1, q * nq:(q + 1) * nq] * kmax) * (-1.0 - 2.0 ** -7)
        first = lax.broadcasted_iota(jnp.int32, (128 - HD, nq), 0) == 0
        return jnp.where(first, jnp.broadcast_to(m, (128 - HD, nq)), 0.0).astype(bf16)

    def score(u):
        h, q, k = u
        if k == 0:
            rhs[h, q] = jnp.concatenate([q_ref[rows(h), q * nq:(q + 1) * nq], shift_rows(h, q)], axis=0)
        st[u] = dot(k_ref[h, k * kb:(k + 1) * kb, :], rhs[h, q])

    def mix(u):
        h, q, k = u
        p = jnp.exp2(st.pop(u) * C)
        ls = jnp.sum(p.reshape(kb // 8, 8, nq), axis=0)
        pv = dot(v_ref[rows(h), k * kb:(k + 1) * kb], p.astype(bf16))
        if k:
            a, b = acc[h, q]
            ls, pv = a + ls, b + pv
        acc[h, q] = (ls, pv)
        if k == nk - 1:
            a, b = acc.pop((h, q))
            l = jnp.sum(a, axis=0, keepdims=True)
            lows.append(l)
            o_ref[rows(h), q * nq:(q + 1) * nq] = (b * (1.0 / l)).astype(bf16)

    for i in range(len(units) + lag):
        if i < len(units):
            score(units[i])
        if i >= lag:
            mix(units[i - lag])
    low = lows[0]
    for l in lows[1:]:
        low = jnp.minimum(low, l)
    low = jnp.min(low)

    @pl.when(jnp.logical_not(low >= LOW))
    def _():
        qb = 256
        def body(j, c):
            h = lax.div(j, SEQ // qb)
            qs = pl.ds(pl.multiple_of(lax.rem(j, SEQ // qb) * qb, qb), qb)
            r = pl.ds(pl.multiple_of(h * HD, 32), HD)
            s = dot(k_ref[h, :, :HD], q_ref[r, qs])
            m = jnp.max(s, axis=0, keepdims=True)
            p = jnp.exp2((s - m) * C)
            l = jnp.sum(p, axis=0, keepdims=True)
            o_ref[r, qs] = (dot(v_ref[r, :], p.astype(bf16)) / l).astype(bf16)
            return c
        lax.fori_loop(0, hp * (SEQ // qb), body, 0)


def attn(q, k, v, nq2, nk2, w_o, w_up, w_down, layer, first, count, hp=4, nq=512, kb=256, lag=3):
    blk = pl.BlockSpec((hp * HD, SEQ), lambda i, j: (j, first + i))
    nrm = pl.BlockSpec((1, hp, SEQ), lambda i, j: (j, 0, first + i))
    split = lambda a: a.reshape(HEADS // hp, hp, T)
    return pl.pallas_call(
        functools.partial(attn_kernel, layer=layer, hp=hp, nq=nq, kb=kb, lag=lag),
        out_shape=(pltpu.HBM((D, count * SEQ), bf16), pltpu.VMEM((D + 2 * F, D), bf16)),
        grid=(count, HEADS // hp),
        in_specs=[blk, pl.BlockSpec((hp, SEQ, 128), lambda i, j: (j, first + i, 0)), blk, nrm, nrm, HBM, HBM, HBM],
        out_specs=(pl.BlockSpec((hp * HD, SEQ), lambda i, j: (j, i)), VMEM),
        scratch_shapes=[pltpu.SemaphoreType.DMA((2 + F // D,))],
        compiler_params=pltpu.CompilerParams(vmem_limit_bytes=(ATTN_LIMIT), dimension_semantics=("arbitrary", "arbitrary")),
        cost_estimate=pl.CostEstimate(flops=4 * count * SEQ * SEQ * D, bytes_accessed=count * SEQ * D * 9, transcendentals=count * SEQ * SEQ * HEADS),
        name="attn",
    )(*at_hbm(q, k, v, split(nq2), split(nk2)), w_o, w_up, w_down)


def gelu(u):
    c = 0.7978845608028654
    return (0.5 * u) * (1.0 + jnp.tanh(u * (c + (c * 0.044715) * (u * u))))


def mlp_kernel(*refs, layer, base, n, fc, nc, alias, send, fetch):
    (x_hbm, o_hbm, wb, bo_ref, g_ref, s_ref, bu_ref, bd_ref), refs = refs[:8], refs[8:]
    if fetch is not None:
        wq_hbm, refs = refs[0], refs[1:]
    refs = refs[alias:]
    out_ref, refs = refs[0], refs[1:]
    if fetch is not None:
        wq, refs = refs[0], refs[1:]
    (xb, ob, m_s, n_s, act, acc, xsem, osem, wsem), refs = refs[:9], refs[9:]
    i = pl.program_id(0)
    tm = BLK
    assert fc == D
    nj = F // fc
    one = slice(layer, layer + 1)
    gain, shift, bo = g_ref[one, :], s_ref[one, :], bo_ref[one, :]

    def block(g):
        if not send:
            return g
        p, m = g // IMAGES, g % IMAGES
        return m * 4 + jnp.where(p < 2, p + 2, 3 - p)

    def x_copy(g):
        slot = g % 2
        return pltpu.make_async_copy(x_hbm.at[pl.ds((base + block(g)) * tm, tm)], xb.at[slot], xsem.at[slot])

    def o_copy(g):
        slot = g % 2
        return pltpu.make_async_copy(o_hbm.at[:, pl.ds(pl.multiple_of(block(g) * tm, tm), tm)], ob.at[slot], osem.at[slot])

    if fetch is not None:
        wq_copy = pltpu.make_async_copy(wq_hbm.at[fetch], wq, wsem)

    if send:
        out_v, ssem, rsem = refs
        dp, me = lax.axis_index("dp"), lax.axis_index("sp")
        slots = out_v.shape[0]

        def peer(k):
            return jnp.where(k == 1, me + 1 - 2 * (me % 2), jnp.where(k == 2, lax.rem(me + 2, 4), 3 - me))

        def remote(g):
            p, m = g // IMAGES, g % IMAGES
            k = jnp.where(p < 2, p + 2, 3 - p)
            return pltpu.make_async_remote_copy(
                src_ref=out_v.at[g % slots], dst_ref=out_ref.at[me * IMAGES + m], send_sem=ssem.at[g], recv_sem=rsem.at[g],
                device_id=(dp, peer(k)), device_id_type=MESH)

        def local(g):
            m = g % IMAGES
            return pltpu.make_async_copy(out_v.at[g % slots], out_ref.at[me * IMAGES + m], ssem.at[g])

    def put(cs, v):
        if send:
            out_v[i % slots, :, cs] = v
        else:
            out_ref[:, cs] = v

    def cols(c):
        return slice(c * nc, (c + 1) * nc)

    def project(slot):
        for c in range(D // nc):
            y = dot_tn(ob[slot], wb[:D, cols(c)])
            m_s[:, cols(c)] = (xb[slot, :, cols(c)].astype(f32) + (y + bo[:, cols(c)])).astype(bf16)

    def norm():
        def store(r, m, v):
            n_s[r:r + m, :] = v
        ln_rows(lambda r, m: m_s[r:r + m, :], store, gain, shift, 0, tm)

    @pl.when(i == 0)
    def _():
        x_copy(0).start()
        o_copy(0).start()
        x_copy(1).start()
        o_copy(1).start()
        if fetch is not None:
            wq_copy.start()
        if send:
            barrier = pltpu.get_barrier_semaphore()
            for k in range(1, 4):
                pl.semaphore_signal(barrier, inc=1, device_id=(dp, peer(k)), device_id_type=MESH)
            pl.semaphore_wait(barrier, 3)
        x_copy(0).wait()
        o_copy(0).wait()
        project(0)
        norm()

    @pl.when(i + 1 < n)
    def _():
        x_copy(i + 1).wait()
        o_copy(i + 1).wait()

    @pl.when(i + 2 < n)
    def _():
        x_copy(i + 2).start()
        o_copy(i + 2).start()

    if send:
        @pl.when(jnp.logical_and(i >= 1, i - 1 < 3 * IMAGES))
        def _():
            remote(i - 1).start()

        @pl.when(i - 1 >= 3 * IMAGES)
        def _():
            local(i - 1).start()

        @pl.when(i >= slots)
        def _():
            remote(i - slots).wait_send()

    def up(j, c):
        f0 = j * fc + c * nc
        act[j % 2, :, cols(c)] = gelu(dot(n_s[...], wb[D * (1 + j):D * (2 + j), cols(c)]) + bu_ref[one, f0:f0 + nc]).astype(bf16)

    def down(j, c):
        y = dot(act[j % 2], wb[D + F + j * fc:D + F + (j + 1) * fc, cols(c)])
        if j == 0:
            acc[:, cols(c)] = (m_s[:, cols(c)].astype(f32) + bd_ref[one, cols(c)]) + y
        elif j < nj - 1:
            acc[:, cols(c)] = acc[:, cols(c)] + y
        else:
            put(cols(c), (acc[:, cols(c)] + y).astype(bf16))

    for c in range(fc // nc):
        up(0, c)
    for j in range(1, nj):
        for c in range(max(fc, D) // nc):
            if c < fc // nc:
                up(j, c)
            if c < D // nc:
                down(j - 1, c)
    project((i + 1) % 2)
    for c in range(D // nc):
        down(nj - 1, c)
    norm()

    @pl.when(i == n - 1)
    def _():
        if fetch is not None:
            wq_copy.wait()
        if send:
            local(n - 1).start()
            for g in range(n - slots, 3 * IMAGES):
                remote(g).wait_send()
            for g in range(3 * IMAGES, n):
                local(g).wait()
            for g in range(3 * IMAGES):
                remote(g).wait_recv()


def mlp(x, o, w, bo, g, s, bu, bd, layer, first, count, into=None, send=False, fetch=None, w_t=None, fc=1536, nc=512):
    n = count * SEQ // BLK
    base = first * SEQ // BLK
    dma = pltpu.SemaphoreType.DMA
    vm = pltpu.VMEM
    sd = jax.ShapeDtypeStruct
    scratch = [vm((2, BLK, D), bf16), vm((2, D, BLK), bf16), vm((BLK, D), bf16), vm((BLK, D), bf16), vm((2, BLK, fc), bf16), vm((BLK, D), f32),
               dma((2,)), dma((2,)), dma(())]
    limit = MLP_LIMIT
    params = dict(dimension_semantics=("arbitrary",))
    if send:
        scratch += [vm((8, BLK, D), bf16), dma((n,)), dma((3 * IMAGES,))]
        out_shape, out_spec = [sd((4 * IMAGES, BLK, D), bf16)], [HBM]
        params.update(collective_id=0, has_side_effects=True)
        limit += 6 << 20
    else:
        out_shape, out_spec = [pltpu.HBM((T, D), bf16)], [pl.BlockSpec((BLK, D), lambda i: (base + i, 0))]
    extra = []
    if fetch is not None:
        extra.append(w_t)
        out_shape.append(pltpu.VMEM((3 * D, D), bf16))
        out_spec.append(VMEM)
    if into is not None:
        extra.append(into)
    tok = n * BLK
    return pl.pallas_call(
        functools.partial(mlp_kernel, layer=layer, base=base, n=n, fc=fc, nc=nc, alias=into is not None, send=send, fetch=fetch),
        out_shape=out_shape,
        grid=(n,),
        in_specs=[HBM, HBM, VMEM, whole((2, D)), whole((2, D)), whole((2, D)), whole((2, F)), whole((2, D))] + [HBM] * len(extra),
        out_specs=out_spec,
        scratch_shapes=scratch,
        input_output_aliases={7 + len(extra): 0} if into is not None else {},
        compiler_params=pltpu.CompilerParams(vmem_limit_bytes=limit, **params),
        cost_estimate=pl.CostEstimate(flops=2 * tok * D * (2 * F + D), bytes_accessed=tok * D * 6, transcendentals=tok * F),
        name="mlp",
    )(*at_hbm(x, o), *at_vmem(w), *at_hbm(bo, g, s, bu, bd), *extra)


def solution(mesh):
    token_spec = P('dp', 'sp', None)

    def device_step(image_tokens, ln1_gain, ln1_shift, w_qkv, b_qkv, w_out, b_out, ln2_gain, ln2_shift, w_up, b_up, w_down, b_down):
        layers = w_qkv.shape[0]
        w_t = w_qkv.transpose(0, 2, 3, 4, 1).reshape(layers, 3 * D, D)
        w_o = w_out.reshape(layers, D, D)
        me = lax.axis_index('sp')
        par = me.reshape(1).astype(jnp.int32)

        def exchange(k, part):
            return lax.ppermute(part, 'sp', [(s, s ^ k) for s in range(4)])

        def images(k, first, count):
            return lax.dynamic_slice_in_dim(image_tokens, (me ^ k) * IMAGES + first, count)

        far_a, far_b = exchange(2, images(2, 0, 1)), exchange(3, images(3, 0, 1))
        near = exchange(1, images(1, 0, IMAGES))
        rest_a, rest_b, wq, *bias = start(par, image_tokens, w_t, b_qkv)
        rest_a, rest_b = exchange(2, rest_a), exchange(3, rest_b)

        here = lambda i, m: i
        pre = (ln1_gain, ln1_shift)
        fold = (w_o, w_up, w_down)

        def post(l, o, w, *place, **kw):
            return mlp(x, o, w, b_out, ln2_gain, ln2_shift, b_up, b_down, l, *place, **kw)

        bufs = qkv(par, image_tokens, lambda i, m: m[0] * IMAGES + i, near, here, *pre, wq, bias[0], 0, IMAGES, lambda i: 2 * i, True)
        bufs = qkv(par, far_a, here, far_b, here, *pre, wq, bias[0], 0, 1, lambda i: 1, True, into=bufs)
        x = bufs[5]
        h, = post(0, *attn(*bufs[:5], *fold, 0, 0, 1), 0, 1)
        bufs = qkv(par, rest_a, here, rest_b, here, *pre, w_t, bias[0], 0, IMAGES - 1, lambda i: 2 * i + 3, True, into=bufs, after=h)
        x = bufs[5]
        h, = post(0, *attn(*bufs[:5], *fold, 0, 1, IMAGES - 1), 1, IMAGES - 1, into=h)
        x = h.reshape(4 * IMAGES, BLK, D)
        bufs = qkv(par, x, lambda i, m: 2 * i, x, lambda i, m: 2 * i + 1, *pre, w_t, bias[1], 1, 2 * IMAGES, lambda i: i, False)
        x = h
        return post(1, *attn(*bufs[:5], *fold, 1, 0, IMAGES), 0, IMAGES, send=True)[0]

    return jax.shard_map(device_step, mesh=mesh, in_specs=(token_spec,) + (P(),) * 12, out_specs=token_spec, check_vma=False)
```

```python
import functools

import jax
import jax.numpy as jnp
from jax import lax
from jax.experimental import pallas as pl
from jax.experimental.pallas import tpu as pltpu
from jax.sharding import PartitionSpec as P

LN_EPS = 1e-6
HD = 96
HEADS = 16
D = HD * HEADS
F = 4 * D
IMAGES = 4
BLK = 256
SEQ = 4 * BLK
T = IMAGES * SEQ
CH = 4 * HD
C = HD ** -0.5 * 1.4426950408889634
LOW = 2.0 ** -80
f32, bf16 = jnp.float32, jnp.bfloat16
MESH = pl.DeviceIdType.MESH
HBM = pl.BlockSpec(memory_space=pltpu.HBM)


def dot(a, b):
    return jnp.dot(a, b, preferred_element_type=f32)


def dot_nt(a, b):
    return lax.dot_general(a, b, (((1,), (1,)), ((), ())), preferred_element_type=f32)


def dot_tn(a, b):
    return lax.dot_general(a, b, (((0,), (0,)), ((), ())), preferred_element_type=f32)


VMEM = pl.BlockSpec(memory_space=pltpu.VMEM)
QKV_LIMIT = 50 << 20
LAYER_LIMIT = 23 << 20


def at_hbm(*arrays):
    return tuple(pltpu.with_memory_space_constraint(a, pltpu.HBM) for a in arrays)


def at_vmem(*arrays):
    return tuple(pltpu.with_memory_space_constraint(a, pltpu.VMEM) for a in arrays)


def whole(shape):
    return pl.BlockSpec(shape, lambda *_: (0,) * len(shape))


def ln_rows(load, store, gain, shift, start, rows, step=16):
    for r in range(start, start + rows, step):
        v = load(r, step).astype(f32)
        mu = jnp.sum(v, axis=-1, keepdims=True) * (1.0 / D)
        c = v - mu
        var = jnp.sum(c * c, axis=-1, keepdims=True) * (1.0 / D)
        store(r, step, (c * lax.rsqrt(var + LN_EPS) * gain + shift).astype(bf16))


def start_kernel(tokens, w_hbm, sa, sb, near, w_out, buf, w_sem, in_sem, out_sem, s_sem, r_sem):
    dp, me = lax.axis_index("dp"), lax.axis_index("sp")
    peer = me + 1 - 2 * (me % 2)
    w_copy = pltpu.make_async_copy(w_hbm.at[0], w_out, w_sem)
    swap = pltpu.make_async_remote_copy(
        src_ref=tokens.at[pl.ds(peer * IMAGES, IMAGES)], dst_ref=near, send_sem=s_sem, recv_sem=r_sem, device_id=(dp, peer), device_id_type=MESH)
    far = (lax.rem(me + 2, 4), 3 - me)
    ins = [pltpu.make_async_copy(tokens.at[pl.ds(f * IMAGES + 1, IMAGES - 1)], buf.at[n], in_sem.at[n]) for n, f in enumerate(far)]
    outs = [pltpu.make_async_copy(buf.at[n], out, out_sem.at[n]) for n, out in enumerate((sa, sb))]
    for c in ins:
        c.start()
    w_copy.start()
    barrier = pltpu.get_barrier_semaphore()
    pl.semaphore_signal(barrier, inc=1, device_id=(dp, peer), device_id_type=MESH)
    pl.semaphore_wait(barrier, 1)
    swap.start()
    for i, o in zip(ins, outs):
        i.wait()
        o.start()
    for o in outs:
        o.wait()
    swap.wait()
    w_copy.wait()


def start(tokens, w_t):
    part = pltpu.HBM((IMAGES - 1, BLK, D), bf16)
    dma = pltpu.SemaphoreType.DMA
    return pl.pallas_call(
        start_kernel,
        out_shape=(part, part, pltpu.HBM((IMAGES, BLK, D), bf16), pltpu.VMEM((3 * D, D), bf16)),
        in_specs=[HBM, HBM],
        out_specs=(HBM, HBM, HBM, VMEM),
        scratch_shapes=[pltpu.VMEM((2, IMAGES - 1, BLK, D), bf16), dma(()), dma((2,)), dma((2,)), dma(()), dma(())],
        compiler_params=pltpu.CompilerParams(vmem_limit_bytes=QKV_LIMIT, collective_id=1, has_side_effects=True),
        cost_estimate=pl.CostEstimate(flops=1 << 30, bytes_accessed=30 << 20, transcendentals=0),
        name="start",
    )(*at_hbm(tokens), w_t)


def qkv_kernel(*refs, layer, n, copy_h, alias, fetch):
    (_, xa, xb, xan, xbn, g_ref, s_ref, w, b_ref), refs = refs[:9], refs[9:]
    refs = refs[alias:]
    (q_ref, k_ref, v_ref, nq_ref, nk_ref), refs = refs[:5], refs[5:]
    if copy_h:
        h_ref, refs = refs[0], refs[1:]
    n_s, n_next = refs[:2]
    if fetch:
        w_hbm, w, w_sem = w, refs[2], refs[3]
        w_copy = pltpu.make_async_copy(w_hbm.at[layer], w, w_sem)
    i = pl.program_id(0)
    tm = 2 * BLK
    per = D // CH
    order = (1, 0, 2)
    gain, shift = g_ref[layer:layer + 1, :], s_ref[layer:layer + 1, :]

    def norm(a, b, start, rows):
        def load(r, m):
            return a[0, r:r + m, :] if r < BLK else b[0, r - BLK:r - BLK + m, :]
        def store(r, m, v):
            n_next[r:r + m, :] = v
        ln_rows(load, store, gain, shift, start, rows)

    def project(o, c):
        t = order[o]
        r0, rw = c * CH, t * D + c * CH
        y = dot_nt(w[rw:rw + CH, :], n_s[...])
        heads = range(c * (CH // HD), (c + 1) * (CH // HD))
        bias = b_ref[layer, t].T
        bias = jnp.concatenate([jnp.broadcast_to(bias[:, h:h + 1], (HD, tm)) for h in heads], axis=0)
        yb = (y + bias).astype(bf16)
        if t == 2:
            v_ref[r0:r0 + CH, :] = yb
            return
        if t == 0:
            q_ref[r0:r0 + CH, :] = yb
        for h, hh in enumerate(heads):
            yh = yb[h * HD:(h + 1) * HD, :]
            yf = yh.astype(f32)
            nn = jnp.sum(yf * yf, axis=0, keepdims=True)
            if t == 0:
                nq_ref[hh:hh + 1, :] = nn
            else:
                nk_ref[hh:hh + 1, :] = nn
                one = (lax.broadcasted_iota(jnp.int32, (128 - HD, tm), 0) == 0).astype(f32).astype(bf16)
                k_ref[hh] = jnp.concatenate([yh, one], axis=0).T

    @pl.when(i == 0)
    def _():
        if fetch:
            w_copy.start()
        norm(xa, xb, 0, tm)
        if fetch:
            w_copy.wait()

    n_s[...] = n_next[...]
    for o in range(3):
        for c in range(per):
            project(o, c)
            m = o * per + c - 2
            if n > 1 and 0 <= m < 8:
                norm(xan, xbn, m * (tm // 8), tm // 8)
    if copy_h:
        h_ref[:BLK, :] = xa[0]
        h_ref[BLK:, :] = xb[0]


def qkv(par, xa, xa_map, xb, xb_map, g, s, w, b, layer, n, out_block, copy_h, into=None, after=None):
    tm = 2 * BLK
    last = n - 1
    piece = lambda f, d: pl.BlockSpec((1, BLK, D), lambda i, m: (f(jnp.minimum(i + d, last), m), 0, 0))
    col = lambda r: pl.BlockSpec((r, tm), lambda i, m: (0, out_block(i)))
    shapes = [pltpu.HBM((D, T), bf16), pltpu.HBM((HEADS, T, 128), bf16), pltpu.HBM((D, T), bf16), pltpu.HBM((HEADS, T), f32), pltpu.HBM((HEADS, T), f32)]
    specs = [col(D), pl.BlockSpec((HEADS, tm, 128), lambda i, m: (0, out_block(i), 0)), col(D), col(HEADS), col(HEADS)]
    if copy_h:
        shapes.append(pltpu.HBM((T, D), bf16))
        specs.append(pl.BlockSpec((tm, D), lambda i, m: (out_block(i), 0)))
    extra = list(into or ()) + ([after] if after is not None else [])
    fetch = w.ndim == 3
    return pl.pallas_call(
        functools.partial(qkv_kernel, layer=layer, n=n, copy_h=copy_h, alias=len(extra), fetch=fetch),
        out_shape=tuple(shapes),
        grid_spec=pltpu.PrefetchScalarGridSpec(
            num_scalar_prefetch=1, grid=(n,),
            in_specs=[piece(xa_map, 0), piece(xb_map, 0), piece(xa_map, 1), piece(xb_map, 1), whole((2, D)), whole((2, D)), HBM if fetch else VMEM,
                      whole(b.shape)] + [HBM] * len(extra),
            out_specs=tuple(specs),
            scratch_shapes=[pltpu.VMEM((tm, D), bf16), pltpu.VMEM((tm, D), bf16)]
            + ([pltpu.VMEM((3 * D, D), bf16), pltpu.SemaphoreType.DMA(())] if fetch else [])),
        input_output_aliases={9 + a: a for a in range(len(into or ()))},
        compiler_params=pltpu.CompilerParams(vmem_limit_bytes=63 << 20 if fetch else QKV_LIMIT, dimension_semantics=("arbitrary",)),
        cost_estimate=pl.CostEstimate(flops=2 * n * tm * D * 3 * D, bytes_accessed=n * tm * D * 10, transcendentals=0),
        name="qkv",
    )(par, *at_hbm(xa, xb, xa, xb), *at_hbm(g, s), *(at_hbm(w) if fetch else at_vmem(w)), *at_hbm(b), *extra)


def attn_kernel(q_ref, k_ref, v_ref, nq_ref, nk_ref, wo_hbm, wu_hbm, wd_hbm, o_ref, wb, sem, *, layer, hp, nq, kb, lag):
    step = pl.program_id(0) * pl.num_programs(1) + pl.program_id(1)
    parts = [wo_hbm.at[layer]] + [wu_hbm.at[layer, :, c * D:(c + 1) * D] for c in range(F // D)] + [wd_hbm.at[layer]]
    copies = [pltpu.make_async_copy(p, wb.at[c * D:(c + 1) * D] if c <= F // D else wb.at[(1 + F // D) * D:], sem.at[c]) for c, p in enumerate(parts)]

    @pl.when(step == 0)
    def _():
        for c in copies:
            c.start(priority=1)

    @pl.when(step == pl.num_programs(0) * pl.num_programs(1) - 1)
    def _():
        for c in copies:
            c.wait()

    nk = SEQ // kb
    units = [(h, q, k) for h in range(hp) for q in range(SEQ // nq) for k in range(nk)]
    st, lows, acc, rhs = {}, [], {}, {}

    def rows(h):
        return slice(h * HD, (h + 1) * HD)

    def shift_rows(h, q):
        kmax = jnp.max(nk_ref[h:h + 1, :], axis=1, keepdims=True)
        m = jnp.sqrt(nq_ref[h:h + 1, q * nq:(q + 1) * nq] * kmax) * (-1.0 - 2.0 ** -7)
        first = lax.broadcasted_iota(jnp.int32, (128 - HD, nq), 0) == 0
        return jnp.where(first, jnp.broadcast_to(m, (128 - HD, nq)), 0.0).astype(bf16)

    def score(u):
        h, q, k = u
        if k == 0:
            rhs[h, q] = jnp.concatenate([q_ref[rows(h), q * nq:(q + 1) * nq], shift_rows(h, q)], axis=0)
        st[u] = dot(k_ref[h, k * kb:(k + 1) * kb, :], rhs[h, q])

    def mix(u):
        h, q, k = u
        p = jnp.exp2(st.pop(u) * C)
        ls = jnp.sum(p.reshape(kb // 8, 8, nq), axis=0)
        pv = dot(v_ref[rows(h), k * kb:(k + 1) * kb], p.astype(bf16))
        if k:
            a, b = acc[h, q]
            ls, pv = a + ls, b + pv
        acc[h, q] = (ls, pv)
        if k == nk - 1:
            a, b = acc.pop((h, q))
            l = jnp.sum(a, axis=0, keepdims=True)
            lows.append(l)
            o_ref[rows(h), q * nq:(q + 1) * nq] = (b * (1.0 / l)).astype(bf16)

    for i in range(len(units) + lag):
        if i < len(units):
            score(units[i])
        if i >= lag:
            mix(units[i - lag])
    low = lows[0]
    for l in lows[1:]:
        low = jnp.minimum(low, l)
    low = jnp.min(low)

    @pl.when(jnp.logical_not(low >= LOW))
    def _():
        qb = 256
        def body(j, c):
            h = lax.div(j, SEQ // qb)
            qs = pl.ds(pl.multiple_of(lax.rem(j, SEQ // qb) * qb, qb), qb)
            r = pl.ds(pl.multiple_of(h * HD, 32), HD)
            s = dot(k_ref[h, :, :HD], q_ref[r, qs])
            m = jnp.max(s, axis=0, keepdims=True)
            p = jnp.exp2((s - m) * C)
            l = jnp.sum(p, axis=0, keepdims=True)
            o_ref[r, qs] = (dot(v_ref[r, :], p.astype(bf16)) / l).astype(bf16)
            return c
        lax.fori_loop(0, hp * (SEQ // qb), body, 0)


def attn(q, k, v, nq2, nk2, w_o, w_up, w_down, layer, first, count, hp=8, nq=512, kb=256, lag=3):
    blk = pl.BlockSpec((hp * HD, SEQ), lambda i, j: (j, first + i))
    nrm = pl.BlockSpec((hp, SEQ), lambda i, j: (j, first + i))
    return pl.pallas_call(
        functools.partial(attn_kernel, layer=layer, hp=hp, nq=nq, kb=kb, lag=lag),
        out_shape=(pltpu.HBM((D, count * SEQ), bf16), pltpu.VMEM((D + 2 * F, D), bf16)),
        grid=(count, HEADS // hp),
        in_specs=[blk, pl.BlockSpec((hp, SEQ, 128), lambda i, j: (j, first + i, 0)), blk, nrm, nrm, HBM, HBM, HBM],
        out_specs=(pl.BlockSpec((hp * HD, SEQ), lambda i, j: (j, i)), VMEM),
        scratch_shapes=[pltpu.SemaphoreType.DMA((2 + F // D,))],
        compiler_params=pltpu.CompilerParams(vmem_limit_bytes=LAYER_LIMIT, dimension_semantics=("arbitrary", "arbitrary")),
        cost_estimate=pl.CostEstimate(flops=4 * count * SEQ * SEQ * D, bytes_accessed=count * SEQ * D * 9, transcendentals=count * SEQ * SEQ * HEADS),
        name="attn",
    )(*at_hbm(q, k, v, nq2, nk2), w_o, w_up, w_down)


def gelu(u):
    c = 0.7978845608028654
    return (0.5 * u) * (1.0 + jnp.tanh(u * (c + (c * 0.044715) * (u * u))))


def mlp_kernel(*refs, layer, base, n, fc, nc, alias, send, fetch):
    (x_hbm, o_hbm, wb, bo_ref, g_ref, s_ref, bu_ref, bd_ref), refs = refs[:8], refs[8:]
    if fetch is not None:
        wq_hbm, refs = refs[0], refs[1:]
    refs = refs[alias:]
    out_ref, refs = refs[0], refs[1:]
    if fetch is not None:
        wq, refs = refs[0], refs[1:]
    (xb, ob, m_s, n_s, act, acc, xsem, osem, wsem), refs = refs[:9], refs[9:]
    i = pl.program_id(0)
    tm = BLK
    assert fc == D
    nj = F // fc
    one = slice(layer, layer + 1)
    gain, shift, bo = g_ref[one, :], s_ref[one, :], bo_ref[one, :]

    def block(g):
        if not send:
            return g
        p, m = g // IMAGES, g % IMAGES
        return m * 4 + jnp.where(p < 2, p + 2, 3 - p)

    def x_copy(g):
        slot = g % 2
        return pltpu.make_async_copy(x_hbm.at[pl.ds((base + block(g)) * tm, tm)], xb.at[slot], xsem.at[slot])

    def o_copy(g):
        slot = g % 2
        return pltpu.make_async_copy(o_hbm.at[:, pl.ds(pl.multiple_of(block(g) * tm, tm), tm)], ob.at[slot], osem.at[slot])

    if fetch is not None:
        wq_copy = pltpu.make_async_copy(wq_hbm.at[fetch], wq, wsem)

    if send:
        out_v, ssem, rsem = refs
        dp, me = lax.axis_index("dp"), lax.axis_index("sp")
        slots = out_v.shape[0]

        def peer(k):
            return jnp.where(k == 1, me + 1 - 2 * (me % 2), jnp.where(k == 2, lax.rem(me + 2, 4), 3 - me))

        def remote(g):
            p, m = g // IMAGES, g % IMAGES
            k = jnp.where(p < 2, p + 2, 3 - p)
            return pltpu.make_async_remote_copy(
                src_ref=out_v.at[g % slots], dst_ref=out_ref.at[me * IMAGES + m], send_sem=ssem.at[g], recv_sem=rsem.at[g],
                device_id=(dp, peer(k)), device_id_type=MESH)

        def local(g):
            m = g % IMAGES
            return pltpu.make_async_copy(out_v.at[g % slots], out_ref.at[me * IMAGES + m], ssem.at[g])

    def put(cs, v):
        if send:
            out_v[i % slots, :, cs] = v
        else:
            out_ref[:, cs] = v

    def cols(c):
        return slice(c * nc, (c + 1) * nc)

    def project(slot):
        for c in range(D // nc):
            y = dot_tn(ob[slot], wb[:D, cols(c)])
            m_s[:, cols(c)] = (xb[slot, :, cols(c)].astype(f32) + (y + bo[:, cols(c)])).astype(bf16)

    def norm():
        def store(r, m, v):
            n_s[r:r + m, :] = v
        ln_rows(lambda r, m: m_s[r:r + m, :], store, gain, shift, 0, tm)

    @pl.when(i == 0)
    def _():
        x_copy(0).start()
        o_copy(0).start()
        x_copy(1).start()
        o_copy(1).start()
        if fetch is not None:
            wq_copy.start()
        if send:
            barrier = pltpu.get_barrier_semaphore()
            for k in range(1, 4):
                pl.semaphore_signal(barrier, inc=1, device_id=(dp, peer(k)), device_id_type=MESH)
            pl.semaphore_wait(barrier, 3)
        x_copy(0).wait()
        o_copy(0).wait()
        project(0)
        norm()

    @pl.when(i + 1 < n)
    def _():
        x_copy(i + 1).wait()
        o_copy(i + 1).wait()

    @pl.when(i + 2 < n)
    def _():
        x_copy(i + 2).start()
        o_copy(i + 2).start()

    if send:
        @pl.when(jnp.logical_and(i >= 1, i - 1 < 3 * IMAGES))
        def _():
            remote(i - 1).start()

        @pl.when(i - 1 >= 3 * IMAGES)
        def _():
            local(i - 1).start()

        @pl.when(i >= slots)
        def _():
            remote(i - slots).wait_send()

    def up(j, c):
        f0 = j * fc + c * nc
        act[j % 2, :, cols(c)] = gelu(dot(n_s[...], wb[D * (1 + j):D * (2 + j), cols(c)]) + bu_ref[one, f0:f0 + nc]).astype(bf16)

    def down(j, c):
        y = dot(act[j % 2], wb[D + F + j * fc:D + F + (j + 1) * fc, cols(c)])
        if j == 0:
            acc[:, cols(c)] = (m_s[:, cols(c)].astype(f32) + bd_ref[one, cols(c)]) + y
        elif j < nj - 1:
            acc[:, cols(c)] = acc[:, cols(c)] + y
        else:
            put(cols(c), (acc[:, cols(c)] + y).astype(bf16))

    for c in range(fc // nc):
        up(0, c)
    for j in range(1, nj):
        for c in range(max(fc, D) // nc):
            if c < fc // nc:
                up(j, c)
            if c < D // nc:
                down(j - 1, c)
    project((i + 1) % 2)
    for c in range(D // nc):
        down(nj - 1, c)
    norm()

    @pl.when(i == n - 1)
    def _():
        if fetch is not None:
            wq_copy.wait()
        if send:
            local(n - 1).start()
            for g in range(n - slots, 3 * IMAGES):
                remote(g).wait_send()
            for g in range(3 * IMAGES, n):
                local(g).wait()
            for g in range(3 * IMAGES):
                remote(g).wait_recv()


def mlp(x, o, w, bo, g, s, bu, bd, layer, first, count, into=None, send=False, fetch=None, w_t=None, fc=1536, nc=512):
    n = count * SEQ // BLK
    base = first * SEQ // BLK
    dma = pltpu.SemaphoreType.DMA
    vm = pltpu.VMEM
    sd = jax.ShapeDtypeStruct
    scratch = [vm((2, BLK, D), bf16), vm((2, D, BLK), bf16), vm((BLK, D), bf16), vm((BLK, D), bf16), vm((2, BLK, fc), bf16), vm((BLK, D), f32),
               dma((2,)), dma((2,)), dma(())]
    params = dict(dimension_semantics=("arbitrary",))
    if send:
        scratch += [vm((8, BLK, D), bf16), dma((n,)), dma((3 * IMAGES,))]
        out_shape, out_spec = [sd((4 * IMAGES, BLK, D), bf16)], [HBM]
        params.update(collective_id=0, has_side_effects=True)
    else:
        out_shape, out_spec = [pltpu.HBM((T, D), bf16)], [pl.BlockSpec((BLK, D), lambda i: (base + i, 0))]
    extra = []
    if fetch is not None:
        extra.append(w_t)
        out_shape.append(pltpu.VMEM((3 * D, D), bf16))
        out_spec.append(VMEM)
    if into is not None:
        extra.append(into)
    tok = n * BLK
    return pl.pallas_call(
        functools.partial(mlp_kernel, layer=layer, base=base, n=n, fc=fc, nc=nc, alias=into is not None, send=send, fetch=fetch),
        out_shape=out_shape,
        grid=(n,),
        in_specs=[HBM, HBM, VMEM, whole((2, D)), whole((2, D)), whole((2, D)), whole((2, F)), whole((2, D))] + [HBM] * len(extra),
        out_specs=out_spec,
        scratch_shapes=scratch,
        input_output_aliases={7 + len(extra): 0} if into is not None else {},
        compiler_params=pltpu.CompilerParams(vmem_limit_bytes=LAYER_LIMIT, **params),
        cost_estimate=pl.CostEstimate(flops=2 * tok * D * (2 * F + D), bytes_accessed=tok * D * 6, transcendentals=tok * F),
        name="mlp",
    )(*at_hbm(x, o), *at_vmem(w), *at_hbm(bo, g, s, bu, bd), *extra)


def solution(mesh):
    token_spec = P('dp', 'sp', None)

    def device_step(image_tokens, ln1_gain, ln1_shift, w_qkv, b_qkv, w_out, b_out, ln2_gain, ln2_shift, w_up, b_up, w_down, b_down):
        layers = w_qkv.shape[0]
        w_t = w_qkv.transpose(0, 2, 3, 4, 1).reshape(layers, 3 * D, D)
        w_o = w_out.reshape(layers, D, D)
        me = lax.axis_index('sp')
        par = me.reshape(1).astype(jnp.int32)

        def exchange(k, part):
            return lax.ppermute(part, 'sp', [(s, s ^ k) for s in range(4)])

        def images(k, first, count):
            return lax.dynamic_slice_in_dim(image_tokens, (me ^ k) * IMAGES + first, count)

        far_a, far_b = exchange(2, images(2, 0, 1)), exchange(3, images(3, 0, 1))
        rest_a, rest_b, near, wq = start(image_tokens, w_t)
        rest_a, rest_b = exchange(2, rest_a), exchange(3, rest_b)

        here = lambda i, m: i
        pre = (ln1_gain, ln1_shift)
        fold = (w_o, w_up, w_down)

        def post(l, o, w, *place, **kw):
            return mlp(x, o, w, b_out, ln2_gain, ln2_shift, b_up, b_down, l, *place, **kw)

        bufs = qkv(par, image_tokens, lambda i, m: m[0] * IMAGES + i, near, here, *pre, wq, b_qkv, 0, IMAGES, lambda i: 2 * i, True)
        bufs = qkv(par, far_a, here, far_b, here, *pre, wq, b_qkv, 0, 1, lambda i: 1, True, into=bufs)
        x = bufs[5]
        h, = post(0, *attn(*bufs[:5], *fold, 0, 0, 1), 0, 1)
        bufs = qkv(par, rest_a, here, rest_b, here, *pre, w_t, b_qkv, 0, IMAGES - 1, lambda i: 2 * i + 3, True, into=bufs, after=h)
        x = bufs[5]
        h, = post(0, *attn(*bufs[:5], *fold, 0, 1, IMAGES - 1), 1, IMAGES - 1, into=h)
        x = h.reshape(4 * IMAGES, BLK, D)
        bufs = qkv(par, x, lambda i, m: 2 * i, x, lambda i, m: 2 * i + 1, *pre, w_t, b_qkv, 1, 2 * IMAGES, lambda i: i, False)
        x = h
        return post(1, *attn(*bufs[:5], *fold, 1, 0, IMAGES), 0, IMAGES, send=True)[0]

    return jax.shard_map(device_step, mesh=mesh, in_specs=(token_spec,) + (P(),) * 12, out_specs=token_spec, check_vma=False)
```

```python
import functools

import jax
import jax.numpy as jnp
from jax import lax
from jax.experimental import pallas as pl
from jax.experimental.pallas import tpu as pltpu
from jax.sharding import PartitionSpec as P

LN_EPS = 1e-6
HD = 96
HEADS = 16
D = HD * HEADS
F = 4 * D
IMAGES = 4
BLK = 256
SEQ = 4 * BLK
T = IMAGES * SEQ
CH = 4 * HD
C = HD ** -0.5 * 1.4426950408889634
LOW = 2.0 ** -80
f32, bf16 = jnp.float32, jnp.bfloat16
MESH = pl.DeviceIdType.MESH
HBM = pl.BlockSpec(memory_space=pltpu.HBM)


def dot(a, b):
    return jnp.dot(a, b, preferred_element_type=f32)


def dot_nt(a, b):
    return lax.dot_general(a, b, (((1,), (1,)), ((), ())), preferred_element_type=f32)


def dot_tn(a, b):
    return lax.dot_general(a, b, (((0,), (0,)), ((), ())), preferred_element_type=f32)


VMEM = pl.BlockSpec(memory_space=pltpu.VMEM)
QKV_LIMIT = 50 << 20
LAYER_LIMIT = 23 << 20


def at_hbm(*arrays):
    return tuple(pltpu.with_memory_space_constraint(a, pltpu.HBM) for a in arrays)


def at_vmem(*arrays):
    return tuple(pltpu.with_memory_space_constraint(a, pltpu.VMEM) for a in arrays)


def whole(shape):
    return pl.BlockSpec(shape, lambda *_: (0,) * len(shape))


def ln_rows(load, store, gain, shift, start, rows, step=16):
    for r in range(start, start + rows, step):
        v = load(r, step).astype(f32)
        mu = jnp.sum(v, axis=-1, keepdims=True) * (1.0 / D)
        c = v - mu
        var = jnp.sum(c * c, axis=-1, keepdims=True) * (1.0 / D)
        store(r, step, (c * lax.rsqrt(var + LN_EPS) * gain + shift).astype(bf16))


def start_kernel(tokens, sa, sb, near, buf, in_sem, out_sem, s_sem, r_sem):
    dp, me = lax.axis_index("dp"), lax.axis_index("sp")
    peer = me + 1 - 2 * (me % 2)
    swap = pltpu.make_async_remote_copy(
        src_ref=tokens.at[pl.ds(peer * IMAGES, IMAGES)], dst_ref=near, send_sem=s_sem, recv_sem=r_sem, device_id=(dp, peer), device_id_type=MESH)
    far = (lax.rem(me + 2, 4), 3 - me)
    ins = [pltpu.make_async_copy(tokens.at[pl.ds(f * IMAGES + 1, IMAGES - 1)], buf.at[n], in_sem.at[n]) for n, f in enumerate(far)]
    outs = [pltpu.make_async_copy(buf.at[n], out, out_sem.at[n]) for n, out in enumerate((sa, sb))]
    for c in ins:
        c.start()
    barrier = pltpu.get_barrier_semaphore()
    pl.semaphore_signal(barrier, inc=1, device_id=(dp, peer), device_id_type=MESH)
    pl.semaphore_wait(barrier, 1)
    swap.start()
    for i, o in zip(ins, outs):
        i.wait()
        o.start()
    for o in outs:
        o.wait()
    swap.wait()


def start(tokens):
    part = pltpu.HBM((IMAGES - 1, BLK, D), bf16)
    dma = pltpu.SemaphoreType.DMA
    return pl.pallas_call(
        start_kernel,
        out_shape=(part, part, pltpu.HBM((IMAGES, BLK, D), bf16)),
        in_specs=[HBM],
        out_specs=(HBM, HBM, HBM),
        scratch_shapes=[pltpu.VMEM((2, IMAGES - 1, BLK, D), bf16), dma((2,)), dma((2,)), dma(()), dma(())],
        compiler_params=pltpu.CompilerParams(vmem_limit_bytes=60 << 20, collective_id=1, has_side_effects=True),
        cost_estimate=pl.CostEstimate(flops=1 << 30, bytes_accessed=30 << 20, transcendentals=0),
        name="start",
    )(*at_hbm(tokens))


def qkv_kernel(*refs, layer, n, copy_h, alias, given, hand):
    (_, xa, xb, xan, xbn, g_ref, s_ref, w, b_ref), refs = refs[:9], refs[9:]
    refs = refs[alias:]
    (q_ref, k_ref, v_ref, nq_ref, nk_ref), refs = refs[:5], refs[5:]
    if copy_h:
        h_ref, refs = refs[0], refs[1:]
    if hand:
        w_hbm, w, refs = w, refs[0], refs[1:]
    n_s, n_next, sem = refs[:3]
    if not given and not hand:
        w_hbm, w = w, refs[3]
    i = pl.program_id(0)
    tm = 2 * BLK
    per = D // CH
    order = (1, 0, 2)
    gain, shift = g_ref[layer:layer + 1, :], s_ref[layer:layer + 1, :]
    copies = []
    if not given:
        parts = ((order[0] * D, CH), (order[0] * D + CH, D - CH), (order[1] * D, D), (order[2] * D, D))
        copies = [pltpu.make_async_copy(w_hbm.at[layer, r:r + m], w.at[r:r + m], sem.at[p]) for p, (r, m) in enumerate(parts)]
    def norm(a, b, dst, start, rows):
        def load(r, m):
            return a[0, r:r + m, :] if r < BLK else b[0, r - BLK:r - BLK + m, :]
        def store(r, m, v):
            dst[r:r + m, :] = v
        ln_rows(load, store, gain, shift, start, rows)

    def project(o, c):
        t = order[o]
        r0, rw = c * CH, t * D + c * CH
        y = dot_nt(w[rw:rw + CH, :], n_s[...])
        heads = range(c * (CH // HD), (c + 1) * (CH // HD))
        bias = b_ref[layer, t].T
        bias = jnp.concatenate([jnp.broadcast_to(bias[:, h:h + 1], (HD, tm)) for h in heads], axis=0)
        yb = (y + bias).astype(bf16)
        if t == 2:
            v_ref[r0:r0 + CH, :] = yb
            return
        if t == 0:
            q_ref[r0:r0 + CH, :] = yb
        for h, hh in enumerate(heads):
            yh = yb[h * HD:(h + 1) * HD, :]
            yf = yh.astype(f32)
            nn = jnp.sum(yf * yf, axis=0, keepdims=True)
            if t == 0:
                nq_ref[hh:hh + 1, :] = nn
            else:
                nk_ref[hh:hh + 1, :] = nn
                one = (lax.broadcasted_iota(jnp.int32, (128 - HD, tm), 0) == 0).astype(f32).astype(bf16)
                k_ref[hh] = jnp.concatenate([yh, one], axis=0).T

    def body(first):
        for p in range(3 * per):
            if first and not given and p in (0, 1, per, 2 * per):
                copies[(0, 1, per, 2 * per).index(p)].wait()
            project(p // per, p % per)
            if n > 1 and 0 <= p - 2 < 8:
                norm(xan, xbn, n_next, (p - 2) * (tm // 8), tm // 8)
        if copy_h:
            h_ref[:BLK, :] = xa[0]
            h_ref[BLK:, :] = xb[0]

    @pl.when(i == 0)
    def _():
        for c in copies:
            c.start()
        norm(xa, xb, n_s, 0, tm)
        body(True)

    if n > 1:
        @pl.when(i > 0)
        def _():
            n_s[...] = n_next[...]
            body(False)


def qkv(par, xa, xa_map, xb, xb_map, g, s, w, b, layer, n, out_block, copy_h, into=None, after=None, given=False, hand=False):
    tm = 2 * BLK
    last = n - 1
    piece = lambda f, d: pl.BlockSpec((1, BLK, D), lambda i, m: (f(jnp.minimum(i + d, last), m), 0, 0))
    col = lambda r: pl.BlockSpec((r, tm), lambda i, m: (0, out_block(i)))
    shapes = [pltpu.HBM((D, T), bf16), pltpu.HBM((HEADS, T, 128), bf16), pltpu.HBM((D, T), bf16), pltpu.HBM((HEADS, T), f32), pltpu.HBM((HEADS, T), f32)]
    specs = [col(D), pl.BlockSpec((HEADS, tm, 128), lambda i, m: (0, out_block(i), 0)), col(D), col(HEADS), col(HEADS)]
    if copy_h:
        shapes.append(pltpu.HBM((T, D), bf16))
        specs.append(pl.BlockSpec((tm, D), lambda i, m: (out_block(i), 0)))
    scratch = [pltpu.VMEM((tm, D), bf16), pltpu.VMEM((tm, D), bf16), pltpu.SemaphoreType.DMA((4,))]
    if hand:
        shapes.append(pltpu.VMEM((3 * D, D), bf16))
        specs.append(VMEM)
    elif not given:
        scratch.append(pltpu.VMEM((3 * D, D), bf16))
    into = list(into or ())
    extra = into + ([after] if after is not None else [])
    return pl.pallas_call(
        functools.partial(qkv_kernel, layer=layer, n=n, copy_h=copy_h, alias=len(extra), given=given, hand=hand),
        out_shape=tuple(shapes),
        grid_spec=pltpu.PrefetchScalarGridSpec(
            num_scalar_prefetch=1, grid=(n,),
            in_specs=[piece(xa_map, 0), piece(xb_map, 0), piece(xa_map, 1), piece(xb_map, 1), whole((2, D)), whole((2, D)), VMEM if given else HBM,
                      whole(b.shape)] + [HBM] * len(extra),
            out_specs=tuple(specs),
            scratch_shapes=scratch),
        input_output_aliases={9 + a: a for a in range(len(into))},
        compiler_params=pltpu.CompilerParams(vmem_limit_bytes=QKV_LIMIT if given or hand else 63 << 20, dimension_semantics=("arbitrary",)),
        cost_estimate=pl.CostEstimate(flops=2 * n * tm * D * 3 * D, bytes_accessed=n * tm * D * 10, transcendentals=0),
        name="qkv",
    )(par, *at_hbm(xa, xb, xa, xb, g, s), *(at_vmem(w) if given else at_hbm(w)), *at_hbm(b), *extra)


def attn_kernel(q_ref, k_ref, v_ref, nq_ref, nk_ref, wo_hbm, wu_hbm, wd_hbm, o_ref, wb, sem, *, layer, hp, nq, kb, lag):
    step = pl.program_id(0) * pl.num_programs(1) + pl.program_id(1)
    parts = [wo_hbm.at[layer]] + [wu_hbm.at[layer, :, c * D:(c + 1) * D] for c in range(F // D)] + [wd_hbm.at[layer]]
    copies = [pltpu.make_async_copy(p, wb.at[c * D:(c + 1) * D] if c < len(parts) - 1 else wb.at[c * D:], sem.at[c]) for c, p in enumerate(parts)]

    @pl.when(step == 0)
    def _():
        for c in copies:
            c.start(priority=1)

    @pl.when(step == pl.num_programs(0) * pl.num_programs(1) - 1)
    def _():
        for c in copies:
            c.wait()

    nk = SEQ // kb
    units = [(h, q, k) for h in range(hp) for q in range(SEQ // nq) for k in range(nk)]
    st, lows, acc, rhs = {}, [], {}, {}

    def rows(h):
        return slice(h * HD, (h + 1) * HD)

    def shift_rows(h, q):
        kmax = jnp.max(nk_ref[h:h + 1, :], axis=1, keepdims=True)
        m = jnp.sqrt(nq_ref[h:h + 1, q * nq:(q + 1) * nq] * kmax) * (-1.0 - 2.0 ** -7)
        first = lax.broadcasted_iota(jnp.int32, (128 - HD, nq), 0) == 0
        return jnp.where(first, jnp.broadcast_to(m, (128 - HD, nq)), 0.0).astype(bf16)

    def score(u):
        h, q, k = u
        if k == 0:
            rhs[h, q] = jnp.concatenate([q_ref[rows(h), q * nq:(q + 1) * nq], shift_rows(h, q)], axis=0)
        st[u] = dot(k_ref[h, k * kb:(k + 1) * kb, :], rhs[h, q])

    def mix(u):
        h, q, k = u
        p = jnp.exp2(st.pop(u) * C)
        ls = jnp.sum(p.reshape(kb // 8, 8, nq), axis=0)
        pv = dot(v_ref[rows(h), k * kb:(k + 1) * kb], p.astype(bf16))
        if k:
            a, b = acc[h, q]
            ls, pv = a + ls, b + pv
        acc[h, q] = (ls, pv)
        if k == nk - 1:
            a, b = acc.pop((h, q))
            l = jnp.sum(a, axis=0, keepdims=True)
            lows.append(l)
            o_ref[rows(h), q * nq:(q + 1) * nq] = (b * (1.0 / l)).astype(bf16)

    for i in range(len(units) + lag):
        if i < len(units):
            score(units[i])
        if i >= lag:
            mix(units[i - lag])
    low = lows[0]
    for l in lows[1:]:
        low = jnp.minimum(low, l)
    low = jnp.min(low)

    @pl.when(jnp.logical_not(low >= LOW))
    def _():
        qb = 256
        def body(j, c):
            h = lax.div(j, SEQ // qb)
            qs = pl.ds(pl.multiple_of(lax.rem(j, SEQ // qb) * qb, qb), qb)
            r = pl.ds(pl.multiple_of(h * HD, 32), HD)
            s = dot(k_ref[h, :, :HD], q_ref[r, qs])
            m = jnp.max(s, axis=0, keepdims=True)
            p = jnp.exp2((s - m) * C)
            l = jnp.sum(p, axis=0, keepdims=True)
            o_ref[r, qs] = (dot(v_ref[r, :], p.astype(bf16)) / l).astype(bf16)
            return c
        lax.fori_loop(0, hp * (SEQ // qb), body, 0)


def attn(q, k, v, nq2, nk2, w_o, w_up, w_down, layer, first, count, hp=8, nq=512, kb=256, lag=3):
    blk = pl.BlockSpec((hp * HD, SEQ), lambda i, j: (j, first + i))
    nrm = pl.BlockSpec((hp, SEQ), lambda i, j: (j, first + i))
    return pl.pallas_call(
        functools.partial(attn_kernel, layer=layer, hp=hp, nq=nq, kb=kb, lag=lag),
        out_shape=(pltpu.HBM((D, count * SEQ), bf16), pltpu.VMEM((D + 2 * F, D), bf16)),
        grid=(count, HEADS // hp),
        in_specs=[blk, pl.BlockSpec((hp, SEQ, 128), lambda i, j: (j, first + i, 0)), blk, nrm, nrm, HBM, HBM, HBM],
        out_specs=(pl.BlockSpec((hp * HD, SEQ), lambda i, j: (j, i)), VMEM),
        scratch_shapes=[pltpu.SemaphoreType.DMA((2 + F // D,))],
        compiler_params=pltpu.CompilerParams(vmem_limit_bytes=LAYER_LIMIT, dimension_semantics=("arbitrary", "arbitrary")),
        cost_estimate=pl.CostEstimate(flops=4 * count * SEQ * SEQ * D, bytes_accessed=count * SEQ * D * 9, transcendentals=count * SEQ * SEQ * HEADS),
        name="attn",
    )(*at_hbm(q, k, v, nq2, nk2), w_o, w_up, w_down)


def gelu(u):
    c = 0.7978845608028654
    return (0.5 * u) * (1.0 + jnp.tanh(u * (c + (c * 0.044715) * (u * u))))


def mlp_kernel(*refs, layer, base, n, fc, nc, alias, send):
    (x_hbm, o_hbm, bo_ref, g_ref, s_ref, bu_ref, bd_ref), refs = refs[:7], refs[7:]
    wb, refs = refs[0], refs[1 + alias:]
    out_ref, refs = refs[0], refs[1:]
    (xb, ob, m_s, n_s, act, acc, xsem, osem), refs = refs[:8], refs[8:]

    def w(b, cs):
        return wb[b * D:(b + 1) * D, cs]

    i = pl.program_id(0)
    tm = BLK
    assert fc == D
    nj = F // fc
    one = slice(layer, layer + 1)
    gain, shift, bo = g_ref[one, :], s_ref[one, :], bo_ref[one, :]

    def block(g):
        if not send:
            return g
        p, m = g // IMAGES, g % IMAGES
        return m * 4 + jnp.where(p < 2, p + 2, 3 - p)

    def x_copy(g):
        slot = g % 2
        return pltpu.make_async_copy(x_hbm.at[pl.ds((base + block(g)) * tm, tm)], xb.at[slot], xsem.at[slot])

    def o_copy(g):
        slot = g % 2
        return pltpu.make_async_copy(o_hbm.at[:, pl.ds(pl.multiple_of(block(g) * tm, tm), tm)], ob.at[slot], osem.at[slot])

    if send:
        out_v, ssem, rsem = refs
        dp, me = lax.axis_index("dp"), lax.axis_index("sp")
        slots = out_v.shape[0]

        def peer(k):
            return jnp.where(k == 1, me + 1 - 2 * (me % 2), jnp.where(k == 2, lax.rem(me + 2, 4), 3 - me))

        def remote(g):
            p, m = g // IMAGES, g % IMAGES
            k = jnp.where(p < 2, p + 2, 3 - p)
            return pltpu.make_async_remote_copy(
                src_ref=out_v.at[g % slots], dst_ref=out_ref.at[me * IMAGES + m], send_sem=ssem.at[g], recv_sem=rsem.at[g],
                device_id=(dp, peer(k)), device_id_type=MESH)

        def local(g):
            m = g % IMAGES
            return pltpu.make_async_copy(out_v.at[g % slots], out_ref.at[me * IMAGES + m], ssem.at[g])

    def put(cs, v):
        if send:
            out_v[i % slots, :, cs] = v
        else:
            out_ref[:, cs] = v

    def cols(c):
        return slice(c * nc, (c + 1) * nc)

    def project(slot):
        for c in range(D // nc):
            y = dot_tn(ob[slot], w(0, cols(c)))
            m_s[:, cols(c)] = (xb[slot, :, cols(c)].astype(f32) + (y + bo[:, cols(c)])).astype(bf16)

    def norm():
        def store(r, m, v):
            n_s[r:r + m, :] = v
        ln_rows(lambda r, m: m_s[r:r + m, :], store, gain, shift, 0, tm)

    @pl.when(i == 0)
    def _():
        x_copy(0).start()
        o_copy(0).start()
        x_copy(1).start()
        o_copy(1).start()
        if send:
            barrier = pltpu.get_barrier_semaphore()
            for k in range(1, 4):
                pl.semaphore_signal(barrier, inc=1, device_id=(dp, peer(k)), device_id_type=MESH)
            pl.semaphore_wait(barrier, 3)
        x_copy(0).wait()
        o_copy(0).wait()
        project(0)
        norm()

    @pl.when(i + 1 < n)
    def _():
        x_copy(i + 1).wait()
        o_copy(i + 1).wait()

    @pl.when(i + 2 < n)
    def _():
        x_copy(i + 2).start()
        o_copy(i + 2).start()

    if send:
        @pl.when(jnp.logical_and(i >= 1, i - 1 < 3 * IMAGES))
        def _():
            remote(i - 1).start()

        @pl.when(i - 1 >= 3 * IMAGES)
        def _():
            local(i - 1).start()

        @pl.when(i >= slots)
        def _():
            remote(i - slots).wait_send()

    def up(j, c):
        f0 = j * fc + c * nc
        act[j % 2, :, cols(c)] = gelu(dot(n_s[...], w(1 + j, cols(c))) + bu_ref[one, f0:f0 + nc]).astype(bf16)

    def down(j, c):
        y = dot(act[j % 2], w(1 + nj + j, cols(c)))
        if j == 0:
            acc[:, cols(c)] = (m_s[:, cols(c)].astype(f32) + bd_ref[one, cols(c)]) + y
        elif j < nj - 1:
            acc[:, cols(c)] = acc[:, cols(c)] + y
        else:
            put(cols(c), (acc[:, cols(c)] + y).astype(bf16))

    for c in range(fc // nc):
        up(0, c)
    for j in range(1, nj):
        for c in range(max(fc, D) // nc):
            if c < fc // nc:
                up(j, c)
            if c < D // nc:
                down(j - 1, c)
    project((i + 1) % 2)
    for c in range(D // nc):
        down(nj - 1, c)
    norm()

    if send:
        @pl.when(i == n - 1)
        def _():
            local(n - 1).start()
            for g in range(n - slots, 3 * IMAGES):
                remote(g).wait_send()
            for g in range(3 * IMAGES, n):
                local(g).wait()
            for g in range(3 * IMAGES):
                remote(g).wait_recv()


def mlp(x, o, w, bo, g, s, bu, bd, layer, first, count, into=None, send=False, fc=1536, nc=512):
    n = count * SEQ // BLK
    base = first * SEQ // BLK
    dma = pltpu.SemaphoreType.DMA
    vm = pltpu.VMEM
    scratch = [vm((2, BLK, D), bf16), vm((2, D, BLK), bf16), vm((BLK, D), bf16), vm((BLK, D), bf16), vm((2, BLK, fc), bf16), vm((BLK, D), f32),
               dma((2,)), dma((2,))]
    params = dict(dimension_semantics=("arbitrary",))
    if send:
        scratch += [vm((8, BLK, D), bf16), dma((n,)), dma((3 * IMAGES,))]
        out_shape, out_spec = jax.ShapeDtypeStruct((4 * IMAGES, BLK, D), bf16), HBM
        params.update(collective_id=0, has_side_effects=True)
    else:
        out_shape, out_spec = pltpu.HBM((T, D), bf16), pl.BlockSpec((BLK, D), lambda i: (base + i, 0))
    extra = [] if into is None else [into]
    tok = n * BLK
    return pl.pallas_call(
        functools.partial(mlp_kernel, layer=layer, base=base, n=n, fc=fc, nc=nc, alias=len(extra), send=send),
        out_shape=out_shape,
        grid=(n,),
        in_specs=[HBM, HBM, whole((2, D)), whole((2, D)), whole((2, D)), whole((2, F)), whole((2, D))] + [VMEM] + [HBM] * len(extra),
        out_specs=out_spec,
        scratch_shapes=scratch,
        input_output_aliases={8: 0} if extra else {},
        compiler_params=pltpu.CompilerParams(vmem_limit_bytes=LAYER_LIMIT, **params),
        cost_estimate=pl.CostEstimate(flops=2 * tok * D * (2 * F + D), bytes_accessed=tok * D * 6, transcendentals=tok * F),
        name="mlp",
    )(*at_hbm(x, o, bo, g, s, bu, bd), *at_vmem(w), *extra)


def solution(mesh):
    token_spec = P('dp', 'sp', None)

    def device_step(image_tokens, ln1_gain, ln1_shift, w_qkv, b_qkv, w_out, b_out, ln2_gain, ln2_shift, w_up, b_up, w_down, b_down):
        layers = w_qkv.shape[0]
        w_t = w_qkv.transpose(0, 2, 3, 4, 1).reshape(layers, 3 * D, D)
        w_o = w_out.reshape(layers, D, D)
        me = lax.axis_index('sp')
        par = me.reshape(1).astype(jnp.int32)

        def exchange(k, part):
            return lax.ppermute(part, 'sp', [(s, s ^ k) for s in range(4)])

        def images(k, first, count):
            return lax.dynamic_slice_in_dim(image_tokens, (me ^ k) * IMAGES + first, count)

        far_a, far_b = exchange(2, images(2, 0, 1)), exchange(3, images(3, 0, 1))
        rest_a, rest_b, near = start(image_tokens)
        rest_a, rest_b = exchange(2, rest_a), exchange(3, rest_b)

        here = lambda i, m: i
        pre = (ln1_gain, ln1_shift)
        others = (w_o, w_up, w_down)

        def post(x, l, o, w, *place, **kw):
            return mlp(x, o, w, b_out, ln2_gain, ln2_shift, b_up, b_down, l, *place, **kw)

        *bufs, wq = qkv(par, image_tokens, lambda i, m: m[0] * IMAGES + i, near, here, *pre, w_t, b_qkv, 0, IMAGES, lambda i: 2 * i, True, hand=True)
        bufs = qkv(par, far_a, here, far_b, here, *pre, wq, b_qkv, 0, 1, lambda i: 1, True, into=bufs, given=True)
        o, wb = attn(*bufs[:5], *others, 0, 0, 1)
        h = post(bufs[5], 0, o, wb, 0, 1)
        bufs = qkv(par, rest_a, here, rest_b, here, *pre, w_t, b_qkv, 0, IMAGES - 1, lambda i: 2 * i + 3, True, into=bufs, after=h)
        o, wb = attn(*bufs[:5], *others, 0, 1, IMAGES - 1)
        h = post(bufs[5], 0, o, wb, 1, IMAGES - 1, into=h)
        x = h.reshape(4 * IMAGES, BLK, D)
        bufs = qkv(par, x, lambda i, m: 2 * i, x, lambda i, m: 2 * i + 1, *pre, w_t, b_qkv, 1, 2 * IMAGES, lambda i: i, False)
        o, wb = attn(*bufs[:5], *others, 1, 0, IMAGES)
        return post(h, 1, o, wb, 0, IMAGES, send=True)

    return jax.shard_map(device_step, mesh=mesh, in_specs=(token_spec,) + (P(),) * 12, out_specs=token_spec, check_vma=False)
```

```python
import functools

import jax
import jax.numpy as jnp
from jax import lax
from jax.experimental import pallas as pl
from jax.experimental.pallas import tpu as pltpu
from jax.sharding import PartitionSpec as P

LN_EPS = 1e-6
HD = 96
HEADS = 16
D = HD * HEADS
F = 4 * D
IMAGES = 4
BLK = 256
SEQ = 4 * BLK
T = IMAGES * SEQ
CH = 4 * HD
C = HD ** -0.5 * 1.4426950408889634
LOW = 2.0 ** -80
f32, bf16 = jnp.float32, jnp.bfloat16
MESH = pl.DeviceIdType.MESH
HBM = pl.BlockSpec(memory_space=pltpu.HBM)


def dot(a, b):
    return jnp.dot(a, b, preferred_element_type=f32)


def dot_nt(a, b):
    return lax.dot_general(a, b, (((1,), (1,)), ((), ())), preferred_element_type=f32)


def dot_tn(a, b):
    return lax.dot_general(a, b, (((0,), (0,)), ((), ())), preferred_element_type=f32)


VMEM = pl.BlockSpec(memory_space=pltpu.VMEM)
QKV_LIMIT = 50 << 20
LAYER_LIMIT = 23 << 20
SEND_LIMIT = 18 << 20
SLOTS = 3


def at_hbm(*arrays):
    return tuple(pltpu.with_memory_space_constraint(a, pltpu.HBM) for a in arrays)


def at_vmem(*arrays):
    return tuple(pltpu.with_memory_space_constraint(a, pltpu.VMEM) for a in arrays)


def whole(shape):
    return pl.BlockSpec(shape, lambda *_: (0,) * len(shape))


def ln_rows(load, store, gain, shift, start, rows, step=16):
    for r in range(start, start + rows, step):
        v = load(r, step).astype(f32)
        mu = jnp.sum(v, axis=-1, keepdims=True) * (1.0 / D)
        c = v - mu
        var = jnp.sum(c * c, axis=-1, keepdims=True) * (1.0 / D)
        store(r, step, (c * lax.rsqrt(var + LN_EPS) * gain + shift).astype(bf16))


def start_kernel(tokens, sa, sb, near, buf, in_sem, out_sem, s_sem, r_sem):
    dp, me = lax.axis_index("dp"), lax.axis_index("sp")
    peer = me + 1 - 2 * (me % 2)
    swap = pltpu.make_async_remote_copy(
        src_ref=tokens.at[pl.ds(peer * IMAGES, IMAGES)], dst_ref=near, send_sem=s_sem, recv_sem=r_sem, device_id=(dp, peer), device_id_type=MESH)
    far = (lax.rem(me + 2, 4), 3 - me)
    ins = [pltpu.make_async_copy(tokens.at[pl.ds(f * IMAGES + 1, IMAGES - 1)], buf.at[n], in_sem.at[n]) for n, f in enumerate(far)]
    outs = [pltpu.make_async_copy(buf.at[n], out, out_sem.at[n]) for n, out in enumerate((sa, sb))]
    for c in ins:
        c.start()
    barrier = pltpu.get_barrier_semaphore()
    pl.semaphore_signal(barrier, inc=1, device_id=(dp, peer), device_id_type=MESH)
    pl.semaphore_wait(barrier, 1)
    swap.start()
    for i, o in zip(ins, outs):
        i.wait()
        o.start()
    for o in outs:
        o.wait()
    swap.wait()


def start(tokens):
    part = pltpu.HBM((IMAGES - 1, BLK, D), bf16)
    dma = pltpu.SemaphoreType.DMA
    return pl.pallas_call(
        start_kernel,
        out_shape=(part, part, pltpu.HBM((IMAGES, BLK, D), bf16)),
        in_specs=[HBM],
        out_specs=(HBM, HBM, HBM),
        scratch_shapes=[pltpu.VMEM((2, IMAGES - 1, BLK, D), bf16), dma((2,)), dma((2,)), dma(()), dma(())],
        compiler_params=pltpu.CompilerParams(vmem_limit_bytes=60 << 20, collective_id=1, has_side_effects=True),
        cost_estimate=pl.CostEstimate(flops=1 << 30, bytes_accessed=30 << 20, transcendentals=0),
        name="start",
    )(*at_hbm(tokens))


def qkv_kernel(*refs, layer, n, copy_h, alias, given, hand):
    (_, xa, xb, xan, xbn, g_ref, s_ref, w, b_ref), refs = refs[:9], refs[9:]
    refs = refs[alias:]
    (q_ref, k_ref, v_ref, nq_ref, nk_ref), refs = refs[:5], refs[5:]
    if copy_h:
        h_ref, refs = refs[0], refs[1:]
    if hand:
        w_hbm, w, refs = w, refs[0], refs[1:]
    n_s, n_next, sem = refs[:3]
    if not given and not hand:
        w_hbm, w = w, refs[3]
    i = pl.program_id(0)
    tm = 2 * BLK
    per = D // CH
    order = (1, 0, 2)
    gain, shift = g_ref[layer:layer + 1, :], s_ref[layer:layer + 1, :]
    copies = []
    if not given:
        parts = ((order[0] * D, CH), (order[0] * D + CH, D - CH), (order[1] * D, D), (order[2] * D, D))
        copies = [pltpu.make_async_copy(w_hbm.at[layer, r:r + m], w.at[r:r + m], sem.at[p]) for p, (r, m) in enumerate(parts)]
    def norm(a, b, dst, start, rows):
        def load(r, m):
            return a[0, r:r + m, :] if r < BLK else b[0, r - BLK:r - BLK + m, :]
        def store(r, m, v):
            dst[r:r + m, :] = v
        ln_rows(load, store, gain, shift, start, rows)

    def project(o, c):
        t = order[o]
        r0, rw = c * CH, t * D + c * CH
        y = dot_nt(w[rw:rw + CH, :], n_s[...])
        heads = range(c * (CH // HD), (c + 1) * (CH // HD))
        bias = b_ref[layer, t].T
        bias = jnp.concatenate([jnp.broadcast_to(bias[:, h:h + 1], (HD, tm)) for h in heads], axis=0)
        yb = (y + bias).astype(bf16)
        if t == 2:
            v_ref[r0:r0 + CH, :] = yb
            return
        if t == 0:
            q_ref[r0:r0 + CH, :] = yb
        for h, hh in enumerate(heads):
            yh = yb[h * HD:(h + 1) * HD, :]
            yf = yh.astype(f32)
            nn = jnp.sum(yf * yf, axis=0, keepdims=True)
            if t == 0:
                nq_ref[hh:hh + 1, :] = nn
            else:
                nk_ref[hh:hh + 1, :] = nn
                one = (lax.broadcasted_iota(jnp.int32, (128 - HD, tm), 0) == 0).astype(f32).astype(bf16)
                k_ref[hh] = jnp.concatenate([yh, one], axis=0).T

    def body(first):
        for p in range(3 * per):
            if first and not given and p in (0, 1, per, 2 * per):
                copies[(0, 1, per, 2 * per).index(p)].wait()
            project(p // per, p % per)
            if n > 1 and 0 <= p - 2 < 8:
                norm(xan, xbn, n_next, (p - 2) * (tm // 8), tm // 8)
        if copy_h:
            h_ref[:BLK, :] = xa[0]
            h_ref[BLK:, :] = xb[0]

    @pl.when(i == 0)
    def _():
        for c in copies:
            c.start()
        norm(xa, xb, n_s, 0, tm)
        body(True)

    if n > 1:
        @pl.when(i > 0)
        def _():
            n_s[...] = n_next[...]
            body(False)


def qkv(par, xa, xa_map, xb, xb_map, g, s, w, b, layer, n, out_block, copy_h, into=None, after=None, given=False, hand=False):
    tm = 2 * BLK
    last = n - 1
    piece = lambda f, d: pl.BlockSpec((1, BLK, D), lambda i, m: (f(jnp.minimum(i + d, last), m), 0, 0))
    col = lambda r: pl.BlockSpec((r, tm), lambda i, m: (0, out_block(i)))
    shapes = [pltpu.HBM((D, T), bf16), pltpu.HBM((HEADS, T, 128), bf16), pltpu.HBM((D, T), bf16), pltpu.HBM((HEADS, T), f32), pltpu.HBM((HEADS, T), f32)]
    specs = [col(D), pl.BlockSpec((HEADS, tm, 128), lambda i, m: (0, out_block(i), 0)), col(D), col(HEADS), col(HEADS)]
    if copy_h:
        shapes.append(pltpu.HBM((T, D), bf16))
        specs.append(pl.BlockSpec((tm, D), lambda i, m: (out_block(i), 0)))
    scratch = [pltpu.VMEM((tm, D), bf16), pltpu.VMEM((tm, D), bf16), pltpu.SemaphoreType.DMA((4,))]
    if hand:
        shapes.append(pltpu.VMEM((3 * D, D), bf16))
        specs.append(VMEM)
    elif not given:
        scratch.append(pltpu.VMEM((3 * D, D), bf16))
    into = list(into or ())
    extra = into + ([after] if after is not None else [])
    return pl.pallas_call(
        functools.partial(qkv_kernel, layer=layer, n=n, copy_h=copy_h, alias=len(extra), given=given, hand=hand),
        out_shape=tuple(shapes),
        grid_spec=pltpu.PrefetchScalarGridSpec(
            num_scalar_prefetch=1, grid=(n,),
            in_specs=[piece(xa_map, 0), piece(xb_map, 0), piece(xa_map, 1), piece(xb_map, 1), whole((2, D)), whole((2, D)), VMEM if given else HBM,
                      whole(b.shape)] + [HBM] * len(extra),
            out_specs=tuple(specs),
            scratch_shapes=scratch),
        input_output_aliases={9 + a: a for a in range(len(into))},
        compiler_params=pltpu.CompilerParams(vmem_limit_bytes=QKV_LIMIT if given or hand else 63 << 20, dimension_semantics=("arbitrary",)),
        cost_estimate=pl.CostEstimate(flops=2 * n * tm * D * 3 * D, bytes_accessed=n * tm * D * 10, transcendentals=0),
        name="qkv",
    )(par, *at_hbm(xa, xb, xa, xb, g, s), *(at_vmem(w) if given else at_hbm(w)), *at_hbm(b), *extra)


def attn_kernel(q_ref, k_ref, v_ref, nq_ref, nk_ref, wo_hbm, wu_hbm, wd_hbm, o_ref, wb, sem, *, layer, hp, nq, kb, lag):
    step = pl.program_id(0) * pl.num_programs(1) + pl.program_id(1)
    parts = [wo_hbm.at[layer]] + [wu_hbm.at[layer, :, c * D:(c + 1) * D] for c in range(F // D)] + [wd_hbm.at[layer]]
    copies = [pltpu.make_async_copy(p, wb.at[c * D:(c + 1) * D] if c < len(parts) - 1 else wb.at[c * D:], sem.at[c]) for c, p in enumerate(parts)]

    @pl.when(step == 0)
    def _():
        for c in copies:
            c.start(priority=1)

    @pl.when(step == pl.num_programs(0) * pl.num_programs(1) - 1)
    def _():
        for c in copies:
            c.wait()

    nk = SEQ // kb
    units = [(h, q, k) for h in range(hp) for q in range(SEQ // nq) for k in range(nk)]
    st, lows, acc, rhs = {}, [], {}, {}

    def rows(h):
        return slice(h * HD, (h + 1) * HD)

    def shift_rows(h, q):
        kmax = jnp.max(nk_ref[h:h + 1, :], axis=1, keepdims=True)
        m = jnp.sqrt(nq_ref[h:h + 1, q * nq:(q + 1) * nq] * kmax) * (-1.0 - 2.0 ** -7)
        first = lax.broadcasted_iota(jnp.int32, (128 - HD, nq), 0) == 0
        return jnp.where(first, jnp.broadcast_to(m, (128 - HD, nq)), 0.0).astype(bf16)

    def score(u):
        h, q, k = u
        if k == 0:
            rhs[h, q] = jnp.concatenate([q_ref[rows(h), q * nq:(q + 1) * nq], shift_rows(h, q)], axis=0)
        st[u] = dot(k_ref[h, k * kb:(k + 1) * kb, :], rhs[h, q])

    def mix(u):
        h, q, k = u
        p = jnp.exp2(st.pop(u) * C)
        ls = jnp.sum(p.reshape(kb // 8, 8, nq), axis=0)
        pv = dot(v_ref[rows(h), k * kb:(k + 1) * kb], p.astype(bf16))
        if k:
            a, b = acc[h, q]
            ls, pv = a + ls, b + pv
        acc[h, q] = (ls, pv)
        if k == nk - 1:
            a, b = acc.pop((h, q))
            l = jnp.sum(a, axis=0, keepdims=True)
            lows.append(l)
            o_ref[rows(h), q * nq:(q + 1) * nq] = (b * (1.0 / l)).astype(bf16)

    for i in range(len(units) + lag):
        if i < len(units):
            score(units[i])
        if i >= lag:
            mix(units[i - lag])
    low = lows[0]
    for l in lows[1:]:
        low = jnp.minimum(low, l)
    low = jnp.min(low)

    @pl.when(jnp.logical_not(low >= LOW))
    def _():
        qb = 256
        def body(j, c):
            h = lax.div(j, SEQ // qb)
            qs = pl.ds(pl.multiple_of(lax.rem(j, SEQ // qb) * qb, qb), qb)
            r = pl.ds(pl.multiple_of(h * HD, 32), HD)
            s = dot(k_ref[h, :, :HD], q_ref[r, qs])
            m = jnp.max(s, axis=0, keepdims=True)
            p = jnp.exp2((s - m) * C)
            l = jnp.sum(p, axis=0, keepdims=True)
            o_ref[r, qs] = (dot(v_ref[r, :], p.astype(bf16)) / l).astype(bf16)
            return c
        lax.fori_loop(0, hp * (SEQ // qb), body, 0)


def attn(q, k, v, nq2, nk2, w_o, w_up, w_down, layer, first, count, limit=LAYER_LIMIT, hp=8, nq=512, kb=256, lag=3):
    blk = pl.BlockSpec((hp * HD, SEQ), lambda i, j: (j, first + i))
    nrm = pl.BlockSpec((hp, SEQ), lambda i, j: (j, first + i))
    return pl.pallas_call(
        functools.partial(attn_kernel, layer=layer, hp=hp, nq=nq, kb=kb, lag=lag),
        out_shape=(pltpu.HBM((D, count * SEQ), bf16), pltpu.VMEM((D + 2 * F, D), bf16)),
        grid=(count, HEADS // hp),
        in_specs=[blk, pl.BlockSpec((hp, SEQ, 128), lambda i, j: (j, first + i, 0)), blk, nrm, nrm, HBM, HBM, HBM],
        out_specs=(pl.BlockSpec((hp * HD, SEQ), lambda i, j: (j, i)), VMEM),
        scratch_shapes=[pltpu.SemaphoreType.DMA((2 + F // D,))],
        compiler_params=pltpu.CompilerParams(vmem_limit_bytes=limit, dimension_semantics=("arbitrary", "arbitrary")),
        cost_estimate=pl.CostEstimate(flops=4 * count * SEQ * SEQ * D, bytes_accessed=count * SEQ * D * 9, transcendentals=count * SEQ * SEQ * HEADS),
        name="attn",
    )(*at_hbm(q, k, v, nq2, nk2), w_o, w_up, w_down)


def gelu(u):
    c = 0.7978845608028654
    return (0.5 * u) * (1.0 + jnp.tanh(u * (c + (c * 0.044715) * (u * u))))


def mlp_kernel(*refs, layer, base, n, fc, nc, alias, send):
    (x_hbm, o_hbm, bo_ref, g_ref, s_ref, bu_ref, bd_ref), refs = refs[:7], refs[7:]
    wb, refs = refs[0], refs[1 + alias:]
    out_ref, refs = refs[0], refs[1:]
    if send:
        vbuf, refs = refs[0], refs[1:]
    (xb, ob, m_s, n_s, act, acc, xsem, osem), refs = refs[:8], refs[8:]

    def w(b, cs):
        return wb[b * D:(b + 1) * D, cs]

    i = pl.program_id(0)
    tm = BLK
    assert fc == D
    nj = F // fc
    one = slice(layer, layer + 1)
    gain, shift, bo = g_ref[one, :], s_ref[one, :], bo_ref[one, :]

    away = 3 * IMAGES

    def far(g):
        return g // 3 * 2 + g % 3

    def block(g):
        if not send:
            return g
        f = far(g)
        k = jnp.where(g >= away, 0, jnp.where(g % 3 == 2, 1, 2 + f // IMAGES))
        m = jnp.where(g >= away, g - away, jnp.where(g % 3 == 2, g // 3, f % IMAGES))
        return m * 4 + k

    def x_copy(g):
        slot = g % 2
        return pltpu.make_async_copy(x_hbm.at[pl.ds((base + block(g)) * tm, tm)], xb.at[slot], xsem.at[slot])

    def o_copy(g):
        slot = g % 2
        return pltpu.make_async_copy(o_hbm.at[:, pl.ds(pl.multiple_of(block(g) * tm, tm), tm)], ob.at[slot], osem.at[slot])

    if send:
        ssem, rsem = refs
        dp, me = lax.axis_index("dp"), lax.axis_index("sp")

        def remote(g, dst, peer):
            return pltpu.make_async_remote_copy(
                src_ref=vbuf.at[g % SLOTS], dst_ref=dst, send_sem=ssem.at[g], recv_sem=rsem.at[g], device_id=(dp, peer), device_id_type=MESH)

        def to_far(g):
            return remote(g, out_ref.at[far(g)], jnp.where(far(g) < IMAGES, lax.rem(me + 2, 4), 3 - me))

        def to_near(g):
            return remote(g, out_ref.at[2 * IMAGES + g // 3], me + 1 - 2 * (me % 2))

        slot = jnp.where(i < away, lax.rem(i, SLOTS), SLOTS + i - away)

    def put(cs, v):
        if send:
            vbuf[slot, :, cs] = v
        else:
            out_ref[:, cs] = v

    def cols(c):
        return slice(c * nc, (c + 1) * nc)

    def project(slot):
        for c in range(D // nc):
            y = dot_tn(ob[slot], w(0, cols(c)))
            m_s[:, cols(c)] = (xb[slot, :, cols(c)].astype(f32) + (y + bo[:, cols(c)])).astype(bf16)

    def norm():
        def store(r, m, v):
            n_s[r:r + m, :] = v
        ln_rows(lambda r, m: m_s[r:r + m, :], store, gain, shift, 0, tm)

    @pl.when(i == 0)
    def _():
        x_copy(0).start()
        o_copy(0).start()
        x_copy(1).start()
        o_copy(1).start()
        if send:
            barrier = pltpu.get_barrier_semaphore()
            for peer in (me + 1 - 2 * (me % 2), lax.rem(me + 2, 4), 3 - me):
                pl.semaphore_signal(barrier, inc=1, device_id=(dp, peer), device_id_type=MESH)
            pl.semaphore_wait(barrier, 3)
        x_copy(0).wait()
        o_copy(0).wait()
        project(0)
        norm()

    @pl.when(i + 1 < n)
    def _():
        x_copy(i + 1).wait()
        o_copy(i + 1).wait()

    @pl.when(i + 2 < n)
    def _():
        x_copy(i + 2).start()
        o_copy(i + 2).start()

    if send:
        last = i - 1

        @pl.when(jnp.logical_and(jnp.logical_and(last >= 0, last < away), last % 3 < 2))
        def _():
            to_far(last).start()

        @pl.when(jnp.logical_and(jnp.logical_and(last >= 0, last < away), last % 3 == 2))
        def _():
            to_near(last).start()

        @pl.when(jnp.logical_and(i >= SLOTS, i < away))
        def _():
            to_near(i - SLOTS).wait_send()

    def up(j, c):
        f0 = j * fc + c * nc
        act[j % 2, :, cols(c)] = gelu(dot(n_s[...], w(1 + j, cols(c))) + bu_ref[one, f0:f0 + nc]).astype(bf16)

    def down(j, c):
        y = dot(act[j % 2], w(1 + nj + j, cols(c)))
        if j == 0:
            acc[:, cols(c)] = (m_s[:, cols(c)].astype(f32) + bd_ref[one, cols(c)]) + y
        elif j < nj - 1:
            acc[:, cols(c)] = acc[:, cols(c)] + y
        else:
            put(cols(c), (acc[:, cols(c)] + y).astype(bf16))

    for c in range(fc // nc):
        up(0, c)
    for j in range(1, nj):
        if j == nj - 1:
            project((i + 1) % 2)
        for c in range(D // nc):
            up(j, c)
            down(j - 1, c)
    norm()
    for c in range(D // nc):
        down(nj - 1, c)

    if send:
        @pl.when(i == n - 1)
        def _():
            for g in range(away - SLOTS, away):
                to_near(g).wait_send()
            for g in range(away):
                (to_near if g % 3 == 2 else to_far)(g).wait_recv()


def mlp(x, o, w, bo, g, s, bu, bd, layer, first, count, into=None, send=False, fc=1536, nc=512):
    n = count * SEQ // BLK
    base = first * SEQ // BLK
    dma = pltpu.SemaphoreType.DMA
    vm = pltpu.VMEM
    scratch = [vm((2, BLK, D), bf16), vm((2, D, BLK), bf16), vm((BLK, D), bf16), vm((BLK, D), bf16), vm((2, BLK, fc), bf16), vm((BLK, D), f32),
               dma((2,)), dma((2,))]
    params = dict(dimension_semantics=("arbitrary",))
    if send:
        scratch += [dma((3 * IMAGES,)), dma((3 * IMAGES,))]
        out_shape = (pltpu.HBM((3 * IMAGES, BLK, D), bf16), vm((SLOTS + IMAGES, BLK, D), bf16))
        out_spec = (HBM, VMEM)
        params.update(collective_id=0, has_side_effects=True)
    else:
        out_shape, out_spec = pltpu.HBM((T, D), bf16), pl.BlockSpec((BLK, D), lambda i: (base + i, 0))
    extra = [] if into is None else [into]
    tok = n * BLK
    return pl.pallas_call(
        functools.partial(mlp_kernel, layer=layer, base=base, n=n, fc=fc, nc=nc, alias=len(extra), send=send),
        out_shape=out_shape,
        grid=(n,),
        in_specs=[HBM, HBM, whole((2, D)), whole((2, D)), whole((2, D)), whole((2, F)), whole((2, D))] + [VMEM] + [HBM] * len(extra),
        out_specs=out_spec,
        scratch_shapes=scratch,
        input_output_aliases={8: 0} if extra else {},
        compiler_params=pltpu.CompilerParams(vmem_limit_bytes=SEND_LIMIT if send else LAYER_LIMIT, **params),
        cost_estimate=pl.CostEstimate(flops=2 * tok * D * (2 * F + D), bytes_accessed=tok * D * 6, transcendentals=tok * F),
        name="mlp",
    )(*at_hbm(x, o, bo, g, s, bu, bd), *at_vmem(w), *extra)


def finish_kernel(arrived, vbuf, out, buf, in_sem, via_sem, v_sem):
    me = lax.axis_index("sp")
    copy = pltpu.make_async_copy
    owner = (lax.rem(me + 2, 4), 3 - me, me + 1 - 2 * (me % 2))
    ins = [copy(arrived.at[p * IMAGES:(p + 1) * IMAGES], buf.at[p], in_sem.at[p]) for p in range(3)]
    outs = [copy(buf.at[p], out.at[pl.ds(o * IMAGES, IMAGES)], via_sem.at[p]) for p, o in enumerate(owner)]
    own = copy(vbuf.at[SLOTS:], out.at[pl.ds(me * IMAGES, IMAGES)], v_sem)
    for c in ins:
        c.start()
    own.start()
    for i, o in zip(ins, outs):
        i.wait()
        o.start()
    for c in outs:
        c.wait()
    own.wait()


def finish(arrived, vbuf):
    dma = pltpu.SemaphoreType.DMA
    return pl.pallas_call(
        finish_kernel,
        out_shape=jax.ShapeDtypeStruct((4 * IMAGES, BLK, D), bf16),
        in_specs=[HBM, VMEM],
        out_specs=HBM,
        scratch_shapes=[pltpu.VMEM((3, IMAGES, BLK, D), bf16), dma((3,)), dma((3,)), dma(())],
        compiler_params=pltpu.CompilerParams(vmem_limit_bytes=SEND_LIMIT),
        cost_estimate=pl.CostEstimate(flops=0, bytes_accessed=24 << 20, transcendentals=0),
        name="finish",
    )(*at_hbm(arrived), *at_vmem(vbuf))


def solution(mesh):
    token_spec = P('dp', 'sp', None)

    def device_step(image_tokens, ln1_gain, ln1_shift, w_qkv, b_qkv, w_out, b_out, ln2_gain, ln2_shift, w_up, b_up, w_down, b_down):
        layers = w_qkv.shape[0]
        w_t = w_qkv.transpose(0, 2, 3, 4, 1).reshape(layers, 3 * D, D)
        w_o = w_out.reshape(layers, D, D)
        me = lax.axis_index('sp')
        par = me.reshape(1).astype(jnp.int32)

        def exchange(k, part):
            return lax.ppermute(part, 'sp', [(s, s ^ k) for s in range(4)])

        def images(k, first, count):
            return lax.dynamic_slice_in_dim(image_tokens, (me ^ k) * IMAGES + first, count)

        far_a, far_b = exchange(2, images(2, 0, 1)), exchange(3, images(3, 0, 1))
        rest_a, rest_b, near = start(image_tokens)
        rest_a, rest_b = exchange(2, rest_a), exchange(3, rest_b)

        here = lambda i, m: i
        pre = (ln1_gain, ln1_shift)
        others = (w_o, w_up, w_down)

        def post(x, l, o, w, *place, **kw):
            return mlp(x, o, w, b_out, ln2_gain, ln2_shift, b_up, b_down, l, *place, **kw)

        *bufs, wq = qkv(par, image_tokens, lambda i, m: m[0] * IMAGES + i, near, here, *pre, w_t, b_qkv, 0, IMAGES, lambda i: 2 * i, True, hand=True)
        bufs = qkv(par, far_a, here, far_b, here, *pre, wq, b_qkv, 0, 1, lambda i: 1, True, into=bufs, given=True)
        o, wb = attn(*bufs[:5], *others, 0, 0, 1)
        h = post(bufs[5], 0, o, wb, 0, 1)
        bufs = qkv(par, rest_a, here, rest_b, here, *pre, w_t, b_qkv, 0, IMAGES - 1, lambda i: 2 * i + 3, True, into=bufs, after=h)
        o, wb = attn(*bufs[:5], *others, 0, 1, IMAGES - 1)
        h = post(bufs[5], 0, o, wb, 1, IMAGES - 1, into=h)
        x = h.reshape(4 * IMAGES, BLK, D)
        bufs = qkv(par, x, lambda i, m: 2 * i, x, lambda i, m: 2 * i + 1, *pre, w_t, b_qkv, 1, 2 * IMAGES, lambda i: i, False)
        o, wb = attn(*bufs[:5], *others, 1, 0, IMAGES, limit=SEND_LIMIT)
        return finish(*post(h, 1, o, wb, 0, IMAGES, send=True))

    return jax.shard_map(device_step, mesh=mesh, in_specs=(token_spec,) + (P(),) * 12, out_specs=token_spec, check_vma=False)
```

```python
import functools

import jax
import jax.numpy as jnp
from jax import lax
from jax.experimental import pallas as pl
from jax.experimental.pallas import tpu as pltpu
from jax.sharding import PartitionSpec as P

LN_EPS = 1e-6
HD = 96
HEADS = 16
D = HD * HEADS
F = 4 * D
IMAGES = 4
BLK = 256
SEQ = 4 * BLK
T = IMAGES * SEQ
CH = 4 * HD
C = HD ** -0.5 * 1.4426950408889634
LOW = 2.0 ** -80
f32, bf16 = jnp.float32, jnp.bfloat16
MESH = pl.DeviceIdType.MESH
HBM = pl.BlockSpec(memory_space=pltpu.HBM)


def dot(a, b):
    return jnp.dot(a, b, preferred_element_type=f32)


def dot_nt(a, b):
    return lax.dot_general(a, b, (((1,), (1,)), ((), ())), preferred_element_type=f32)


def dot_tn(a, b):
    return lax.dot_general(a, b, (((0,), (0,)), ((), ())), preferred_element_type=f32)


VMEM = pl.BlockSpec(memory_space=pltpu.VMEM)
QKV_LIMIT = 50 << 20
LAYER_LIMIT = 23 << 20
SEND_LIMIT = 18 << 20
TURNS = 2
SLOTS = 3


def at_hbm(*arrays):
    return tuple(pltpu.with_memory_space_constraint(a, pltpu.HBM) for a in arrays)


def at_vmem(*arrays):
    return tuple(pltpu.with_memory_space_constraint(a, pltpu.VMEM) for a in arrays)


def whole(shape):
    return pl.BlockSpec(shape, lambda *_: (0,) * len(shape))


def ln_rows(load, store, gain, shift, start, rows, step=16):
    for r in range(start, start + rows, step):
        v = load(r, step).astype(f32)
        mu = jnp.sum(v, axis=-1, keepdims=True) * (1.0 / D)
        c = v - mu
        var = jnp.sum(c * c, axis=-1, keepdims=True) * (1.0 / D)
        store(r, step, (c * lax.rsqrt(var + LN_EPS) * gain + shift).astype(bf16))


def start_kernel(tokens, sa, sb, near, buf, in_sem, out_sem, s_sem, r_sem):
    dp, me = lax.axis_index("dp"), lax.axis_index("sp")
    peer = me + 1 - 2 * (me % 2)
    swap = pltpu.make_async_remote_copy(
        src_ref=tokens.at[pl.ds(peer * IMAGES, IMAGES)], dst_ref=near, send_sem=s_sem, recv_sem=r_sem, device_id=(dp, peer), device_id_type=MESH)
    far = (lax.rem(me + 2, 4), 3 - me)
    ins = [pltpu.make_async_copy(tokens.at[pl.ds(f * IMAGES + 1, IMAGES - 1)], buf.at[n], in_sem.at[n]) for n, f in enumerate(far)]
    outs = [pltpu.make_async_copy(buf.at[n], out, out_sem.at[n]) for n, out in enumerate((sa, sb))]
    for c in ins:
        c.start()
    barrier = pltpu.get_barrier_semaphore()
    pl.semaphore_signal(barrier, inc=1, device_id=(dp, peer), device_id_type=MESH)
    pl.semaphore_wait(barrier, 1)
    swap.start()
    for i, o in zip(ins, outs):
        i.wait()
        o.start()
    for o in outs:
        o.wait()
    swap.wait()


def start(tokens):
    part = pltpu.HBM((IMAGES - 1, BLK, D), bf16)
    dma = pltpu.SemaphoreType.DMA
    return pl.pallas_call(
        start_kernel,
        out_shape=(part, part, pltpu.HBM((IMAGES, BLK, D), bf16)),
        in_specs=[HBM],
        out_specs=(HBM, HBM, HBM),
        scratch_shapes=[pltpu.VMEM((2, IMAGES - 1, BLK, D), bf16), dma((2,)), dma((2,)), dma(()), dma(())],
        compiler_params=pltpu.CompilerParams(vmem_limit_bytes=60 << 20, collective_id=1, has_side_effects=True),
        cost_estimate=pl.CostEstimate(flops=1 << 30, bytes_accessed=30 << 20, transcendentals=0),
        name="start",
    )(*at_hbm(tokens))


def qkv_kernel(*refs, layer, n, copy_h, alias, given, hand):
    (_, xa, xb, xan, xbn, g_ref, s_ref, w, b_ref), refs = refs[:9], refs[9:]
    refs = refs[alias:]
    (q_ref, k_ref, v_ref, nq_ref, nk_ref), refs = refs[:5], refs[5:]
    if copy_h:
        h_ref, refs = refs[0], refs[1:]
    if hand:
        w_hbm, w, refs = w, refs[0], refs[1:]
    both, sem = refs[:2]
    if hand:
        ahead = refs[2]
    elif not given:
        w_hbm, w = w, refs[2]
    i = pl.program_id(0)
    tm = 2 * BLK
    per = D // CH
    order = (1, 0, 2)
    gain, shift = g_ref[layer:layer + 1, :], s_ref[layer:layer + 1, :]

    def w_copy(p, t, row, rows):
        r = pl.ds(t * D + row, rows)
        return pltpu.make_async_copy(w_hbm.at[layer, r], w.at[r], sem.at[p])

    def chunk(c, size):
        return c * size if isinstance(c, int) else pl.multiple_of(c * size, size)

    def norm(src, dst, slot, src_row, dst_row):
        def load(r, m):
            return src[0, pl.ds(src_row, m), :]
        def store(r, m, v):
            dst[slot, pl.ds(dst_row, m), :] = v
        ln_rows(load, store, gain, shift, 0, 16)

    def norm_all(a, b, dst, slot):
        for r in range(0, BLK, 16):
            norm(a, dst, slot, r, r)
        for r in range(0, BLK, 16):
            norm(b, dst, slot, r, r + BLK)

    def project(t, c, slot):
        y = dot_nt(w[pl.ds(chunk(c, CH) + t * D, CH), :], both[slot])
        heads = CH // HD
        bias = b_ref[layer, t, pl.ds(chunk(c, heads), heads), :].T
        bias = jnp.concatenate([jnp.broadcast_to(bias[:, h:h + 1], (HD, tm)) for h in range(heads)], axis=0)
        yb = (y + bias).astype(bf16)
        r0 = pl.ds(chunk(c, CH), CH)
        if t == 2:
            v_ref[r0, :] = yb
            return
        if t == 0:
            q_ref[r0, :] = yb
        for h in range(heads):
            yh = yb[h * HD:(h + 1) * HD, :]
            yf = yh.astype(f32)
            nn = jnp.sum(yf * yf, axis=0, keepdims=True)
            if t == 0:
                nq_ref[pl.ds(c * heads + h, 1), :] = nn
            else:
                nk_ref[pl.ds(c * heads + h, 1), :] = nn
                one = (lax.broadcasted_iota(jnp.int32, (128 - HD, tm), 0) == 0).astype(f32).astype(bf16)
                k_ref[c * heads + h] = jnp.concatenate([yh, one], axis=0).T

    def keep():
        if copy_h:
            h_ref[:BLK, :] = xa[0]
            h_ref[BLK:, :] = xb[0]

    if hand:
        copies = lambda part: [w_copy(part * 3 + t, t, part * (D // TURNS), D // TURNS) for t in range(3)]

        @pl.when(i == 0)
        def _():
            for part in range(TURNS):
                for c in copies(part):
                    c.start()
            norm_all(xa, xb, ahead, 0)

        both[0] = ahead[0]

        def turn(part, carry):
            @pl.when(i == 0)
            def _():
                for c in copies(part):
                    c.wait()
            products = [(t, c) for c in range(per // TURNS) for t in order]
            half = BLK // TURNS // 16
            for p, (t, c) in enumerate(products):
                project(t, part * (per // TURNS) + c, 0)
                for g in range(p * 2 * half // len(products), (p + 1) * 2 * half // len(products)):
                    src, base = (xan, 0) if g < half else (xbn, BLK)
                    at = pl.multiple_of(part * (BLK // TURNS) + g % half * 16, 16)
                    norm(src, ahead, 0, at, pl.multiple_of(base + at, 16))
            return carry
        lax.fori_loop(0, TURNS, turn, 0)
        keep()
        return

    parts = {} if given else {0: w_copy(0, order[0], 0, CH), 1: w_copy(1, order[0], CH, D - CH),
                              per: w_copy(2, order[1], 0, D), 2 * per: w_copy(3, order[2], 0, D)}

    def body(first, now, later):
        for p in range(3 * per):
            if first and p in parts:
                parts[p].wait()
            project(order[p // per], p % per, now)
            if n > 1 and 0 <= p - 2 < 8:
                for r in range((p - 2) * (tm // 8), (p - 1) * (tm // 8), 16):
                    norm(xan if r < BLK else xbn, both, later, r % BLK, r)
        keep()

    @pl.when(i == 0)
    def _():
        for c in parts.values():
            c.start()
        norm_all(xa, xb, both, 0)
        body(True, 0, 1)

    if n > 1:
        @pl.when(i > 0)
        def _():
            body(False, lax.rem(i, 2), lax.rem(i + 1, 2))


def qkv(par, xa, xa_map, xb, xb_map, g, s, w, b, layer, n, out_block, copy_h, into=None, after=None, given=False, hand=False):
    tm = 2 * BLK
    last = n - 1
    piece = lambda f, d: pl.BlockSpec((1, BLK, D), lambda i, m: (f(jnp.minimum(i + d, last), m), 0, 0))
    col = lambda r: pl.BlockSpec((r, tm), lambda i, m: (0, out_block(i)))
    shapes = [pltpu.HBM((D, T), bf16), pltpu.HBM((HEADS, T, 128), bf16), pltpu.HBM((D, T), bf16), pltpu.HBM((HEADS, T), f32), pltpu.HBM((HEADS, T), f32)]
    specs = [col(D), pl.BlockSpec((HEADS, tm, 128), lambda i, m: (0, out_block(i), 0)), col(D), col(HEADS), col(HEADS)]
    if copy_h:
        shapes.append(pltpu.HBM((T, D), bf16))
        specs.append(pl.BlockSpec((tm, D), lambda i, m: (out_block(i), 0)))
    scratch = [pltpu.VMEM((1 if hand else 2, tm, D), bf16), pltpu.SemaphoreType.DMA((3 * TURNS if hand else 4,))]
    if hand:
        shapes.append(pltpu.VMEM((3 * D, D), bf16))
        specs.append(VMEM)
        scratch.append(pltpu.VMEM((1, tm, D), bf16))
    elif not given:
        scratch.append(pltpu.VMEM((3 * D, D), bf16))
    into = list(into or ())
    extra = into + ([after] if after is not None else [])
    return pl.pallas_call(
        functools.partial(qkv_kernel, layer=layer, n=n, copy_h=copy_h, alias=len(extra), given=given, hand=hand),
        out_shape=tuple(shapes),
        grid_spec=pltpu.PrefetchScalarGridSpec(
            num_scalar_prefetch=1, grid=(n,),
            in_specs=[piece(xa_map, 0), piece(xb_map, 0), piece(xa_map, 1), piece(xb_map, 1), whole((2, D)), whole((2, D)), VMEM if given else HBM,
                      whole(b.shape)] + [HBM] * len(extra),
            out_specs=tuple(specs),
            scratch_shapes=scratch),
        input_output_aliases={9 + a: a for a in range(len(into))},
        compiler_params=pltpu.CompilerParams(vmem_limit_bytes=QKV_LIMIT if given or hand else 63 << 20, dimension_semantics=("arbitrary",)),
        cost_estimate=pl.CostEstimate(flops=2 * n * tm * D * 3 * D, bytes_accessed=n * tm * D * 10, transcendentals=0),
        name="qkv",
    )(par, *at_hbm(xa, xb, xa, xb, g, s), *(at_vmem(w) if given else at_hbm(w)), *at_hbm(b), *extra)


def attn_kernel(q_ref, k_ref, v_ref, nq_ref, nk_ref, wo_hbm, wu_hbm, wd_hbm, o_ref, wb, sem, *, layer, hp, nq, kb, lag):
    step = pl.program_id(0) * pl.num_programs(1) + pl.program_id(1)
    parts = [wo_hbm.at[layer]] + [wu_hbm.at[layer, :, c * D:(c + 1) * D] for c in range(F // D)] + [wd_hbm.at[layer]]
    copies = [pltpu.make_async_copy(p, wb.at[c * D:(c + 1) * D] if c < len(parts) - 1 else wb.at[c * D:], sem.at[c]) for c, p in enumerate(parts)]

    @pl.when(step == 0)
    def _():
        for c in copies:
            c.start(priority=1)

    @pl.when(step == pl.num_programs(0) * pl.num_programs(1) - 1)
    def _():
        for c in copies:
            c.wait()

    nk = SEQ // kb
    units = [(h, q, k) for h in range(hp) for q in range(SEQ // nq) for k in range(nk)]
    st, lows, acc, rhs = {}, [], {}, {}

    def rows(h):
        return slice(h * HD, (h + 1) * HD)

    def shift_rows(h, q):
        kmax = jnp.max(nk_ref[h:h + 1, :], axis=1, keepdims=True)
        m = jnp.sqrt(nq_ref[h:h + 1, q * nq:(q + 1) * nq] * kmax) * (-1.0 - 2.0 ** -7)
        first = lax.broadcasted_iota(jnp.int32, (128 - HD, nq), 0) == 0
        return jnp.where(first, jnp.broadcast_to(m, (128 - HD, nq)), 0.0).astype(bf16)

    def score(u):
        h, q, k = u
        if k == 0:
            rhs[h, q] = jnp.concatenate([q_ref[rows(h), q * nq:(q + 1) * nq], shift_rows(h, q)], axis=0)
        st[u] = dot(k_ref[h, k * kb:(k + 1) * kb, :], rhs[h, q])

    def mix(u):
        h, q, k = u
        p = jnp.exp2(st.pop(u) * C)
        ls = jnp.sum(p.reshape(kb // 8, 8, nq), axis=0)
        pv = dot(v_ref[rows(h), k * kb:(k + 1) * kb], p.astype(bf16))
        if k:
            a, b = acc[h, q]
            ls, pv = a + ls, b + pv
        acc[h, q] = (ls, pv)
        if k == nk - 1:
            a, b = acc.pop((h, q))
            l = jnp.sum(a, axis=0, keepdims=True)
            lows.append(l)
            o_ref[rows(h), q * nq:(q + 1) * nq] = (b * (1.0 / l)).astype(bf16)

    for i in range(len(units) + lag):
        if i < len(units):
            score(units[i])
        if i >= lag:
            mix(units[i - lag])
    low = lows[0]
    for l in lows[1:]:
        low = jnp.minimum(low, l)
    low = jnp.min(low)

    @pl.when(jnp.logical_not(low >= LOW))
    def _():
        qb = 256
        def body(j, c):
            h = lax.div(j, SEQ // qb)
            qs = pl.ds(pl.multiple_of(lax.rem(j, SEQ // qb) * qb, qb), qb)
            r = pl.ds(pl.multiple_of(h * HD, 32), HD)
            s = dot(k_ref[h, :, :HD], q_ref[r, qs])
            m = jnp.max(s, axis=0, keepdims=True)
            p = jnp.exp2((s - m) * C)
            l = jnp.sum(p, axis=0, keepdims=True)
            o_ref[r, qs] = (dot(v_ref[r, :], p.astype(bf16)) / l).astype(bf16)
            return c
        lax.fori_loop(0, hp * (SEQ // qb), body, 0)


def attn(q, k, v, nq2, nk2, w_o, w_up, w_down, layer, first, count, limit=LAYER_LIMIT, hp=8, nq=512, kb=256, lag=3):
    blk = pl.BlockSpec((hp * HD, SEQ), lambda i, j: (j, first + i))
    nrm = pl.BlockSpec((hp, SEQ), lambda i, j: (j, first + i))
    return pl.pallas_call(
        functools.partial(attn_kernel, layer=layer, hp=hp, nq=nq, kb=kb, lag=lag),
        out_shape=(pltpu.HBM((D, count * SEQ), bf16), pltpu.VMEM((D + 2 * F, D), bf16)),
        grid=(count, HEADS // hp),
        in_specs=[blk, pl.BlockSpec((hp, SEQ, 128), lambda i, j: (j, first + i, 0)), blk, nrm, nrm, HBM, HBM, HBM],
        out_specs=(pl.BlockSpec((hp * HD, SEQ), lambda i, j: (j, i)), VMEM),
        scratch_shapes=[pltpu.SemaphoreType.DMA((2 + F // D,))],
        compiler_params=pltpu.CompilerParams(vmem_limit_bytes=limit, dimension_semantics=("arbitrary", "arbitrary")),
        cost_estimate=pl.CostEstimate(flops=4 * count * SEQ * SEQ * D, bytes_accessed=count * SEQ * D * 9, transcendentals=count * SEQ * SEQ * HEADS),
        name="attn",
    )(*at_hbm(q, k, v, nq2, nk2), w_o, w_up, w_down)


def gelu(u):
    c = 0.7978845608028654
    return (0.5 * u) * (1.0 + jnp.tanh(u * (c + (c * 0.044715) * (u * u))))


def mlp_kernel(*refs, layer, base, n, fc, nc, alias, send):
    (x_hbm, o_hbm, bo_ref, g_ref, s_ref, bu_ref, bd_ref), refs = refs[:7], refs[7:]
    wb, refs = refs[0], refs[1 + alias:]
    out_ref, refs = refs[0], refs[1:]
    if send:
        vbuf, refs = refs[0], refs[1:]
    (xb, ob, m_s, n_s, act, acc, xsem, osem), refs = refs[:8], refs[8:]

    def w(b, cs):
        return wb[b * D:(b + 1) * D, cs]

    i = pl.program_id(0)
    tm = BLK
    assert fc == D
    nj = F // fc
    one = slice(layer, layer + 1)
    gain, shift, bo = g_ref[one, :], s_ref[one, :], bo_ref[one, :]

    away = 3 * IMAGES

    def far(g):
        return g // 3 * 2 + g % 3

    def block(g):
        if not send:
            return g
        f = far(g)
        k = jnp.where(g >= away, 0, jnp.where(g % 3 == 2, 1, 2 + f // IMAGES))
        m = jnp.where(g >= away, g - away, jnp.where(g % 3 == 2, g // 3, f % IMAGES))
        return m * 4 + k

    def x_copy(g):
        slot = g % 2
        return pltpu.make_async_copy(x_hbm.at[pl.ds((base + block(g)) * tm, tm)], xb.at[slot], xsem.at[slot])

    def o_copy(g):
        slot = g % 2
        return pltpu.make_async_copy(o_hbm.at[:, pl.ds(pl.multiple_of(block(g) * tm, tm), tm)], ob.at[slot], osem.at[slot])

    if send:
        ssem, rsem = refs
        dp, me = lax.axis_index("dp"), lax.axis_index("sp")

        def remote(g, dst, peer):
            return pltpu.make_async_remote_copy(
                src_ref=vbuf.at[g % SLOTS], dst_ref=dst, send_sem=ssem.at[g], recv_sem=rsem.at[g], device_id=(dp, peer), device_id_type=MESH)

        def to_far(g):
            return remote(g, out_ref.at[far(g)], jnp.where(far(g) < IMAGES, lax.rem(me + 2, 4), 3 - me))

        def to_near(g):
            return remote(g, out_ref.at[2 * IMAGES + g // 3], me + 1 - 2 * (me % 2))

        slot = jnp.where(i < away, lax.rem(i, SLOTS), SLOTS + i - away)

    def put(cs, v):
        if send:
            vbuf[slot, :, cs] = v
        else:
            out_ref[:, cs] = v

    def cols(c):
        return slice(c * nc, (c + 1) * nc)

    def project(slot):
        for c in range(D // nc):
            y = dot_tn(ob[slot], w(0, cols(c)))
            m_s[:, cols(c)] = (xb[slot, :, cols(c)].astype(f32) + (y + bo[:, cols(c)])).astype(bf16)

    def norm():
        def store(r, m, v):
            n_s[r:r + m, :] = v
        ln_rows(lambda r, m: m_s[r:r + m, :], store, gain, shift, 0, tm)

    @pl.when(i == 0)
    def _():
        x_copy(0).start()
        o_copy(0).start()
        x_copy(1).start()
        o_copy(1).start()
        if send:
            barrier = pltpu.get_barrier_semaphore()
            for peer in (me + 1 - 2 * (me % 2), lax.rem(me + 2, 4), 3 - me):
                pl.semaphore_signal(barrier, inc=1, device_id=(dp, peer), device_id_type=MESH)
            pl.semaphore_wait(barrier, 3)
        x_copy(0).wait()
        o_copy(0).wait()
        project(0)
        norm()

    @pl.when(i + 1 < n)
    def _():
        x_copy(i + 1).wait()
        o_copy(i + 1).wait()

    @pl.when(i + 2 < n)
    def _():
        x_copy(i + 2).start()
        o_copy(i + 2).start()

    if send:
        last = i - 1

        @pl.when(jnp.logical_and(jnp.logical_and(last >= 0, last < away), last % 3 < 2))
        def _():
            to_far(last).start()

        @pl.when(jnp.logical_and(jnp.logical_and(last >= 0, last < away), last % 3 == 2))
        def _():
            to_near(last).start()

        @pl.when(jnp.logical_and(i >= SLOTS, i < away))
        def _():
            to_near(i - SLOTS).wait_send()

    def up(j, c):
        f0 = j * fc + c * nc
        act[j % 2, :, cols(c)] = gelu(dot(n_s[...], w(1 + j, cols(c))) + bu_ref[one, f0:f0 + nc]).astype(bf16)

    def down(j, c):
        y = dot(act[j % 2], w(1 + nj + j, cols(c)))
        if j == 0:
            acc[:, cols(c)] = (m_s[:, cols(c)].astype(f32) + bd_ref[one, cols(c)]) + y
        elif j < nj - 1:
            acc[:, cols(c)] = acc[:, cols(c)] + y
        else:
            put(cols(c), (acc[:, cols(c)] + y).astype(bf16))

    for c in range(fc // nc):
        up(0, c)
    for j in range(1, nj):
        if j == nj - 1:
            project((i + 1) % 2)
        for c in range(D // nc):
            up(j, c)
            down(j - 1, c)
    norm()
    for c in range(D // nc):
        down(nj - 1, c)

    if send:
        @pl.when(i == n - 1)
        def _():
            for g in range(away - SLOTS, away):
                to_near(g).wait_send()
            for g in range(away):
                (to_near if g % 3 == 2 else to_far)(g).wait_recv()


def mlp(x, o, w, bo, g, s, bu, bd, layer, first, count, into=None, send=False, fc=1536, nc=512):
    n = count * SEQ // BLK
    base = first * SEQ // BLK
    dma = pltpu.SemaphoreType.DMA
    vm = pltpu.VMEM
    scratch = [vm((2, BLK, D), bf16), vm((2, D, BLK), bf16), vm((BLK, D), bf16), vm((BLK, D), bf16), vm((2, BLK, fc), bf16), vm((BLK, D), f32),
               dma((2,)), dma((2,))]
    params = dict(dimension_semantics=("arbitrary",))
    if send:
        scratch += [dma((3 * IMAGES,)), dma((3 * IMAGES,))]
        out_shape = (pltpu.HBM((3 * IMAGES, BLK, D), bf16), vm((SLOTS + IMAGES, BLK, D), bf16))
        out_spec = (HBM, VMEM)
        params.update(collective_id=0, has_side_effects=True)
    else:
        out_shape, out_spec = pltpu.HBM((T, D), bf16), pl.BlockSpec((BLK, D), lambda i: (base + i, 0))
    extra = [] if into is None else [into]
    tok = n * BLK
    return pl.pallas_call(
        functools.partial(mlp_kernel, layer=layer, base=base, n=n, fc=fc, nc=nc, alias=len(extra), send=send),
        out_shape=out_shape,
        grid=(n,),
        in_specs=[HBM, HBM, whole((2, D)), whole((2, D)), whole((2, D)), whole((2, F)), whole((2, D))] + [VMEM] + [HBM] * len(extra),
        out_specs=out_spec,
        scratch_shapes=scratch,
        input_output_aliases={8: 0} if extra else {},
        compiler_params=pltpu.CompilerParams(vmem_limit_bytes=SEND_LIMIT if send else LAYER_LIMIT, **params),
        cost_estimate=pl.CostEstimate(flops=2 * tok * D * (2 * F + D), bytes_accessed=tok * D * 6, transcendentals=tok * F),
        name="mlp",
    )(*at_hbm(x, o, bo, g, s, bu, bd), *at_vmem(w), *extra)


def finish_kernel(arrived, vbuf, out, buf, in_sem, via_sem, v_sem):
    me = lax.axis_index("sp")
    copy = pltpu.make_async_copy
    owner = (lax.rem(me + 2, 4), 3 - me, me + 1 - 2 * (me % 2))
    ins = [copy(arrived.at[p * IMAGES:(p + 1) * IMAGES], buf.at[p], in_sem.at[p]) for p in range(3)]
    outs = [copy(buf.at[p], out.at[pl.ds(o * IMAGES, IMAGES)], via_sem.at[p]) for p, o in enumerate(owner)]
    own = copy(vbuf.at[SLOTS:], out.at[pl.ds(me * IMAGES, IMAGES)], v_sem)
    for c in ins:
        c.start()
    own.start()
    for i, o in zip(ins, outs):
        i.wait()
        o.start()
    for c in outs:
        c.wait()
    own.wait()


def finish(arrived, vbuf):
    dma = pltpu.SemaphoreType.DMA
    return pl.pallas_call(
        finish_kernel,
        out_shape=jax.ShapeDtypeStruct((4 * IMAGES, BLK, D), bf16),
        in_specs=[HBM, VMEM],
        out_specs=HBM,
        scratch_shapes=[pltpu.VMEM((3, IMAGES, BLK, D), bf16), dma((3,)), dma((3,)), dma(())],
        compiler_params=pltpu.CompilerParams(vmem_limit_bytes=SEND_LIMIT),
        cost_estimate=pl.CostEstimate(flops=0, bytes_accessed=24 << 20, transcendentals=0),
        name="finish",
    )(*at_hbm(arrived), *at_vmem(vbuf))


def solution(mesh):
    token_spec = P('dp', 'sp', None)

    def device_step(image_tokens, ln1_gain, ln1_shift, w_qkv, b_qkv, w_out, b_out, ln2_gain, ln2_shift, w_up, b_up, w_down, b_down):
        layers = w_qkv.shape[0]
        w_t = w_qkv.transpose(0, 2, 3, 4, 1).reshape(layers, 3 * D, D)
        w_o = w_out.reshape(layers, D, D)
        me = lax.axis_index('sp')
        par = me.reshape(1).astype(jnp.int32)

        def exchange(k, part):
            return lax.ppermute(part, 'sp', [(s, s ^ k) for s in range(4)])

        def images(k, first, count):
            return lax.dynamic_slice_in_dim(image_tokens, (me ^ k) * IMAGES + first, count)

        far_a, far_b = exchange(2, images(2, 0, 1)), exchange(3, images(3, 0, 1))
        rest_a, rest_b, near = start(image_tokens)
        rest_a, rest_b = exchange(2, rest_a), exchange(3, rest_b)

        here = lambda i, m: i
        pre = (ln1_gain, ln1_shift)
        others = (w_o, w_up, w_down)

        def post(x, l, o, w, *place, **kw):
            return mlp(x, o, w, b_out, ln2_gain, ln2_shift, b_up, b_down, l, *place, **kw)

        *bufs, wq = qkv(par, image_tokens, lambda i, m: m[0] * IMAGES + i, near, here, *pre, w_t, b_qkv, 0, IMAGES, lambda i: 2 * i, True, hand=True)
        bufs = qkv(par, far_a, here, far_b, here, *pre, wq, b_qkv, 0, 1, lambda i: 1, True, into=bufs, given=True)
        o, wb = attn(*bufs[:5], *others, 0, 0, 1)
        h = post(bufs[5], 0, o, wb, 0, 1)
        bufs = qkv(par, rest_a, here, rest_b, here, *pre, w_t, b_qkv, 0, IMAGES - 1, lambda i: 2 * i + 3, True, into=bufs, after=h)
        o, wb = attn(*bufs[:5], *others, 0, 1, IMAGES - 1)
        h = post(bufs[5], 0, o, wb, 1, IMAGES - 1, into=h)
        x = h.reshape(4 * IMAGES, BLK, D)
        bufs = qkv(par, x, lambda i, m: 2 * i, x, lambda i, m: 2 * i + 1, *pre, w_t, b_qkv, 1, 2 * IMAGES, lambda i: i, False)
        o, wb = attn(*bufs[:5], *others, 1, 0, IMAGES, limit=SEND_LIMIT)
        return finish(*post(h, 1, o, wb, 0, IMAGES, send=True))

    return jax.shard_map(device_step, mesh=mesh, in_specs=(token_spec,) + (P(),) * 12, out_specs=token_spec, check_vma=False)
```

```python
import functools

import jax
import jax.numpy as jnp
from jax import lax
from jax.experimental import pallas as pl
from jax.experimental.pallas import tpu as pltpu
from jax.sharding import PartitionSpec as P

LN_EPS = 1e-6
HD = 96
HEADS = 16
D = HD * HEADS
F = 4 * D
IMAGES = 4
BLK = 256
SEQ = 4 * BLK
T = IMAGES * SEQ
CH = 4 * HD
C = HD ** -0.5 * 1.4426950408889634
LOW = 2.0 ** -80
f32, bf16 = jnp.float32, jnp.bfloat16
MESH = pl.DeviceIdType.MESH
HBM = pl.BlockSpec(memory_space=pltpu.HBM)


def dot(a, b):
    return jnp.dot(a, b, preferred_element_type=f32)


def dot_nt(a, b):
    return lax.dot_general(a, b, (((1,), (1,)), ((), ())), preferred_element_type=f32)


def dot_tn(a, b):
    return lax.dot_general(a, b, (((0,), (0,)), ((), ())), preferred_element_type=f32)


VMEM = pl.BlockSpec(memory_space=pltpu.VMEM)
LAYER_LIMIT = 93 << 18
EARLY = 6
SEND_LIMIT = 18 << 20
TURNS = 2
SLOTS = 3


def at_hbm(*arrays):
    return tuple(pltpu.with_memory_space_constraint(a, pltpu.HBM) for a in arrays)


def at_vmem(*arrays):
    return tuple(pltpu.with_memory_space_constraint(a, pltpu.VMEM) for a in arrays)


def layer_blocks(layer, wo, wu, wd):
    cuts = [slice(c * D, (c + 1) * D) for c in range(F // D)]
    return [wo.at[layer]] + [wu.at[layer, :, c] for c in cuts] + [wd.at[layer, c] for c in cuts]


def whole(shape):
    return pl.BlockSpec(shape, lambda *_: (0,) * len(shape))


def ln_rows(load, store, gain, shift, start, rows, step=16):
    for r in range(start, start + rows, step):
        v = load(r, step).astype(f32)
        mu = jnp.sum(v, axis=-1, keepdims=True) * (1.0 / D)
        c = v - mu
        var = jnp.sum(c * c, axis=-1, keepdims=True) * (1.0 / D)
        store(r, step, (c * lax.rsqrt(var + LN_EPS) * gain + shift).astype(bf16))


def start_kernel(tokens, sa, sb, near, buf, in_sem, out_sem, s_sem, r_sem):
    dp, me = lax.axis_index("dp"), lax.axis_index("sp")
    peer = me + 1 - 2 * (me % 2)
    swap = pltpu.make_async_remote_copy(
        src_ref=tokens.at[pl.ds(peer * IMAGES, IMAGES)], dst_ref=near, send_sem=s_sem, recv_sem=r_sem, device_id=(dp, peer), device_id_type=MESH)
    far = (lax.rem(me + 2, 4), 3 - me)
    ins = [pltpu.make_async_copy(tokens.at[pl.ds(f * IMAGES + 1, IMAGES - 1)], buf.at[n], in_sem.at[n]) for n, f in enumerate(far)]
    outs = [pltpu.make_async_copy(buf.at[n], out, out_sem.at[n]) for n, out in enumerate((sa, sb))]
    for c in ins:
        c.start()
    barrier = pltpu.get_barrier_semaphore()
    pl.semaphore_signal(barrier, inc=1, device_id=(dp, peer), device_id_type=MESH)
    pl.semaphore_wait(barrier, 1)
    swap.start()
    for i, o in zip(ins, outs):
        i.wait()
        o.start()
    for o in outs:
        o.wait()
    swap.wait()


def start(tokens):
    part = pltpu.HBM((IMAGES - 1, BLK, D), bf16)
    dma = pltpu.SemaphoreType.DMA
    return pl.pallas_call(
        start_kernel,
        out_shape=(part, part, pltpu.HBM((IMAGES, BLK, D), bf16)),
        in_specs=[HBM],
        out_specs=(HBM, HBM, HBM),
        scratch_shapes=[pltpu.VMEM((2, IMAGES - 1, BLK, D), bf16), dma((2,)), dma((2,)), dma(()), dma(())],
        compiler_params=pltpu.CompilerParams(vmem_limit_bytes=60 << 20, collective_id=1, has_side_effects=True),
        cost_estimate=pl.CostEstimate(flops=1 << 30, bytes_accessed=30 << 20, transcendentals=0),
        name="start",
    )(*at_hbm(tokens))


def qkv_kernel(*refs, layer, n, copy_h, alias, given, hand, out_block):
    (_, xa, xb, xan, xbn, g_ref, s_ref), refs = refs[:7], refs[7:]
    (w, b_ref), refs = refs[given:2 + given], refs[2 + given:]
    if hand:
        others, refs = refs[:3], refs[3:]
    refs = refs[alias:]
    (q_ref, k_ref, v_ref, nq_ref, nk_ref), refs = refs[:5], refs[5:]
    if copy_h:
        h_ref, refs = refs[0], refs[1:]
    if hand:
        w_hbm, wa, w, refs = w, refs[0], refs[1], refs[2:]
    refs = refs[given:]
    if copy_h and not given:
        h_sem, refs = refs[0], refs[1:]
    both, sem = refs[:2]
    if hand:
        ahead, early_sem = refs[2:]
        early = [pltpu.make_async_copy(p, wa.at[c * D:(c + 1) * D], early_sem.at[c]) for c, p in enumerate(layer_blocks(layer, *others)[:EARLY])]
    elif not given:
        w_hbm, w = w, refs[2]
    i = pl.program_id(0)
    tm = 2 * BLK
    per = D // CH
    order = (1, 0, 2)
    gain, shift = g_ref[layer:layer + 1, :], s_ref[layer:layer + 1, :]

    def w_copy(p, t, row, rows):
        r = pl.ds(t * D + row, rows)
        return pltpu.make_async_copy(w_hbm.at[layer, r], w.at[r], sem.at[p])

    def chunk(c, size):
        return c * size if isinstance(c, int) else pl.multiple_of(c * size, size)

    def norm(src, dst, slot, src_row, dst_row):
        def load(r, m):
            return src[0, pl.ds(src_row + r, m), :]
        def store(r, m, v):
            dst[slot, pl.ds(dst_row + r, m), :] = v
        ln_rows(load, store, gain, shift, 0, 16, 8 if given else 16)

    def norm_all(a, b, dst, slot):
        for r in range(0, BLK, 16):
            norm(a, dst, slot, r, r)
        for r in range(0, BLK, 16):
            norm(b, dst, slot, r, r + BLK)

    def project(t, c, slot):
        y = dot_nt(w[pl.ds(chunk(c, CH) + t * D, CH), :], both[slot])
        heads = CH // HD
        bias = b_ref[layer, t, pl.ds(chunk(c, heads), heads), :].T
        bias = jnp.concatenate([jnp.broadcast_to(bias[:, h:h + 1], (HD, tm)) for h in range(heads)], axis=0)
        yb = (y + bias).astype(bf16)
        r0 = pl.ds(chunk(c, CH), CH)
        if t == 2:
            v_ref[r0, :] = yb
            return
        if t == 0:
            q_ref[r0, :] = yb
        for h in range(heads):
            yh = yb[h * HD:(h + 1) * HD, :]
            yf = yh.astype(f32)
            nn = jnp.sum(yf * yf, axis=0, keepdims=True)
            if t == 0:
                nq_ref[pl.ds(c * heads + h, 1), :] = nn
            else:
                nk_ref[pl.ds(c * heads + h, 1), :] = nn
                one = (lax.broadcasted_iota(jnp.int32, (128 - HD, tm), 0) == 0).astype(f32).astype(bf16)
                k_ref[c * heads + h] = jnp.concatenate([yh, one], axis=0).T

    if copy_h and not given:
        row = pl.multiple_of(out_block(i) * tm, tm)
        h_copies = [pltpu.make_async_copy(x.at[0], h_ref.at[pl.ds(row + p * BLK, BLK)], h_sem.at[p]) for p, x in enumerate((xa, xb))]
        for c in h_copies:
            c.start()

    def keep():
        if given:
            h_ref[:BLK, :] = xa[0]
            h_ref[BLK:, :] = xb[0]
        elif copy_h:
            for c in h_copies:
                c.wait()

    if hand:
        copies = lambda part: [w_copy(part * 3 + t, t, part * (D // TURNS), D // TURNS) for t in range(3)]

        @pl.when(i == 0)
        def _():
            for part in range(TURNS):
                for c in copies(part):
                    c.start()
            for c in early:
                c.start(priority=1)
            norm_all(xa, xb, ahead, 0)

        both[0] = ahead[0]

        def turn(part, carry):
            @pl.when(i == 0)
            def _():
                for c in copies(part):
                    c.wait()
            products = [(t, c) for c in range(per // TURNS) for t in order]
            half = BLK // TURNS // 16
            for p, (t, c) in enumerate(products):
                project(t, part * (per // TURNS) + c, 0)
                for g in range(p * 2 * half // len(products), (p + 1) * 2 * half // len(products)):
                    src, base = (xan, 0) if g < half else (xbn, BLK)
                    at = pl.multiple_of(part * (BLK // TURNS) + g % half * 16, 16)
                    norm(src, ahead, 0, at, pl.multiple_of(base + at, 16))
            return carry
        lax.fori_loop(0, TURNS, turn, 0)
        keep()

        @pl.when(i == n - 1)
        def _():
            for c in early:
                c.wait()
        return

    parts = {} if given else {0: w_copy(0, order[0], 0, CH), 1: w_copy(1, order[0], CH, D - CH),
                              per: w_copy(2, order[1], 0, D), 2 * per: w_copy(3, order[2], 0, D)}

    def body(first, now, later):
        for p in range(3 * per):
            if first and p in parts:
                parts[p].wait()
            project(order[p // per], p % per, now)
            if n > 1 and 0 <= p - 2 < 8:
                for r in range((p - 2) * (tm // 8), (p - 1) * (tm // 8), 16):
                    norm(xan if r < BLK else xbn, both, later, r % BLK, r)
        keep()

    @pl.when(i == 0)
    def _():
        for p in parts:
            if p < 2 * per:
                parts[p].start()
        norm_all(xa, xb, both, 0)
        if not given:
            parts[2 * per].start()
        body(True, 0, 1)

    if n > 1:
        @pl.when(i > 0)
        def _():
            body(False, lax.rem(i, 2), lax.rem(i + 1, 2))


def qkv(par, xa, xa_map, xb, xb_map, g, s, w, b, layer, n, out_block, copy_h, into=None, after=None, given=None, hand=()):
    tm = 2 * BLK
    last = n - 1
    held = [] if given is None else [given]
    chain = bool(held or hand)
    once = dict(pipeline_mode=pl.Buffered(1))
    piece = lambda f, d: pl.BlockSpec((1, BLK, D), lambda i, m: (f(jnp.minimum(i + d, last), m), 0, 0), **(once if n == 1 else {}))
    col = lambda r: pl.BlockSpec((r, tm), lambda i, m: (0, out_block(i)))
    shapes = [pltpu.HBM((D, T), bf16), pltpu.HBM((HEADS, T, 128), bf16), pltpu.HBM((D, T), bf16), pltpu.HBM((HEADS, T), f32), pltpu.HBM((HEADS, T), f32)]
    specs = [col(D), pl.BlockSpec((HEADS, tm, 128), lambda i, m: (0, out_block(i), 0)), col(D), col(HEADS), col(HEADS)]
    if copy_h:
        shapes.append(pltpu.HBM((T, D), bf16))
        specs.append(pl.BlockSpec((tm, D), lambda i, m: (out_block(i), 0)) if held else HBM)
    dma = pltpu.SemaphoreType.DMA
    scratch = [dma((2,))] * (copy_h and not held) + [pltpu.VMEM((1 if chain else 2, tm, D), bf16), dma((3 * TURNS if hand else 4,))]
    if hand:
        shapes += [pltpu.VMEM((EARLY * D, D), bf16), pltpu.VMEM((3 * D, D), bf16)]
        specs += [VMEM, VMEM]
        scratch += [pltpu.VMEM((1, tm, D), bf16), dma((EARLY,))]
    elif held:
        shapes.append(pltpu.VMEM(given.shape, bf16))
        specs.append(VMEM)
    else:
        scratch.append(pltpu.VMEM((3 * D, D), bf16))
    into = list(into or ())
    extra = into + ([after] if after is not None else [])
    alias = {9 + len(held) + len(hand) + a: a for a in range(len(into))}
    if held:
        alias[7] = len(shapes) - 1
    return pl.pallas_call(
        functools.partial(qkv_kernel, layer=layer, n=n, copy_h=copy_h, alias=len(extra), given=len(held), hand=bool(hand), out_block=out_block),
        out_shape=tuple(shapes),
        grid_spec=pltpu.PrefetchScalarGridSpec(
            num_scalar_prefetch=1, grid=(n,),
            in_specs=[piece(xa_map, 0), piece(xb_map, 0), piece(xa_map, 1), piece(xb_map, 1), whole((2, D)), whole((2, D))]
            + ([VMEM, VMEM] if held else [HBM]) + [whole(b.shape)] + [HBM] * (len(hand) + len(extra)),
            out_specs=tuple(specs),
            scratch_shapes=scratch),
        input_output_aliases=alias,
        compiler_params=pltpu.CompilerParams(vmem_limit_bytes=LAYER_LIMIT if chain else 63 << 20, dimension_semantics=("arbitrary",)),
        cost_estimate=pl.CostEstimate(flops=2 * n * tm * D * 3 * D, bytes_accessed=n * tm * D * 10, transcendentals=0),
        name="qkv",
    )(par, *at_hbm(xa, xb, xa, xb, g, s), *(at_vmem(*held, w) if held else at_hbm(w)), *at_hbm(b, *hand), *extra)


def attn_kernel(q_ref, k_ref, v_ref, nq_ref, nk_ref, wo_hbm, wu_hbm, wd_hbm, *refs, layer, have, hp, nq, kb, lag):
    o_ref, wb, sem = (refs[1], refs[3], refs[4]) if have else refs
    step = pl.program_id(0) * pl.num_programs(1) + pl.program_id(1)
    parts = layer_blocks(layer, wo_hbm, wu_hbm, wd_hbm)[have:]
    copies = [pltpu.make_async_copy(p, wb.at[c * D:(c + 1) * D], sem.at[c]) for c, p in enumerate(parts)]

    @pl.when(step == 0)
    def _():
        for c in copies:
            c.start(priority=1)

    @pl.when(step == pl.num_programs(0) * pl.num_programs(1) - 1)
    def _():
        for c in copies:
            c.wait()

    nk = SEQ // kb
    units = [(h, q, k) for h in range(hp) for q in range(SEQ // nq) for k in range(nk)]
    st, lows, acc, rhs = {}, [], {}, {}

    def rows(h):
        return slice(h * HD, (h + 1) * HD)

    def shift_rows(h, q):
        kmax = jnp.max(nk_ref[h:h + 1, :], axis=1, keepdims=True)
        m = jnp.sqrt(nq_ref[h:h + 1, q * nq:(q + 1) * nq] * kmax) * (-1.0 - 2.0 ** -7)
        first = lax.broadcasted_iota(jnp.int32, (128 - HD, nq), 0) == 0
        return jnp.where(first, jnp.broadcast_to(m, (128 - HD, nq)), 0.0).astype(bf16)

    def score(u):
        h, q, k = u
        if k == 0:
            rhs[h, q] = jnp.concatenate([q_ref[rows(h), q * nq:(q + 1) * nq], shift_rows(h, q)], axis=0)
        st[u] = dot(k_ref[h, k * kb:(k + 1) * kb, :], rhs[h, q])

    def mix(u):
        h, q, k = u
        p = jnp.exp2(st.pop(u) * C)
        ls = jnp.sum(p.reshape(kb // 8, 8, nq), axis=0)
        pv = dot(v_ref[rows(h), k * kb:(k + 1) * kb], p.astype(bf16))
        if k:
            a, b = acc[h, q]
            ls, pv = a + ls, b + pv
        acc[h, q] = (ls, pv)
        if k == nk - 1:
            a, b = acc.pop((h, q))
            l = jnp.sum(a, axis=0, keepdims=True)
            lows.append(l)
            o_ref[rows(h), q * nq:(q + 1) * nq] = (b * (1.0 / l)).astype(bf16)

    for i in range(len(units) + lag):
        if i < len(units):
            score(units[i])
        if i >= lag:
            mix(units[i - lag])
    low = lows[0]
    for l in lows[1:]:
        low = jnp.minimum(low, l)
    low = jnp.min(low)

    @pl.when(jnp.logical_not(low >= LOW))
    def _():
        qb = 256
        def body(j, c):
            h = lax.div(j, SEQ // qb)
            qs = pl.ds(pl.multiple_of(lax.rem(j, SEQ // qb) * qb, qb), qb)
            r = pl.ds(pl.multiple_of(h * HD, 32), HD)
            s = dot(k_ref[h, :, :HD], q_ref[r, qs])
            m = jnp.max(s, axis=0, keepdims=True)
            p = jnp.exp2((s - m) * C)
            l = jnp.sum(p, axis=0, keepdims=True)
            o_ref[r, qs] = (dot(v_ref[r, :], p.astype(bf16)) / l).astype(bf16)
            return c
        lax.fori_loop(0, hp * (SEQ // qb), body, 0)


def attn(q, k, v, nq2, nk2, w_o, w_up, w_down, layer, first, count, limit=LAYER_LIMIT, keep=None, hp=8, nq=512, kb=256, lag=3):
    held = [] if keep is None else [keep]
    have = EARLY if held else 0
    blk = pl.BlockSpec((hp * HD, SEQ), lambda i, j: (j, first + i))
    nrm = pl.BlockSpec((hp, SEQ), lambda i, j: (j, first + i))
    return pl.pallas_call(
        functools.partial(attn_kernel, layer=layer, have=have, hp=hp, nq=nq, kb=kb, lag=lag),
        out_shape=(pltpu.HBM((D, count * SEQ), bf16), *(pltpu.VMEM(a.shape, bf16) for a in held), pltpu.VMEM((D + 2 * F - have * D, D), bf16)),
        grid=(count, HEADS // hp),
        in_specs=[blk, pl.BlockSpec((hp, SEQ, 128), lambda i, j: (j, first + i, 0)), blk, nrm, nrm, HBM, HBM, HBM] + [VMEM] * len(held),
        out_specs=(pl.BlockSpec((hp * HD, SEQ), lambda i, j: (j, i)),) + (VMEM,) * (1 + len(held)),
        input_output_aliases={8: 1} if held else {},
        scratch_shapes=[pltpu.SemaphoreType.DMA((1 + 2 * F // D,))],
        compiler_params=pltpu.CompilerParams(vmem_limit_bytes=limit, dimension_semantics=("arbitrary", "arbitrary")),
        cost_estimate=pl.CostEstimate(flops=4 * count * SEQ * SEQ * D, bytes_accessed=count * SEQ * D * 9, transcendentals=count * SEQ * SEQ * HEADS),
        name="attn",
    )(*at_hbm(q, k, v, nq2, nk2), w_o, w_up, w_down, *at_vmem(*held))


def gelu(u):
    c = 0.7978845608028654
    return (0.5 * u) * (1.0 + jnp.tanh(u * (c + (c * 0.044715) * (u * u))))


def mlp_kernel(*refs, layer, base, n, fc, nc, alias, send, count):
    (x_hbm, o_hbm, bo_ref, g_ref, s_ref, bu_ref, bd_ref), refs = refs[:7], refs[7:]
    weights, refs = refs[:count], refs[count + alias:]
    out_ref, refs = refs[0], refs[1:]
    if send:
        vbuf, refs = refs[0], refs[1:]
    (xb, ob, m_s, n_s, act, acc, xsem, osem), refs = refs[:8], refs[8:]

    def w(b, cs):
        if count == 2:
            ref, b = (weights[0], b) if b < EARLY else (weights[1], b - EARLY)
            return ref[b * D:(b + 1) * D, cs]
        return weights[0][b * D:(b + 1) * D, cs]

    i = pl.program_id(0)
    tm = BLK
    assert fc == D
    nj = F // fc
    one = slice(layer, layer + 1)
    gain, shift, bo = g_ref[one, :], s_ref[one, :], bo_ref[one, :]

    away = 3 * IMAGES

    def far(g):
        return g // 3 * 2 + g % 3

    def block(g):
        if not send:
            return g
        f = far(g)
        k = jnp.where(g >= away, 0, jnp.where(g % 3 == 2, 1, 2 + f // IMAGES))
        m = jnp.where(g >= away, g - away, jnp.where(g % 3 == 2, g // 3, f % IMAGES))
        return m * 4 + k

    def x_copy(g):
        slot = g % 2
        return pltpu.make_async_copy(x_hbm.at[pl.ds((base + block(g)) * tm, tm)], xb.at[slot], xsem.at[slot])

    def o_copy(g):
        slot = g % 2
        return pltpu.make_async_copy(o_hbm.at[:, pl.ds(pl.multiple_of(block(g) * tm, tm), tm)], ob.at[slot], osem.at[slot])

    if send:
        ssem, rsem = refs
        dp, me = lax.axis_index("dp"), lax.axis_index("sp")

        def remote(g, dst, peer):
            return pltpu.make_async_remote_copy(
                src_ref=vbuf.at[g % SLOTS], dst_ref=dst, send_sem=ssem.at[g], recv_sem=rsem.at[g], device_id=(dp, peer), device_id_type=MESH)

        def to_far(g):
            return remote(g, out_ref.at[far(g)], jnp.where(far(g) < IMAGES, lax.rem(me + 2, 4), 3 - me))

        def to_near(g):
            return remote(g, out_ref.at[2 * IMAGES + g // 3], me + 1 - 2 * (me % 2))

        slot = jnp.where(i < away, lax.rem(i, SLOTS), SLOTS + i - away)

    def put(cs, v):
        if send:
            vbuf[slot, :, cs] = v
        else:
            out_ref[:, cs] = v

    def cols(c):
        return slice(c * nc, (c + 1) * nc)

    def project(slot):
        for c in range(D // nc):
            y = dot_tn(ob[slot], w(0, cols(c)))
            m_s[:, cols(c)] = (xb[slot, :, cols(c)].astype(f32) + (y + bo[:, cols(c)])).astype(bf16)

    def norm():
        def store(r, m, v):
            n_s[r:r + m, :] = v
        ln_rows(lambda r, m: m_s[r:r + m, :], store, gain, shift, 0, tm)

    @pl.when(i == 0)
    def _():
        o_copy(0).start()
        x_copy(0).start()
        if send:
            barrier = pltpu.get_barrier_semaphore()
            for peer in (me + 1 - 2 * (me % 2), lax.rem(me + 2, 4), 3 - me):
                pl.semaphore_signal(barrier, inc=1, device_id=(dp, peer), device_id_type=MESH)
            pl.semaphore_wait(barrier, 3)
        o_copy(0).wait()
        x_copy(0).wait()
        o_copy(1).start()
        x_copy(1).start()
        project(0)
        norm()

    @pl.when(i + 1 < n)
    def _():
        x_copy(i + 1).wait()
        o_copy(i + 1).wait()

    @pl.when(i + 2 < n)
    def _():
        x_copy(i + 2).start()
        o_copy(i + 2).start()

    if send:
        last = i - 1

        @pl.when(jnp.logical_and(jnp.logical_and(last >= 0, last < away), last % 3 < 2))
        def _():
            to_far(last).start()

        @pl.when(jnp.logical_and(jnp.logical_and(last >= 0, last < away), last % 3 == 2))
        def _():
            to_near(last).start()

        @pl.when(jnp.logical_and(i >= SLOTS, i < away))
        def _():
            to_near(i - SLOTS).wait_send()

    def up(j, c):
        f0 = j * fc + c * nc
        act[j % 2, :, cols(c)] = gelu(dot(n_s[...], w(1 + j, cols(c))) + bu_ref[one, f0:f0 + nc]).astype(bf16)

    def down(j, c):
        y = dot(act[j % 2], w(1 + nj + j, cols(c)))
        if j == 0:
            acc[:, cols(c)] = (m_s[:, cols(c)].astype(f32) + bd_ref[one, cols(c)]) + y
        elif j < nj - 1:
            acc[:, cols(c)] = acc[:, cols(c)] + y
        else:
            put(cols(c), (acc[:, cols(c)] + y).astype(bf16))

    for c in range(fc // nc):
        up(0, c)
    for j in range(1, nj):
        if j == nj - 1:
            project((i + 1) % 2)
        for c in range(D // nc):
            up(j, c)
            down(j - 1, c)
    norm()
    for c in range(D // nc):
        down(nj - 1, c)

    if send:
        @pl.when(i == n - 1)
        def _():
            for g in range(away - SLOTS, away):
                to_near(g).wait_send()
            for g in range(away):
                (to_near if g % 3 == 2 else to_far)(g).wait_recv()


def mlp(x, o, w, bo, g, s, bu, bd, layer, first, count, into=None, send=False, fc=1536, nc=512):
    n = count * SEQ // BLK
    base = first * SEQ // BLK
    dma = pltpu.SemaphoreType.DMA
    vm = pltpu.VMEM
    scratch = [vm((2, BLK, D), bf16), vm((2, D, BLK), bf16), vm((BLK, D), bf16), vm((BLK, D), bf16), vm((2, BLK, fc), bf16), vm((BLK, D), f32),
               dma((2,)), dma((2,))]
    params = dict(dimension_semantics=("arbitrary",))
    if send:
        scratch += [dma((3 * IMAGES,)), dma((3 * IMAGES,))]
        out_shape = (pltpu.HBM((3 * IMAGES, BLK, D), bf16), vm((SLOTS + IMAGES, BLK, D), bf16))
        out_spec = (HBM, VMEM)
        params.update(collective_id=0, has_side_effects=True)
    else:
        out_shape, out_spec = pltpu.HBM((T, D), bf16), pl.BlockSpec((BLK, D), lambda i: (base + i, 0))
    extra = [] if into is None else [into]
    tok = n * BLK
    return pl.pallas_call(
        functools.partial(mlp_kernel, layer=layer, base=base, n=n, fc=fc, nc=nc, alias=len(extra), send=send, count=len(w)),
        out_shape=out_shape,
        grid=(n,),
        in_specs=[HBM, HBM, whole((2, D)), whole((2, D)), whole((2, D)), whole((2, F)), whole((2, D))] + [VMEM] * len(w) + [HBM] * len(extra),
        out_specs=out_spec,
        scratch_shapes=scratch,
        input_output_aliases={7 + len(w): 0} if extra else {},
        compiler_params=pltpu.CompilerParams(vmem_limit_bytes=SEND_LIMIT if send else LAYER_LIMIT, **params),
        cost_estimate=pl.CostEstimate(flops=2 * tok * D * (2 * F + D), bytes_accessed=tok * D * 6, transcendentals=tok * F),
        name="mlp",
    )(*at_hbm(x, o, bo, g, s, bu, bd), *at_vmem(*w), *extra)


def finish_kernel(arrived, vbuf, out, buf, in_sem, via_sem, v_sem):
    me = lax.axis_index("sp")
    copy = pltpu.make_async_copy
    owner = (lax.rem(me + 2, 4), 3 - me, me + 1 - 2 * (me % 2))
    blocks = range(3 * IMAGES)
    ins = [copy(arrived.at[p], buf.at[p], in_sem.at[p]) for p in blocks]
    outs = [copy(buf.at[p], out.at[owner[p // IMAGES] * IMAGES + p % IMAGES], via_sem.at[p]) for p in blocks]
    own = copy(vbuf.at[SLOTS:], out.at[pl.ds(me * IMAGES, IMAGES)], v_sem)
    for c in ins:
        c.start()
    own.start()
    for i, o in zip(ins, outs):
        i.wait()
        o.start()
    for c in outs:
        c.wait()
    own.wait()


def finish(arrived, vbuf):
    dma = pltpu.SemaphoreType.DMA
    return pl.pallas_call(
        finish_kernel,
        out_shape=jax.ShapeDtypeStruct((4 * IMAGES, BLK, D), bf16),
        in_specs=[HBM, VMEM],
        out_specs=HBM,
        scratch_shapes=[pltpu.VMEM((3 * IMAGES, BLK, D), bf16), dma((3 * IMAGES,)), dma((3 * IMAGES,)), dma(())],
        compiler_params=pltpu.CompilerParams(vmem_limit_bytes=SEND_LIMIT),
        cost_estimate=pl.CostEstimate(flops=0, bytes_accessed=24 << 20, transcendentals=0),
        name="finish",
    )(*at_hbm(arrived), *at_vmem(vbuf))


def solution(mesh):
    token_spec = P('dp', 'sp', None)

    def device_step(image_tokens, ln1_gain, ln1_shift, w_qkv, b_qkv, w_out, b_out, ln2_gain, ln2_shift, w_up, b_up, w_down, b_down):
        layers = w_qkv.shape[0]
        w_t = w_qkv.transpose(0, 2, 3, 4, 1).reshape(layers, 3 * D, D)
        w_o = w_out.reshape(layers, D, D)
        me = lax.axis_index('sp')
        par = me.reshape(1).astype(jnp.int32)

        def exchange(k, part):
            return lax.ppermute(part, 'sp', [(s, s ^ k) for s in range(4)])

        def images(k, first, count):
            return lax.dynamic_slice_in_dim(image_tokens, (me ^ k) * IMAGES + first, count)

        far_a, far_b = exchange(2, images(2, 0, 1)), exchange(3, images(3, 0, 1))
        rest_a, rest_b, near = start(image_tokens)
        rest_a, rest_b = exchange(2, rest_a), exchange(3, rest_b)

        here = lambda i, m: i
        pre = (ln1_gain, ln1_shift)
        others = (w_o, w_up, w_down)

        def post(x, l, o, w, *place, **kw):
            return mlp(x, o, w, b_out, ln2_gain, ln2_shift, b_up, b_down, l, *place, **kw)

        *bufs, wa, wq = qkv(par, image_tokens, lambda i, m: m[0] * IMAGES + i, near, here, *pre, w_t, b_qkv, 0, IMAGES, lambda i: 2 * i, True,
                            hand=others)
        *bufs, wa = qkv(par, far_a, here, far_b, here, *pre, wq, b_qkv, 0, 1, lambda i: 1, True, into=bufs, given=wa)
        o, *w = attn(*bufs[:5], *others, 0, 0, 1, keep=wa)
        h = post(bufs[5], 0, o, w, 0, 1)
        bufs = qkv(par, rest_a, here, rest_b, here, *pre, w_t, b_qkv, 0, IMAGES - 1, lambda i: 2 * i + 3, True, into=bufs, after=h)
        o, *w = attn(*bufs[:5], *others, 0, 1, IMAGES - 1)
        h = post(bufs[5], 0, o, w, 1, IMAGES - 1, into=h)
        x = h.reshape(4 * IMAGES, BLK, D)
        bufs = qkv(par, x, lambda i, m: 2 * i, x, lambda i, m: 2 * i + 1, *pre, w_t, b_qkv, 1, 2 * IMAGES, lambda i: i, False)
        o, *w = attn(*bufs[:5], *others, 1, 0, IMAGES, limit=SEND_LIMIT)
        return finish(*post(h, 1, o, w, 0, IMAGES, send=True))

    return jax.shard_map(device_step, mesh=mesh, in_specs=(token_spec,) + (P(),) * 12, out_specs=token_spec, check_vma=False)
```

```python
import functools

import jax
import jax.numpy as jnp
from jax import lax
from jax.experimental import pallas as pl
from jax.experimental.pallas import tpu as pltpu
from jax.sharding import PartitionSpec as P

LN_EPS = 1e-6
HD = 96
HEADS = 16
D = HD * HEADS
F = 4 * D
IMAGES = 4
BLK = 256
SEQ = 4 * BLK
T = IMAGES * SEQ
CH = 4 * HD
C = HD ** -0.5 * 1.4426950408889634
LOW = 2.0 ** -80
f32, bf16 = jnp.float32, jnp.bfloat16
MESH = pl.DeviceIdType.MESH
HBM = pl.BlockSpec(memory_space=pltpu.HBM)


def dot(a, b):
    return jnp.dot(a, b, preferred_element_type=f32)


def dot_nt(a, b):
    return lax.dot_general(a, b, (((1,), (1,)), ((), ())), preferred_element_type=f32)


def dot_tn(a, b):
    return lax.dot_general(a, b, (((0,), (0,)), ((), ())), preferred_element_type=f32)


VMEM = pl.BlockSpec(memory_space=pltpu.VMEM)
LAYER_LIMIT = 93 << 18
EARLY = 6
SEND_LIMIT = 18 << 20
TURNS = 4
SLOTS = 3


def at_hbm(*arrays):
    return tuple(pltpu.with_memory_space_constraint(a, pltpu.HBM) for a in arrays)


def at_vmem(*arrays):
    return tuple(pltpu.with_memory_space_constraint(a, pltpu.VMEM) for a in arrays)


def layer_blocks(layer, wo, wu, wd):
    cuts = [slice(c * D, (c + 1) * D) for c in range(F // D)]
    return [wo.at[layer]] + [wu.at[layer, :, c] for c in cuts] + [wd.at[layer, c] for c in cuts]


def whole(shape):
    return pl.BlockSpec(shape, lambda *_: (0,) * len(shape))


def ln_rows(load, store, gain, shift, start, rows, step=16):
    for r in range(start, start + rows, step):
        v = load(r, step).astype(f32)
        mu = jnp.sum(v, axis=-1, keepdims=True) * (1.0 / D)
        c = v - mu
        var = jnp.sum(c * c, axis=-1, keepdims=True) * (1.0 / D)
        store(r, step, (c * lax.rsqrt(var + LN_EPS) * gain + shift).astype(bf16))


def start_kernel(tokens, sa, sb, near, buf, in_sem, out_sem, s_sem, r_sem):
    dp, me = lax.axis_index("dp"), lax.axis_index("sp")
    peer = me + 1 - 2 * (me % 2)
    swap = pltpu.make_async_remote_copy(
        src_ref=tokens.at[pl.ds(peer * IMAGES, IMAGES)], dst_ref=near, send_sem=s_sem, recv_sem=r_sem, device_id=(dp, peer), device_id_type=MESH)
    far = (lax.rem(me + 2, 4), 3 - me)
    ins = [pltpu.make_async_copy(tokens.at[pl.ds(f * IMAGES + 1, IMAGES - 1)], buf.at[n], in_sem.at[n]) for n, f in enumerate(far)]
    outs = [pltpu.make_async_copy(buf.at[n], out, out_sem.at[n]) for n, out in enumerate((sa, sb))]
    for c in ins:
        c.start()
    barrier = pltpu.get_barrier_semaphore()
    pl.semaphore_signal(barrier, inc=1, device_id=(dp, peer), device_id_type=MESH)
    pl.semaphore_wait(barrier, 1)
    swap.start()
    for i, o in zip(ins, outs):
        i.wait()
        o.start()
    for o in outs:
        o.wait()
    swap.wait()


def start(tokens):
    part = pltpu.HBM((IMAGES - 1, BLK, D), bf16)
    dma = pltpu.SemaphoreType.DMA
    return pl.pallas_call(
        start_kernel,
        out_shape=(part, part, pltpu.HBM((IMAGES, BLK, D), bf16)),
        in_specs=[HBM],
        out_specs=(HBM, HBM, HBM),
        scratch_shapes=[pltpu.VMEM((2, IMAGES - 1, BLK, D), bf16), dma((2,)), dma((2,)), dma(()), dma(())],
        compiler_params=pltpu.CompilerParams(vmem_limit_bytes=60 << 20, collective_id=1, has_side_effects=True),
        cost_estimate=pl.CostEstimate(flops=1 << 30, bytes_accessed=30 << 20, transcendentals=0),
        name="start",
    )(*at_hbm(tokens))


def qkv_kernel(*refs, layer, n, copy_h, alias, given, hand, out_block):
    (_, xa, xb, xan, xbn, g_ref, s_ref), refs = refs[:7], refs[7:]
    (w, b_ref), refs = refs[given:2 + given], refs[2 + given:]
    if hand:
        others, refs = refs[:3], refs[3:]
    refs = refs[alias:]
    (q_ref, k_ref, v_ref, nq_ref, nk_ref), refs = refs[:5], refs[5:]
    if copy_h:
        h_ref, refs = refs[0], refs[1:]
    if hand:
        w_hbm, wa, w, refs = w, refs[0], refs[1], refs[2:]
    refs = refs[given:]
    if copy_h and not given:
        h_sem, refs = refs[0], refs[1:]
    both, sem = refs[:2]
    if hand:
        ahead, early_sem = refs[2:]
        early = [pltpu.make_async_copy(p, wa.at[c * D:(c + 1) * D], early_sem.at[c]) for c, p in enumerate(layer_blocks(layer, *others)[:EARLY])]
    elif not given:
        w_hbm, w = w, refs[2]
    i = pl.program_id(0)
    tm = 2 * BLK
    ch = CH // 2 if given else CH
    per = D // ch
    order = (1, 0, 2)
    gain, shift = g_ref[layer:layer + 1, :], s_ref[layer:layer + 1, :]

    def w_copy(p, t, row, rows):
        r = pl.ds(t * D + row, rows)
        return pltpu.make_async_copy(w_hbm.at[layer, r], w.at[r], sem.at[p])

    def chunk(c, size):
        return c * size if isinstance(c, int) else pl.multiple_of(c * size, size)

    def norm(src, dst, slot, src_row, dst_row):
        def load(r, m):
            return src[0, pl.ds(src_row + r, m), :]
        def store(r, m, v):
            dst[slot, pl.ds(dst_row + r, m), :] = v
        ln_rows(load, store, gain, shift, 0, 16, 8 if given else 16)

    def norm_all(a, b, dst, slot):
        for r in range(0, BLK, 16):
            norm(a, dst, slot, r, r)
        for r in range(0, BLK, 16):
            norm(b, dst, slot, r, r + BLK)

    def project(t, c, slot):
        y = dot_nt(w[pl.ds(chunk(c, ch) + t * D, ch), :], both[slot])
        heads = ch // HD
        bias = b_ref[layer, t, pl.ds(chunk(c, heads), heads), :].T
        bias = jnp.concatenate([jnp.broadcast_to(bias[:, h:h + 1], (HD, tm)) for h in range(heads)], axis=0)
        yb = (y + bias).astype(bf16)
        r0 = pl.ds(chunk(c, ch), ch)
        if t == 2:
            v_ref[r0, :] = yb
            return
        if t == 0:
            q_ref[r0, :] = yb
        for h in range(heads):
            yh = yb[h * HD:(h + 1) * HD, :]
            yf = yh.astype(f32)
            nn = jnp.sum(yf * yf, axis=0, keepdims=True)
            if t == 0:
                nq_ref[pl.ds(c * heads + h, 1), :] = nn
            else:
                nk_ref[pl.ds(c * heads + h, 1), :] = nn
                one = (lax.broadcasted_iota(jnp.int32, (128 - HD, tm), 0) == 0).astype(f32).astype(bf16)
                k_ref[c * heads + h] = jnp.concatenate([yh, one], axis=0).T

    if copy_h and not given:
        row = pl.multiple_of(out_block(i) * tm, tm)
        h_copies = [pltpu.make_async_copy(x.at[0], h_ref.at[pl.ds(row + p * BLK, BLK)], h_sem.at[p]) for p, x in enumerate((xa, xb))]
        for c in h_copies:
            c.start()

    def keep():
        if given:
            h_ref[:BLK, :] = xa[0]
            h_ref[BLK:, :] = xb[0]
        elif copy_h:
            for c in h_copies:
                c.wait()

    if hand:
        copies = lambda part: [w_copy(part * 3 + t, t, part * (D // TURNS), D // TURNS) for t in range(3)]

        @pl.when(i == 0)
        def _():
            for part in range(TURNS):
                for c in copies(part):
                    c.start()
            for c in early:
                c.start(priority=1)
            norm_all(xa, xb, ahead, 0)

        both[0] = ahead[0]

        def turn(part, carry):
            @pl.when(i == 0)
            def _():
                for c in copies(part):
                    c.wait()
            products = [(t, c) for c in range(per // TURNS) for t in order]
            half = BLK // TURNS // 16
            for p, (t, c) in enumerate(products):
                project(t, part * (per // TURNS) + c, 0)
                for g in range(p * 2 * half // len(products), (p + 1) * 2 * half // len(products)):
                    src, base = (xan, 0) if g < half else (xbn, BLK)
                    at = pl.multiple_of(part * (BLK // TURNS) + g % half * 16, 16)
                    norm(src, ahead, 0, at, pl.multiple_of(base + at, 16))
            return carry
        lax.fori_loop(0, TURNS, turn, 0)
        keep()

        @pl.when(i == n - 1)
        def _():
            for c in early:
                c.wait()
        return

    parts = {} if given else {0: w_copy(0, order[0], 0, CH), 1: w_copy(1, order[0], CH, D - CH),
                              per: w_copy(2, order[1], 0, D), 2 * per: w_copy(3, order[2], 0, D)}

    def body(first, now, later):
        for p in range(3 * per):
            if first and p in parts:
                parts[p].wait()
            project(order[p // per], p % per, now)
            if n > 1 and 0 <= p - 2 < 8:
                for r in range((p - 2) * (tm // 8), (p - 1) * (tm // 8), 16):
                    norm(xan if r < BLK else xbn, both, later, r % BLK, r)
        keep()

    @pl.when(i == 0)
    def _():
        for p in parts:
            if p < 2 * per:
                parts[p].start()
        norm_all(xa, xb, both, 0)
        if not given:
            parts[2 * per].start()
        body(True, 0, 1)

    if n > 1:
        @pl.when(i > 0)
        def _():
            body(False, lax.rem(i, 2), lax.rem(i + 1, 2))


def qkv(par, xa, xa_map, xb, xb_map, g, s, w, b, layer, n, out_block, copy_h, into=None, after=None, given=None, hand=()):
    tm = 2 * BLK
    last = n - 1
    held = [] if given is None else [given]
    chain = bool(held or hand)
    once = dict(pipeline_mode=pl.Buffered(1))
    piece = lambda f, d: pl.BlockSpec((1, BLK, D), lambda i, m: (f(jnp.minimum(i + d, last), m), 0, 0), **(once if n == 1 else {}))
    col = lambda r: pl.BlockSpec((r, tm), lambda i, m: (0, out_block(i)))
    shapes = [pltpu.HBM((D, T), bf16), pltpu.HBM((HEADS, T, 128), bf16), pltpu.HBM((D, T), bf16), pltpu.HBM((HEADS, T), f32), pltpu.HBM((HEADS, T), f32)]
    specs = [col(D), pl.BlockSpec((HEADS, tm, 128), lambda i, m: (0, out_block(i), 0)), col(D), col(HEADS), col(HEADS)]
    if copy_h:
        shapes.append(pltpu.HBM((T, D), bf16))
        specs.append(pl.BlockSpec((tm, D), lambda i, m: (out_block(i), 0)) if held else HBM)
    dma = pltpu.SemaphoreType.DMA
    scratch = [dma((2,))] * (copy_h and not held) + [pltpu.VMEM((1 if chain else 2, tm, D), bf16), dma((3 * TURNS if hand else 4,))]
    if hand:
        shapes += [pltpu.VMEM((EARLY * D, D), bf16), pltpu.VMEM((3 * D, D), bf16)]
        specs += [VMEM, VMEM]
        scratch += [pltpu.VMEM((1, tm, D), bf16), dma((EARLY,))]
    elif held:
        shapes.append(pltpu.VMEM(given.shape, bf16))
        specs.append(VMEM)
    else:
        scratch.append(pltpu.VMEM((3 * D, D), bf16))
    into = list(into or ())
    extra = into + ([after] if after is not None else [])
    alias = {9 + len(held) + len(hand) + a: a for a in range(len(into))}
    if held:
        alias[7] = len(shapes) - 1
    return pl.pallas_call(
        functools.partial(qkv_kernel, layer=layer, n=n, copy_h=copy_h, alias=len(extra), given=len(held), hand=bool(hand), out_block=out_block),
        out_shape=tuple(shapes),
        grid_spec=pltpu.PrefetchScalarGridSpec(
            num_scalar_prefetch=1, grid=(n,),
            in_specs=[piece(xa_map, 0), piece(xb_map, 0), piece(xa_map, 1), piece(xb_map, 1), whole((2, D)), whole((2, D))]
            + ([VMEM, VMEM] if held else [HBM]) + [whole(b.shape)] + [HBM] * (len(hand) + len(extra)),
            out_specs=tuple(specs),
            scratch_shapes=scratch),
        input_output_aliases=alias,
        compiler_params=pltpu.CompilerParams(vmem_limit_bytes=LAYER_LIMIT if chain else 63 << 20, dimension_semantics=("arbitrary",)),
        cost_estimate=pl.CostEstimate(flops=2 * n * tm * D * 3 * D, bytes_accessed=n * tm * D * 10, transcendentals=0),
        name="qkv",
    )(par, *at_hbm(xa, xb, xa, xb, g, s), *(at_vmem(*held, w) if held else at_hbm(w)), *at_hbm(b, *hand), *extra)


def attn_kernel(q_ref, k_ref, v_ref, nq_ref, nk_ref, wo_hbm, wu_hbm, wd_hbm, *refs, layer, have, hp, nq, kb, lag):
    o_ref, wb, sem = (refs[1], refs[3], refs[4]) if have else refs
    step = pl.program_id(0) * pl.num_programs(1) + pl.program_id(1)
    parts = layer_blocks(layer, wo_hbm, wu_hbm, wd_hbm)[have:]
    copies = [pltpu.make_async_copy(p, wb.at[c * D:(c + 1) * D], sem.at[c]) for c, p in enumerate(parts)]

    @pl.when(step == 0)
    def _():
        for c in copies:
            c.start(priority=1)

    @pl.when(step == pl.num_programs(0) * pl.num_programs(1) - 1)
    def _():
        for c in copies:
            c.wait()

    nk = SEQ // kb
    units = [(h, q, k) for h in range(hp) for q in range(SEQ // nq) for k in range(nk)]
    st, lows, acc, rhs = {}, [], {}, {}

    def rows(h):
        return slice(h * HD, (h + 1) * HD)

    def shift_rows(h, q):
        kmax = jnp.max(nk_ref[h:h + 1, :], axis=1, keepdims=True)
        m = jnp.sqrt(nq_ref[h:h + 1, q * nq:(q + 1) * nq] * kmax) * (-1.0 - 2.0 ** -7)
        first = lax.broadcasted_iota(jnp.int32, (128 - HD, nq), 0) == 0
        return jnp.where(first, jnp.broadcast_to(m, (128 - HD, nq)), 0.0).astype(bf16)

    def score(u):
        h, q, k = u
        if k == 0:
            rhs[h, q] = jnp.concatenate([q_ref[rows(h), q * nq:(q + 1) * nq], shift_rows(h, q)], axis=0)
        st[u] = dot(k_ref[h, k * kb:(k + 1) * kb, :], rhs[h, q])

    def mix(u):
        h, q, k = u
        p = jnp.exp2(st.pop(u) * C)
        ls = jnp.sum(p.reshape(kb // 8, 8, nq), axis=0)
        pv = dot(v_ref[rows(h), k * kb:(k + 1) * kb], p.astype(bf16))
        if k:
            a, b = acc[h, q]
            ls, pv = a + ls, b + pv
        acc[h, q] = (ls, pv)
        if k == nk - 1:
            a, b = acc.pop((h, q))
            l = jnp.sum(a, axis=0, keepdims=True)
            lows.append(l)
            o_ref[rows(h), q * nq:(q + 1) * nq] = (b * (1.0 / l)).astype(bf16)

    for i in range(len(units) + lag):
        if i < len(units):
            score(units[i])
        if i >= lag:
            mix(units[i - lag])
    low = lows[0]
    for l in lows[1:]:
        low = jnp.minimum(low, l)
    low = jnp.min(low)

    @pl.when(jnp.logical_not(low >= LOW))
    def _():
        qb = 256
        def body(j, c):
            h = lax.div(j, SEQ // qb)
            qs = pl.ds(pl.multiple_of(lax.rem(j, SEQ // qb) * qb, qb), qb)
            r = pl.ds(pl.multiple_of(h * HD, 32), HD)
            s = dot(k_ref[h, :, :HD], q_ref[r, qs])
            m = jnp.max(s, axis=0, keepdims=True)
            p = jnp.exp2((s - m) * C)
            l = jnp.sum(p, axis=0, keepdims=True)
            o_ref[r, qs] = (dot(v_ref[r, :], p.astype(bf16)) / l).astype(bf16)
            return c
        lax.fori_loop(0, hp * (SEQ // qb), body, 0)


def attn(q, k, v, nq2, nk2, w_o, w_up, w_down, layer, first, count, limit=LAYER_LIMIT, keep=None, hp=8, nq=512, kb=256, lag=3):
    held = [] if keep is None else [keep]
    have = EARLY if held else 0
    blk = pl.BlockSpec((hp * HD, SEQ), lambda i, j: (j, first + i))
    nrm = pl.BlockSpec((hp, SEQ), lambda i, j: (j, first + i))
    return pl.pallas_call(
        functools.partial(attn_kernel, layer=layer, have=have, hp=hp, nq=nq, kb=kb, lag=lag),
        out_shape=(pltpu.HBM((D, count * SEQ), bf16), *(pltpu.VMEM(a.shape, bf16) for a in held), pltpu.VMEM((D + 2 * F - have * D, D), bf16)),
        grid=(count, HEADS // hp),
        in_specs=[blk, pl.BlockSpec((hp, SEQ, 128), lambda i, j: (j, first + i, 0)), blk, nrm, nrm, HBM, HBM, HBM] + [VMEM] * len(held),
        out_specs=(pl.BlockSpec((hp * HD, SEQ), lambda i, j: (j, i)),) + (VMEM,) * (1 + len(held)),
        input_output_aliases={8: 1} if held else {},
        scratch_shapes=[pltpu.SemaphoreType.DMA((1 + 2 * F // D,))],
        compiler_params=pltpu.CompilerParams(vmem_limit_bytes=limit, dimension_semantics=("arbitrary", "arbitrary")),
        cost_estimate=pl.CostEstimate(flops=4 * count * SEQ * SEQ * D, bytes_accessed=count * SEQ * D * 9, transcendentals=count * SEQ * SEQ * HEADS),
        name="attn",
    )(*at_hbm(q, k, v, nq2, nk2), w_o, w_up, w_down, *at_vmem(*held))


def gelu(u):
    c = 0.7978845608028654
    return (0.5 * u) * (1.0 + jnp.tanh(u * (c + (c * 0.044715) * (u * u))))


def mlp_kernel(*refs, layer, base, n, fc, nc, alias, send, count):
    (x_hbm, o_hbm, bo_ref, g_ref, s_ref, bu_ref, bd_ref), refs = refs[:7], refs[7:]
    weights, refs = refs[:count], refs[count + alias:]
    out_ref, refs = refs[0], refs[1:]
    if send:
        vbuf, refs = refs[0], refs[1:]
    (xb, ob, m_s, n_s, act, acc, xsem, osem), refs = refs[:8], refs[8:]

    def w(b, cs):
        if count == 2:
            ref, b = (weights[0], b) if b < EARLY else (weights[1], b - EARLY)
            return ref[b * D:(b + 1) * D, cs]
        return weights[0][b * D:(b + 1) * D, cs]

    i = pl.program_id(0)
    tm = BLK
    assert fc == D
    nj = F // fc
    one = slice(layer, layer + 1)
    gain, shift, bo = g_ref[one, :], s_ref[one, :], bo_ref[one, :]

    away = 3 * IMAGES

    def far(g):
        return g // 3 * 2 + g % 3

    def block(g):
        if not send:
            return g
        f = far(g)
        k = jnp.where(g >= away, 0, jnp.where(g % 3 == 2, 1, 2 + f // IMAGES))
        m = jnp.where(g >= away, g - away, jnp.where(g % 3 == 2, g // 3, f % IMAGES))
        return m * 4 + k

    def x_copy(g):
        slot = g % 2
        return pltpu.make_async_copy(x_hbm.at[pl.ds((base + block(g)) * tm, tm)], xb.at[slot], xsem.at[slot])

    def o_copy(g):
        slot = g % 2
        return pltpu.make_async_copy(o_hbm.at[:, pl.ds(pl.multiple_of(block(g) * tm, tm), tm)], ob.at[slot], osem.at[slot])

    if send:
        ssem, rsem = refs
        dp, me = lax.axis_index("dp"), lax.axis_index("sp")

        def remote(g, dst, peer):
            return pltpu.make_async_remote_copy(
                src_ref=vbuf.at[g % SLOTS], dst_ref=dst, send_sem=ssem.at[g], recv_sem=rsem.at[g], device_id=(dp, peer), device_id_type=MESH)

        def to_far(g):
            return remote(g, out_ref.at[far(g)], jnp.where(far(g) < IMAGES, lax.rem(me + 2, 4), 3 - me))

        def to_near(g):
            return remote(g, out_ref.at[2 * IMAGES + g // 3], me + 1 - 2 * (me % 2))

        slot = jnp.where(i < away, lax.rem(i, SLOTS), SLOTS + i - away)

    def put(cs, v):
        if send:
            vbuf[slot, :, cs] = v
        else:
            out_ref[:, cs] = v

    def cols(c):
        return slice(c * nc, (c + 1) * nc)

    def project(slot):
        for c in range(D // nc):
            y = dot_tn(ob[slot], w(0, cols(c)))
            m_s[:, cols(c)] = (xb[slot, :, cols(c)].astype(f32) + (y + bo[:, cols(c)])).astype(bf16)

    def norm():
        def store(r, m, v):
            n_s[r:r + m, :] = v
        ln_rows(lambda r, m: m_s[r:r + m, :], store, gain, shift, 0, tm)

    @pl.when(i == 0)
    def _():
        o_copy(0).start()
        x_copy(0).start()
        if send:
            barrier = pltpu.get_barrier_semaphore()
            for peer in (me + 1 - 2 * (me % 2), lax.rem(me + 2, 4), 3 - me):
                pl.semaphore_signal(barrier, inc=1, device_id=(dp, peer), device_id_type=MESH)
            pl.semaphore_wait(barrier, 3)
        o_copy(0).wait()
        x_copy(0).wait()
        o_copy(1).start()
        x_copy(1).start()
        project(0)
        norm()

    @pl.when(i + 1 < n)
    def _():
        x_copy(i + 1).wait()
        o_copy(i + 1).wait()

    @pl.when(i + 2 < n)
    def _():
        x_copy(i + 2).start()
        o_copy(i + 2).start()

    if send:
        last = i - 1

        @pl.when(jnp.logical_and(jnp.logical_and(last >= 0, last < away), last % 3 < 2))
        def _():
            to_far(last).start()

        @pl.when(jnp.logical_and(jnp.logical_and(last >= 0, last < away), last % 3 == 2))
        def _():
            to_near(last).start()

        @pl.when(jnp.logical_and(i >= SLOTS, i < away))
        def _():
            to_near(i - SLOTS).wait_send()

    def up(j, c):
        f0 = j * fc + c * nc
        act[j % 2, :, cols(c)] = gelu(dot(n_s[...], w(1 + j, cols(c))) + bu_ref[one, f0:f0 + nc]).astype(bf16)

    def down(j, c):
        y = dot(act[j % 2], w(1 + nj + j, cols(c)))
        if j == 0:
            acc[:, cols(c)] = (m_s[:, cols(c)].astype(f32) + bd_ref[one, cols(c)]) + y
        elif j < nj - 1:
            acc[:, cols(c)] = acc[:, cols(c)] + y
        else:
            put(cols(c), (acc[:, cols(c)] + y).astype(bf16))

    for c in range(fc // nc):
        up(0, c)
    for j in range(1, nj):
        if j == nj - 1:
            project((i + 1) % 2)
        for c in range(D // nc):
            up(j, c)
            down(j - 1, c)
    norm()
    for c in range(D // nc):
        down(nj - 1, c)

    if send:
        @pl.when(i == n - 1)
        def _():
            for g in range(away - SLOTS, away):
                to_near(g).wait_send()
            for g in range(away):
                (to_near if g % 3 == 2 else to_far)(g).wait_recv()


def mlp(x, o, w, bo, g, s, bu, bd, layer, first, count, into=None, send=False, fc=1536, nc=512):
    n = count * SEQ // BLK
    base = first * SEQ // BLK
    dma = pltpu.SemaphoreType.DMA
    vm = pltpu.VMEM
    scratch = [vm((2, BLK, D), bf16), vm((2, D, BLK), bf16), vm((BLK, D), bf16), vm((BLK, D), bf16), vm((2, BLK, fc), bf16), vm((BLK, D), f32),
               dma((2,)), dma((2,))]
    params = dict(dimension_semantics=("arbitrary",))
    if send:
        scratch += [dma((3 * IMAGES,)), dma((3 * IMAGES,))]
        out_shape = (pltpu.HBM((3 * IMAGES, BLK, D), bf16), vm((SLOTS + IMAGES, BLK, D), bf16))
        out_spec = (HBM, VMEM)
        params.update(collective_id=0, has_side_effects=True)
    else:
        out_shape, out_spec = pltpu.HBM((T, D), bf16), pl.BlockSpec((BLK, D), lambda i: (base + i, 0))
    extra = [] if into is None else [into]
    tok = n * BLK
    return pl.pallas_call(
        functools.partial(mlp_kernel, layer=layer, base=base, n=n, fc=fc, nc=nc, alias=len(extra), send=send, count=len(w)),
        out_shape=out_shape,
        grid=(n,),
        in_specs=[HBM, HBM, whole((2, D)), whole((2, D)), whole((2, D)), whole((2, F)), whole((2, D))] + [VMEM] * len(w) + [HBM] * len(extra),
        out_specs=out_spec,
        scratch_shapes=scratch,
        input_output_aliases={7 + len(w): 0} if extra else {},
        compiler_params=pltpu.CompilerParams(vmem_limit_bytes=SEND_LIMIT if send else LAYER_LIMIT, **params),
        cost_estimate=pl.CostEstimate(flops=2 * tok * D * (2 * F + D), bytes_accessed=tok * D * 6, transcendentals=tok * F),
        name="mlp",
    )(*at_hbm(x, o, bo, g, s, bu, bd), *at_vmem(*w), *extra)


def finish_kernel(arrived, vbuf, out, buf, in_sem, via_sem, v_sem):
    me = lax.axis_index("sp")
    copy = pltpu.make_async_copy
    owner = (lax.rem(me + 2, 4), 3 - me, me + 1 - 2 * (me % 2))
    blocks = range(3 * IMAGES)
    ins = [copy(arrived.at[p], buf.at[p], in_sem.at[p]) for p in blocks]
    outs = [copy(buf.at[p], out.at[owner[p // IMAGES] * IMAGES + p % IMAGES], via_sem.at[p]) for p in blocks]
    own = copy(vbuf.at[SLOTS:], out.at[pl.ds(me * IMAGES, IMAGES)], v_sem)
    for c in ins:
        c.start()
    own.start()
    for i, o in zip(ins, outs):
        i.wait()
        o.start()
    for c in outs:
        c.wait()
    own.wait()


def finish(arrived, vbuf):
    dma = pltpu.SemaphoreType.DMA
    return pl.pallas_call(
        finish_kernel,
        out_shape=jax.ShapeDtypeStruct((4 * IMAGES, BLK, D), bf16),
        in_specs=[HBM, VMEM],
        out_specs=HBM,
        scratch_shapes=[pltpu.VMEM((3 * IMAGES, BLK, D), bf16), dma((3 * IMAGES,)), dma((3 * IMAGES,)), dma(())],
        compiler_params=pltpu.CompilerParams(vmem_limit_bytes=SEND_LIMIT),
        cost_estimate=pl.CostEstimate(flops=0, bytes_accessed=24 << 20, transcendentals=0),
        name="finish",
    )(*at_hbm(arrived), *at_vmem(vbuf))


def solution(mesh):
    token_spec = P('dp', 'sp', None)

    def device_step(image_tokens, ln1_gain, ln1_shift, w_qkv, b_qkv, w_out, b_out, ln2_gain, ln2_shift, w_up, b_up, w_down, b_down):
        layers = w_qkv.shape[0]
        w_t = w_qkv.transpose(0, 2, 3, 4, 1).reshape(layers, 3 * D, D)
        w_o = w_out.reshape(layers, D, D)
        me = lax.axis_index('sp')
        par = me.reshape(1).astype(jnp.int32)

        def exchange(k, part):
            return lax.ppermute(part, 'sp', [(s, s ^ k) for s in range(4)])

        def images(k, first, count):
            return lax.dynamic_slice_in_dim(image_tokens, (me ^ k) * IMAGES + first, count)

        far_a, far_b = exchange(2, images(2, 0, 1)), exchange(3, images(3, 0, 1))
        rest_a, rest_b, near = start(image_tokens)
        rest_a, rest_b = exchange(2, rest_a), exchange(3, rest_b)

        here = lambda i, m: i
        pre = (ln1_gain, ln1_shift)
        others = (w_o, w_up, w_down)

        def post(x, l, o, w, *place, **kw):
            return mlp(x, o, w, b_out, ln2_gain, ln2_shift, b_up, b_down, l, *place, **kw)

        *bufs, wa, wq = qkv(par, image_tokens, lambda i, m: m[0] * IMAGES + i, near, here, *pre, w_t, b_qkv, 0, IMAGES, lambda i: 2 * i, True,
                            hand=others)
        *bufs, wa = qkv(par, far_a, here, far_b, here, *pre, wq, b_qkv, 0, 1, lambda i: 1, True, into=bufs, given=wa)
        o, *w = attn(*bufs[:5], *others, 0, 0, 1, keep=wa)
        h = post(bufs[5], 0, o, w, 0, 1)
        bufs = qkv(par, rest_a, here, rest_b, here, *pre, w_t, b_qkv, 0, IMAGES - 1, lambda i: 2 * i + 3, True, into=bufs, after=h)
        o, *w = attn(*bufs[:5], *others, 0, 1, IMAGES - 1)
        h = post(bufs[5], 0, o, w, 1, IMAGES - 1, into=h)
        x = h.reshape(4 * IMAGES, BLK, D)
        bufs = qkv(par, x, lambda i, m: 2 * i, x, lambda i, m: 2 * i + 1, *pre, w_t, b_qkv, 1, 2 * IMAGES, lambda i: i, False)
        o, *w = attn(*bufs[:5], *others, 1, 0, IMAGES, limit=SEND_LIMIT)
        return finish(*post(h, 1, o, w, 0, IMAGES, send=True))

    return jax.shard_map(device_step, mesh=mesh, in_specs=(token_spec,) + (P(),) * 12, out_specs=token_spec, check_vma=False)
```
